32 devices in a mesh: gx: 4 (over z), gy: 2 (over y), ea: 4 (over x, core).
Axes of the slice: x: 2, y: 2, z: 4, core: 2. Of those that a mesh axis runs over, the one named last changes fastest.
Arguments:
- load_displacement: float32 [3, 16, 32, 512], P(None, 'gx', 'gy', 'ea'), may hold values from -6 to 6
- load_enriched: float32 [15, 8192], P(None, ('gx', 'gy', 'ea')), may hold values from -24 to 24
- stiffness_shift: float32 [16, 32, 512], P('gx', 'gy', 'ea'), may hold values from 2 to 8
- enriched_diag: float32 [15, 8192], P(None, ('gx', 'gy', 'ea')), may hold values from 11 to 17
- enriched_off: float32 [15, 15, 8192], P(None, None, ('gx', 'gy', 'ea')), may hold values from -0.4 to 0.4
- coupling: float32 [3, 15, 16384], P(None, None, ('gx', 'gy', 'ea')), may hold values from -0.15 to 0.15
- slot_kind: int32 [32, 4, 128], P(('gx', 'gy', 'ea')), may hold values from 0 to 2, as said below
- slot_cell: int32 [32, 4, 128], P(('gx', 'gy', 'ea')), may hold values from 0 to 8191, as said below
- slot_node: int32 [32, 4, 128], P(('gx', 'gy', 'ea')), may hold values from 0 to 255, as said below
Outputs:
- solution_displacement: float32 [3, 16, 32, 512], P(None, 'gx', 'gy', 'ea')
- residual_displacement: float32 [3, 16, 32, 512], P(None, 'gx', 'gy', 'ea')
- solution_enriched: float32 [15, 8192], P(None, ('gx', 'gy', 'ea'))
- residual_enriched: float32 [15, 8192], P(None, ('gx', 'gy', 'ea'))
The draws below stay inside these ranges and needn't reach their ends.
Inputs may be any that keep to these rules, and one draw needn't show every extreme that they name: `slot_kind`: within each block of 128 slots of one device to one owner the slots of kind 1 or 2 come first; in every draw some owner receives 128 such slots from each of the 4 devices of its column. `slot_cell`: distinct within one device. `slot_node`: distinct within each block of 128 slots of one device to one owner.
All inputs are finite; a program needn't handle non-finite values.
Results may differ from the reference program's by a relative error of at most 0.0003.
Values sent between devices are 32-bit elements; how exact they have to be, the bound alone decides.
A program may use at most 64 MiB of HBM per device.

```python
import jax
import jax.numpy as jnp
from jax import lax

CX = 4
CY = 16
CZ = 128
ENB = 256
CAP = 128
ECOMP = 15
ITERS = 3
NX = 16
NY = 32
NZ = 512
NE = 8192
SLOTS = 16384
N_GX = 4
N_GY = 2
N_EA = 4
DEVICES = 32


def draw_slot_cell(key, part):
    device_keys = jax.random.split(jax.random.fold_in(key, 11), DEVICES)

    def one_device(device_key):
        return jax.random.permutation(device_key, CX * CY * CZ)[:N_EA * CAP].astype(jnp.int32)
    return jax.vmap(one_device)(device_keys).reshape(DEVICES, N_EA, CAP)


def draw_slot_node(key, part):
    block_keys = jax.random.split(jax.random.fold_in(key, 17), DEVICES * N_EA)

    def one_block(block_key):
        return jax.random.permutation(block_key, ENB)[:CAP].astype(jnp.int32)
    return jax.vmap(one_block)(block_keys).reshape(DEVICES, N_EA, CAP)


def draw_slot_kind(key, part):
    live_key, kind_key, column_key, owner_key = jax.random.split(jax.random.fold_in(key, 29), 4)
    live_count = jax.random.randint(live_key, (DEVICES, N_EA), CAP // 8, CAP + 1)
    columns = DEVICES // N_EA
    column = jax.random.randint(column_key, (), 0, columns)
    target = jax.random.randint(owner_key, (), 0, N_EA)
    device_ids = jnp.arange(DEVICES, dtype=jnp.int32)[:, None]
    owner_ids = jnp.arange(N_EA, dtype=jnp.int32)[None, :]
    full_block = (device_ids // N_EA == column) & (owner_ids == target)
    live_count = jnp.where(full_block, CAP, live_count)
    slot_kinds = jax.random.randint(kind_key, (DEVICES, N_EA, CAP), 1, 3)
    position = jnp.arange(CAP, dtype=jnp.int32)[None, None, :]
    return jnp.where(position < live_count[:, :, None], slot_kinds, 0).astype(jnp.int32)


def shard_levels(own_key, extent, cuts, low, largest):
    gain, own = 1.0, jax.random.fold_in(own_key, 6)
    for dim, blocks in cuts:
        steps = jnp.exp(jax.random.uniform(jax.random.fold_in(own, dim), (blocks,), jnp.float32, low / len(cuts), largest / len(cuts)))
        gain = gain * jnp.repeat(steps, extent[dim] // blocks).reshape([-1 if axis == dim else 1 for axis in range(len(extent))])
    return gain


def gaussian(own_key, extent, spread, limit, cuts=(), kind=jnp.bfloat16):
    loudness = shard_levels(own_key, extent, cuts, -0.22, 0.18) if cuts else 1.0
    entries = jax.random.normal(own_key, extent, jnp.float32) * spread * loudness
    return jnp.minimum(jnp.maximum(entries, -limit), limit).astype(kind)


def setup_inputs(seed: int = 0) -> dict:
    seeds = jax.random.split(jax.random.key(seed), 10)
    load_displacement = gaussian(seeds[0], (3, NX, NY, NZ), 1.0, 6.0, ((1, 4), (2, 2), (3, 4)), jnp.float32)
    load_enriched = gaussian(seeds[1], (ECOMP, NE), 4.0, 24.0, ((1, 32),), jnp.float32)
    stiffness_shift = jnp.clip(2.0 + 6.0 * jax.random.uniform(seeds[2], (NX, NY, NZ), jnp.float32) ** shard_levels(seeds[2], (NX, NY, NZ), ((0, 4), (1, 2), (2, 4)), -0.2, 0.2), 2.0, 8.0)
    enriched_diag = jnp.clip(11.0 + 6.0 * jax.random.uniform(seeds[3], (ECOMP, NE), jnp.float32) ** shard_levels(seeds[3], (ECOMP, NE), ((1, 32),), -0.2, 0.2), 11.0, 17.0)
    enriched_off = jnp.clip(jax.random.uniform(seeds[4], (ECOMP, ECOMP, NE), jnp.float32, -0.4, 0.4) * shard_levels(seeds[4], (ECOMP, ECOMP, NE), ((2, 32),), -0.4, 0.0), -0.4, 0.4)
    coupling = jnp.clip(jax.random.uniform(seeds[5], (3, ECOMP, SLOTS), jnp.float32, -0.15, 0.15) * shard_levels(seeds[5], (3, ECOMP, SLOTS), ((2, 32),), -0.4, 0.0), -0.15, 0.15)
    slot_kind = draw_slot_kind(jax.random.fold_in(seeds[9], 71), 0)
    slot_cell = draw_slot_cell(jax.random.fold_in(seeds[9], 71), 0)
    slot_node = draw_slot_node(jax.random.fold_in(seeds[9], 71), 0)
    return {"load_displacement": load_displacement, "load_enriched": load_enriched, "stiffness_shift": stiffness_shift, "enriched_diag": enriched_diag, "enriched_off": enriched_off, "coupling": coupling, "slot_kind": slot_kind, "slot_cell": slot_cell, "slot_node": slot_node}


HIGHEST_PRECISION = lax.Precision.HIGHEST


def stencil(displacement, stiffness_shift):
    padded = jnp.pad(displacement, ((0, 0), (1, 1), (1, 1), (1, 1)))
    beside = padded[:, 2:, 1:-1, 1:-1] + padded[:, :-2, 1:-1, 1:-1]
    beside = beside + padded[:, 1:-1, 2:, 1:-1] + padded[:, 1:-1, :-2, 1:-1]
    beside = beside + padded[:, 1:-1, 1:-1, 2:] + padded[:, 1:-1, 1:-1, :-2]
    return (6.0 + stiffness_shift)[None] * displacement - beside


def enriched_block(enriched_diag, enriched_off):
    components = enriched_diag.shape[0]
    identity = jnp.eye(components, dtype=jnp.float32)
    symmetric = 0.5 * (enriched_off + jnp.transpose(enriched_off, (1, 0, 2)))
    return symmetric * (1.0 - identity)[:, :, None] + identity[:, :, None] * enriched_diag[:, None, :]


def slot_columns(kinds_flat):
    heaviside = (kinds_flat >= 1).astype(jnp.float32)
    tip_mask = (kinds_flat == 2).astype(jnp.float32)
    return jnp.concatenate([jnp.broadcast_to(heaviside, (3, heaviside.shape[0])), jnp.broadcast_to(tip_mask, (12, tip_mask.shape[0]))], axis=0)


def inner(first, second):
    return jnp.sum(first[0] * second[0]) + jnp.sum(first[1] * second[1])


def reference(load_displacement, load_enriched, stiffness_shift, enriched_diag, enriched_off, coupling, slot_kind, slot_cell, slot_node):
    device_ids = jnp.arange(N_GX * N_GY * N_EA, dtype=jnp.int32)[:, None, None]
    owners = jnp.arange(N_EA, dtype=jnp.int32)[None, :, None]
    column_i = device_ids // (N_GY * N_EA)
    column_j = (device_ids // N_EA) % N_GY
    layer_k = device_ids % N_EA
    cell_x = slot_cell // (CY * CZ)
    cell_y = (slot_cell // CZ) % CY
    cell_z = slot_cell % CZ
    global_cell = (((column_i * CX + cell_x) * NY + column_j * CY + cell_y) * NZ + layer_k * CZ + cell_z).reshape(-1).astype(jnp.int32)
    global_node = ((device_ids - layer_k + owners) * ENB + slot_node).reshape(-1).astype(jnp.int32)
    slot_weights = coupling * slot_columns(slot_kind.reshape(-1))[None]
    enriched_stiff = enriched_block(enriched_diag, enriched_off)
    cell_total = NX * NY * NZ

    def operate(direction):
        displacement, enriched = direction
        flat = displacement.reshape(3, cell_total)
        picked = flat[:, global_cell]
        to_nodes = jnp.einsum('ijs,is->js', slot_weights, picked, precision=HIGHEST_PRECISION)
        pushed_enriched = jnp.einsum('ijn,jn->in', enriched_stiff, enriched, precision=HIGHEST_PRECISION)
        pushed_enriched = pushed_enriched + jnp.zeros(enriched.shape, jnp.float32).at[:, global_node].add(to_nodes)
        values = enriched[:, global_node]
        to_cells = jnp.einsum('ijs,js->is', slot_weights, values, precision=HIGHEST_PRECISION)
        added = jnp.zeros((3, cell_total), jnp.float32).at[:, global_cell].add(to_cells)
        pushed_displacement = stencil(displacement, stiffness_shift) + added.reshape(displacement.shape)
        return (pushed_displacement, pushed_enriched)

    solution = (jnp.zeros_like(load_displacement), jnp.zeros_like(load_enriched))
    residual = (load_displacement, load_enriched)
    direction = residual
    norm_now = inner(residual, residual)
    for iteration in range(ITERS):
        image = operate(direction)
        alpha = norm_now / inner(direction, image)
        solution = jax.tree.map(lambda member, partner: member + alpha * partner, solution, direction)
        residual = jax.tree.map(lambda member, partner: member - alpha * partner, residual, image)
        norm_next = inner(residual, residual)
        ratio = norm_next / norm_now
        direction = jax.tree.map(lambda member, partner: member + ratio * partner, residual, direction)
        norm_now = norm_next
    return solution[0], residual[0], solution[1], residual[1]
```

```python
import functools

import jax
import jax.numpy as jnp
from jax import lax
from jax.experimental import pallas as pl
from jax.experimental.pallas import tpu as pltpu
from jax.sharding import PartitionSpec as P

ITERS = 3
CENTRE = 11.5
AXES = ("gx", "gy", "ea")
MESH = pl.DeviceIdType.MESH
F32 = jnp.float32
BF16 = jnp.bfloat16


def pieces(x):
    high = x.astype(BF16)
    return high, (x - high.astype(F32)).astype(BF16)


def stacked(x):
    high, low = pieces(x)
    return jnp.concatenate([high, low], axis=0)


def folded(product):
    half = product.shape[0] // 2
    return product[:half] + product[half:]


def iota(shape, dim):
    return lax.broadcasted_iota(jnp.int32, shape, dim)


def cg_coefficients(moment):
    def inner(first, second):
        total = None
        for i, a in enumerate(first):
            for j, b in enumerate(second):
                term = a * b * moment[i + j]
                total = term if total is None else total + term
        return total

    one = jnp.ones_like(moment[0])
    residual, direction, solution = [one], [one], []
    norm = moment[0]
    for step in range(ITERS):
        image = [CENTRE * d for d in direction] + [0.0 * one]
        for i, d in enumerate(direction):
            image[i + 1] = image[i + 1] + d
        alpha = norm / inner(direction, image)
        solution = [
            (solution[i] if i < len(solution) else 0.0) + alpha * d
            for i, d in enumerate(direction)
        ]
        residual = [
            (residual[i] if i < len(residual) else 0.0) - alpha * d for i, d in enumerate(image)
        ]
        if step + 1 < ITERS:
            new = inner(residual, residual)
            ratio = new / norm
            norm = new
            direction = [
                r + (ratio * direction[i] if i < len(direction) else 0.0)
                for i, r in enumerate(residual)
            ]
    return solution, residual


def kernel(
    sizes, groups,
    load_v, load_w, shift_h, diag_h, off_h, coupling_h, kind_h, cell_h, node_h,
    vu, wu, coefs,
    w_first, shift, diag, off, coupling, kind, cell, node, load_s,
    weights, stiff, lanes, lanes_t, rows, rows_b, nodes_mine, nodes_recv, centre_diag,
    node_in, x_in, y_in, z_in, w_in, t_in, y_out, z_out, t_out, red, red_out,
    node_s, node_r, x_s, x_r, y_s, y_r, z_s, z_r, w_s, w_r, t_s, t_r, red_s, red_r,
):
    n_gx, n_gy, n_ea = sizes
    comps, dx, dy, dz = load_v.shape
    ecomp, enb = load_w.shape
    epad = wu.shape[1]
    cap = node.shape[2]
    per = dx * dy
    allrows = comps * per
    groups8 = allrows // 8
    gi, gj, ek = (lax.axis_index(a) for a in AXES)
    own = {"gx": gi, "gy": gj, "ea": ek}
    count = dict(zip(AXES, sizes))

    def members(group):
        total = 1
        for a in group:
            total *= count[a]
        me = 0
        for a in group:
            me = me * count[a] + own[a]

        def target(d):
            flat = lax.rem(me + d, total)
            coords = dict(own)
            for a in reversed(group):
                coords[a] = lax.rem(flat, count[a])
                flat = lax.div(flat, count[a])
            return tuple(coords[a] for a in AXES)

        return total, me, target

    barrier = pltpu.get_barrier_semaphore()
    wide = n_gx - 1 > ITERS
    expected = 0
    for group in groups if wide else (("gy", "ea"),):
        total, _, target = members(group)
        for d in range(1, total):
            pl.semaphore_signal(barrier, inc=1, device_id=target(d), device_id_type=MESH)
        expected += total - 1
    if not wide:
        for s, there in ((1, gi < n_gx - 1), (-1, gi > 0)):
            @pl.when(there)
            def _():
                pl.semaphore_signal(
                    barrier, inc=1, device_id=(gi + s, gj, ek), device_id_type=MESH
                )
            expected = expected + jnp.where(there, 1, 0)

    loads = {}
    for at, (name, src, dst) in enumerate((
        ("cell", cell_h, cell), ("v", load_v, vu.at[0]), ("node", node_h, node),
        ("kind", kind_h, kind), ("w", load_w, w_first), ("coupling", coupling_h, coupling),
        ("shift", shift_h, shift), ("off", off_h, off), ("diag", diag_h, diag),
    )):
        loads[name] = pltpu.make_async_copy(src, dst, load_s.at[at])
        loads[name].start()

    def columns(tile):
        full = jnp.concatenate(
            [tile.astype(F32), jnp.zeros((cap - tile.shape[0], cap), F32)], axis=0
        )
        return jnp.transpose(full).astype(jnp.int32)

    loads["cell"].wait()
    tile = cell[0]
    tile_row = lax.div(tile, dz)
    tile_lane = tile - tile_row * dz
    lane_columns = columns(tile_lane)
    for o in range(n_ea):
        span = slice(o * cap, (o + 1) * cap)
        lanes[:, span] = jnp.where(
            iota((dz, cap), 0) == tile_lane[o : o + 1], 1.0, 0.0
        ).astype(BF16)
        lanes_t[span, :] = jnp.where(
            iota((cap, dz), 1) == lane_columns[:, o : o + 1], 1.0, 0.0
        ).astype(BF16)
        r = jnp.where(iota((per, cap), 0) == tile_row[o : o + 1], 1.0, 0.0)
        rows[:, span] = r
        rows_b[:, span] = r.astype(BF16)
    loads["node"].wait()
    for o in range(n_ea):
        nodes_mine[o] = jnp.where(
            iota((enb, cap), 0) == node[0, o : o + 1, :], 1.0, 0.0
        ).astype(BF16)
    loads["kind"].wait()
    loads["coupling"].wait()
    no_row = jnp.zeros((epad - ecomp, n_ea * cap), F32)
    for i in range(comps):
        for o in range(n_ea):
            k = kind[0, o : o + 1, :]
            heavi = jnp.where(k >= 1, 1.0, 0.0)
            tip = jnp.where(k == 2, 1.0, 0.0)
            mask = jnp.where(iota((ecomp, cap), 0) < 3, heavi, tip)
            span = slice(o * cap, (o + 1) * cap)
            weights[i, :, span] = jnp.concatenate(
                [coupling[i, :, span] * mask, no_row[:, span]], axis=0
            )
    loads["w"].wait()
    wu[0] = jnp.concatenate([w_first[...], jnp.zeros((epad - ecomp, enb), F32)], axis=0)
    loads["v"].wait()

    pl.semaphore_wait(barrier, expected)

    def partner(d):
        return lax.rem(ek + d, n_ea)

    has = {
        ("gx", 1): gi < n_gx - 1, ("gx", -1): gi > 0,
        ("gy", 1): gj < n_gy - 1, ("gy", -1): gj > 0,
        ("ea", 1): ek < n_ea - 1, ("ea", -1): ek > 0,
    }
    beside = {
        ("gx", s): (gi + s, gj, ek) for s in (1, -1)
    } | {("gy", s): (gi, gj + s, ek) for s in (1, -1)} | {
        ("ea", s): (gi, gj, ek + s) for s in (1, -1)
    }
    slot = {1: 0, -1: 1}

    def remote(src, dst, s_sem, r_sem, device):
        return pltpu.make_async_remote_copy(
            src_ref=src, dst_ref=dst, send_sem=s_sem, recv_sem=r_sem,
            device_id=device, device_id_type=MESH,
        )

    def x_copy(op, s):
        return remote(
            vu.at[op, :, dx - 1 if s == 1 else 0], x_in.at[op, slot[s]],
            x_s.at[op, slot[s]], x_r.at[op, slot[s]], beside["gx", s],
        )

    def y_copy(op, s):
        return remote(
            y_out.at[op, slot[s]], y_in.at[op, slot[s]],
            y_s.at[op, slot[s]], y_r.at[op, slot[s]], beside["gy", s],
        )

    def z_copy(op, s):
        return remote(
            z_out.at[op, slot[s]], z_in.at[op, slot[s]],
            z_s.at[op, slot[s]], z_r.at[op, slot[s]], beside["ea", s],
        )

    def w_copy(op, d):
        return remote(
            wu.at[op], w_in.at[op, ek], w_s.at[op, d], w_r.at[op, d], (gi, gj, partner(d))
        )

    def t_copy(op, d):
        return remote(
            t_out.at[op, partner(d)], t_in.at[op, ek], t_s.at[op, d], t_r.at[op, d],
            (gi, gj, partner(d)),
        )

    def node_copy(d):
        return remote(
            node, node_in.at[ek], node_s.at[d], node_r.at[d], (gi, gj, partner(d))
        )

    lane_i = iota((8, dz), 1)
    lane_r = iota((1, dz), 1)

    def product(op_a, op_b):
        pv = jnp.sum((vu[op_a] * vu[op_b]).reshape(groups8, 8, dz), axis=0)
        pw = jnp.sum(wu[op_a] * wu[op_b], axis=0, keepdims=True)
        row = jnp.sum(pv, axis=0, keepdims=True)
        total = row
        for b in range(enb // dz):
            total = total + pw[:, b * dz : (b + 1) * dz]
        return total

    moments = []
    for op in range(ITERS):
        for s in (1, -1):
            @pl.when(has["gx", s])
            def _():
                x_copy(op, s).start()
        for d in range(1, n_ea):
            w_copy(op, d).start()
            if op == 0:
                node_copy(d).start()
        v2 = vu[op].reshape(allrows, dz)
        for i in range(comps):
            for a in range(dx):
                at = i * dx + a
                y_out[op, 0, at : at + 1, :] = vu[op, i, a, dy - 1 : dy, :]
                y_out[op, 1, at : at + 1, :] = vu[op, i, a, 0:1, :]
        for s in (1, -1):
            @pl.when(has["gy", s])
            def _():
                y_copy(op, s).start()
        up = jnp.zeros((8, dz), F32)
        down = jnp.zeros((8, dz), F32)
        for g in range(groups8):
            part = v2[8 * g : 8 * g + 8]
            up = jnp.where(lane_i == g, part[:, dz - 1 : dz], up)
            down = jnp.where(lane_i == g, part[:, 0:1], down)
        z_out[op, 0] = up
        z_out[op, 1] = down
        for s in (1, -1):
            @pl.when(has["ea", s])
            def _():
                z_copy(op, s).start()
        seen = folded(jnp.dot(stacked(v2), lanes[...], preferred_element_type=F32))
        total = None
        for i in range(comps):
            picked = jnp.sum(seen[i * per : (i + 1) * per] * rows[...], axis=0, keepdims=True)
            term = weights[i] * picked
            total = term if total is None else total + term
        for o in range(n_ea):
            t_out[op, o] = total[:, o * cap : (o + 1) * cap]
        for d in range(1, n_ea):
            t_copy(op, d).start()

        if op == 0:
            loads["off"].wait()
            loads["diag"].wait()
            for p in range(ecomp):
                whole = 0.5 * (off[p] + off[:, p, :])
                whole = jnp.where(
                    iota((ecomp, enb), 0) == p, diag[p : p + 1, :] - CENTRE, whole
                )
                stiff[p] = jnp.concatenate(
                    [whole, jnp.zeros((epad - ecomp, enb), F32)], axis=0
                )
            loads["shift"].wait()
            centre_diag[...] = shift[...] + (6.0 - CENTRE)
            node_in[ek] = node[...]
        v4 = vu[op]
        zero = jnp.zeros((comps, 1, dy, dz), F32)
        near = jnp.concatenate([zero, v4[:, : dx - 1]], axis=1) + jnp.concatenate(
            [v4[:, 1:], zero], axis=1
        )
        near = near.reshape(allrows, dz)
        lane_all = iota((allrows, dz), 1)
        row_all = lax.rem(iota((allrows, dz), 0), dy)
        near = near + jnp.where(lane_all == 0, 0.0, pltpu.roll(v2, 1, 1))
        near = near + jnp.where(lane_all == dz - 1, 0.0, pltpu.roll(v2, dz - 1, 1))
        near = near + jnp.where(row_all == 0, 0.0, pltpu.roll(v2, 1, 0))
        near = near + jnp.where(row_all == dy - 1, 0.0, pltpu.roll(v2, allrows - 1, 0))
        vu[op + 1] = centre_diag[...][None] * v4 - near.reshape(v4.shape)
        w = wu[op]
        acc = stiff[0] * w[0:1]
        for p in range(1, ecomp):
            acc = acc + stiff[p] * w[p : p + 1]
        if op == 0:
            moments.append(product(0, 0))
        else:
            moments.append(product(op, op))

        w_in[op, ek] = w
        t_in[op, ek] = t_out[op, ek]
        if op + 1 == ITERS:
            packed = jnp.zeros((1, dz), F32)
            for n, row in enumerate(moments):
                packed = jnp.where(lane_r == n, jnp.sum(row, axis=1, keepdims=True), packed)
        if op == 0:
            for d in range(1, n_ea):
                node_copy(d).wait_recv()
            own_rows = jnp.concatenate(
                [node_in[o, 0, pl.ds(ek, 1), :] for o in range(n_ea)], axis=0
            )
            node_columns = columns(own_rows)
            for o in range(n_ea):
                nodes_recv[o * cap : (o + 1) * cap, :] = jnp.where(
                    iota((cap, enb), 1) == node_columns[:, o : o + 1], 1.0, 0.0
                ).astype(BF16)
        for d in range(1, n_ea):
            w_copy(op, d).wait_recv()
        values = jnp.concatenate(
            [
                folded(jnp.dot(stacked(w_in[op, o]), nodes_mine[o], preferred_element_type=F32))
                for o in range(n_ea)
            ],
            axis=1,
        )
        spread_h, spread_l = [], []
        for i in range(comps):
            h, l = pieces(jnp.sum(weights[i] * values, axis=0, keepdims=True))
            spread_h.append(rows_b[...] * h)
            spread_l.append(rows_b[...] * l)
        added = folded(
            jnp.dot(
                jnp.concatenate(spread_h + spread_l, axis=0), lanes_t[...],
                preferred_element_type=F32,
            )
        )
        vu[op + 1] += added.reshape(comps, dx, dy, dz)
        for s in (1, -1):
            @pl.when(has["gx", -s])
            def _():
                x_copy(op, s).wait_recv()
                edge = 0 if s == 1 else dx - 1
                vu[op + 1, :, edge] -= x_in[op, slot[s]]

            @pl.when(has["gy", -s])
            def _():
                y_copy(op, s).wait_recv()
                edge = 0 if s == 1 else dy - 1
                for i in range(comps):
                    for a in range(dx):
                        at = i * dx + a
                        vu[op + 1, i, a, edge : edge + 1, :] -= y_in[op, slot[s], at : at + 1, :]

            @pl.when(has["ea", -s])
            def _():
                z_copy(op, s).wait_recv()
                edge = 0 if s == 1 else dz - 1
                tile = z_in[op, slot[s]]
                for i in range(comps):
                    for a in range(dx):
                        for b in range(dy // 8):
                            g = (i * dx + a) * (dy // 8) + b
                            vu[op + 1, i, a, 8 * b : 8 * b + 8, :] -= jnp.where(
                                lane_i == edge, tile[:, g : g + 1], 0.0
                            )
        for d in range(1, n_ea):
            t_copy(op, d).wait_recv()
        terms = jnp.concatenate([t_in[op, o] for o in range(n_ea)], axis=1)
        acc = acc + folded(
            jnp.dot(stacked(terms), nodes_recv[...], preferred_element_type=F32)
        )
        wu[op + 1] = acc
        moments.append(product(op, op + 1))

    last = 2 * ITERS - 1
    packed = jnp.where(lane_r == last, jnp.sum(moments[last], axis=1, keepdims=True), packed)
    for stage, group in enumerate(groups):
        total, me, target = members(group)
        red_out[stage] = packed

        def red_copy(d):
            return remote(
                red_out.at[stage], red.at[stage, me], red_s.at[stage, d], red_r.at[stage, d],
                target(d),
            )

        for d in range(1, total):
            red_copy(d).start()
        red[stage, me] = packed
        for d in range(1, total):
            red_copy(d).wait_recv()
        packed = jnp.sum(red[stage, :total], axis=0)

    sol, res = cg_coefficients([packed[:, n : n + 1] for n in range(2 * ITERS)])
    tile = jnp.zeros((1, dz), F32)
    for n, c in enumerate(sol + res):
        tile = jnp.where(lane_r == n, c, tile)
    coefs[...] = tile

    for op in range(ITERS):
        for s in (1, -1):
            @pl.when(has["gx", s])
            def _():
                x_copy(op, s).wait_send()

            @pl.when(has["gy", s])
            def _():
                y_copy(op, s).wait_send()

            @pl.when(has["ea", s])
            def _():
                z_copy(op, s).wait_send()
        for d in range(1, n_ea):
            w_copy(op, d).wait_send()
            t_copy(op, d).wait_send()
            if op == 0:
                node_copy(d).wait_send()
    for stage, group in enumerate(groups):
        total, me, target = members(group)
        for d in range(1, total):
            remote(
                red_out.at[stage], red.at[stage, me], red_s.at[stage, d], red_r.at[stage, d],
                target(d),
            ).wait_send()


def combine_kernel(vu, wu, coefs, sol_v, res_v, sol_w, res_w):
    ecomp = sol_w.shape[0]
    tile = coefs[...]
    solution = [tile[:, n : n + 1] for n in range(ITERS)]
    residual = [tile[:, ITERS + n : ITERS + n + 1] for n in range(ITERS + 1)]

    def combine(factors, terms):
        out = factors[0] * terms[0]
        for f, t in zip(factors[1:], terms[1:]):
            out = out + f * t
        return out

    shape = sol_v.shape
    flat = (shape[0] * shape[1] * shape[2], shape[3])
    v_terms = [vu[n].reshape(flat) for n in range(ITERS + 1)]
    w_terms = [wu[n] for n in range(ITERS + 1)]
    sol_v[...] = combine(solution, v_terms).reshape(shape)
    res_v[...] = combine(residual, v_terms).reshape(shape)
    sol_w[...] = combine(solution, w_terms)[:ecomp]
    res_w[...] = combine(residual, w_terms)[:ecomp]


def body(sizes, *args):
    load_v, load_w, shift, diag, off, coupling, kind, cell, node = args
    n_ea = sizes[2]
    total = sizes[0] * sizes[1] * sizes[2]
    groups = (AXES,) if total <= 64 else (("gx",), ("gy", "ea"))
    widest = total if total <= 64 else max(sizes[0], sizes[1] * sizes[2])
    comps, dx, dy, dz = load_v.shape
    ecomp, enb = load_w.shape
    cap = node.shape[2]
    vmem = pltpu.VMEM
    dma = pltpu.SemaphoreType.DMA
    y_rows = -(-comps * dx // 8) * 8
    epad = -(-ecomp // 16) * 16
    slots = n_ea * cap
    scratch = [
        vmem(load_w.shape, F32), vmem(shift.shape, F32), vmem(diag.shape, F32),
        vmem(off.shape, F32), vmem(coupling.shape, F32),
        vmem(kind.shape, jnp.int32), vmem(cell.shape, jnp.int32), vmem(node.shape, jnp.int32),
        dma((9,)),
        vmem((comps, epad, slots), F32),
        vmem((ecomp, epad, enb), F32),
        vmem((dz, slots), BF16),
        vmem((slots, dz), BF16),
        vmem((dx * dy, slots), F32),
        vmem((dx * dy, slots), BF16),
        vmem((n_ea, enb, cap), BF16),
        vmem((slots, enb), BF16),
        vmem((dx, dy, dz), F32),
        vmem((n_ea,) + node.shape, jnp.int32),
        vmem((ITERS, 2, comps, dy, dz), F32),
        vmem((ITERS, 2, y_rows, dz), F32),
        vmem((ITERS, 2, 8, dz), F32),
        vmem((ITERS, n_ea, epad, enb), F32),
        vmem((ITERS, n_ea, epad, cap), F32),
        vmem((ITERS, 2, y_rows, dz), F32),
        vmem((ITERS, 2, 8, dz), F32),
        vmem((ITERS, n_ea, epad, cap), F32),
        vmem((len(groups), widest, 1, dz), F32),
        vmem((len(groups), 1, dz), F32),
        dma((n_ea,)), dma((n_ea,)),
        dma((ITERS, 2)), dma((ITERS, 2)),
        dma((ITERS, 2)), dma((ITERS, 2)),
        dma((ITERS, 2)), dma((ITERS, 2)),
        dma((ITERS, n_ea)), dma((ITERS, n_ea)),
        dma((ITERS, n_ea)), dma((ITERS, n_ea)),
        dma((len(groups), widest)), dma((len(groups), widest)),
    ]
    basis = pl.pallas_call(
        functools.partial(kernel, sizes, groups),
        out_shape=(
            pltpu.VMEM((ITERS + 1,) + load_v.shape, F32),
            pltpu.VMEM((ITERS + 1, epad, enb), F32),
            pltpu.VMEM((1, dz), F32),
        ),
        in_specs=[pl.BlockSpec(memory_space=pltpu.HBM)] * 9,
        out_specs=[pl.BlockSpec(memory_space=vmem)] * 3,
        scratch_shapes=scratch,
        compiler_params=pltpu.CompilerParams(
            collective_id=0, has_side_effects=True
        ),
        name="krylov",
    )(*args)
    return tuple(
        pl.pallas_call(
            combine_kernel,
            out_shape=tuple(
                jax.ShapeDtypeStruct(like.shape, F32)
                for like in (load_v, load_v, load_w, load_w)
            ),
            in_specs=[pl.BlockSpec(memory_space=vmem)] * 3,
            out_specs=[pl.BlockSpec(memory_space=vmem)] * 4,
            compiler_params=pltpu.CompilerParams(vmem_limit_bytes=8 << 20),
            name="combine",
        )(*basis)
    )


def solution(mesh):
    column = ("gx", "gy", "ea")
    placed = (
        P(None, "gx", "gy", "ea"),
        P(None, column),
        P("gx", "gy", "ea"),
        P(None, column),
        P(None, None, column),
        P(None, None, column),
        P(column, None, None),
        P(column, None, None),
        P(column, None, None),
    )
    return jax.shard_map(
        functools.partial(body, tuple(mesh.shape[a] for a in AXES)),
        mesh=mesh,
        in_specs=placed,
        out_specs=(
            P(None, "gx", "gy", "ea"),
            P(None, "gx", "gy", "ea"),
            P(None, column),
            P(None, column),
        ),
        check_vma=False,
    )
```

```python
import functools

import jax
import jax.numpy as jnp
from jax import lax
from jax.experimental import pallas as pl
from jax.experimental.pallas import tpu as pltpu
from jax.sharding import PartitionSpec as P

ITERS = 3
CENTRE = 11.5
AXES = ("gx", "gy", "ea")
MESH = pl.DeviceIdType.MESH
F32 = jnp.float32
BF16 = jnp.bfloat16


def pieces(x):
    high = x.astype(BF16)
    return high, (x - high.astype(F32)).astype(BF16)


def stacked(x):
    high, low = pieces(x)
    return jnp.concatenate([high, low], axis=0)


def folded(product):
    half = product.shape[0] // 2
    return product[:half] + product[half:]


def iota(shape, dim):
    return lax.broadcasted_iota(jnp.int32, shape, dim)


def cg_coefficients(moment):
    def inner(first, second):
        total = None
        for i, a in enumerate(first):
            for j, b in enumerate(second):
                term = a * b * moment[i + j]
                total = term if total is None else total + term
        return total

    one = jnp.ones_like(moment[0])
    residual, direction, solution = [one], [one], []
    norm = moment[0]
    for step in range(ITERS):
        image = [CENTRE * d for d in direction] + [0.0 * one]
        for i, d in enumerate(direction):
            image[i + 1] = image[i + 1] + d
        alpha = norm / inner(direction, image)
        solution = [
            (solution[i] if i < len(solution) else 0.0) + alpha * d
            for i, d in enumerate(direction)
        ]
        residual = [
            (residual[i] if i < len(residual) else 0.0) - alpha * d for i, d in enumerate(image)
        ]
        if step + 1 < ITERS:
            new = inner(residual, residual)
            ratio = new / norm
            norm = new
            direction = [
                r + (ratio * direction[i] if i < len(direction) else 0.0)
                for i, r in enumerate(residual)
            ]
    return solution, residual


def kernel(
    sizes, groups,
    load_v, load_w, shift_h, diag_h, off_h, coupling_h, kind_h, cell_h, node_h,
    vu, wu, coefs,
    w_first, shift, diag, off, coupling, kind, cell, node, load_s,
    weights, win, stiff, lanes, lanes_t, rows, rows_b, nodes_mine, nodes_recv, nodes_t,
    centre_diag, node_in, kind_in, coup_in,
    x_in, y_in, z_in, w_in, p_in, s_in, y_out, z_out, p_out, s_out, red, red_out,
    node_s, node_r, kind_s, kind_r, coup_s, coup_r,
    x_s, x_r, y_s, y_r, z_s, z_r, w_s, w_r, p_s, p_r, s_s, s_r, red_s, red_r,
):
    n_gx, n_gy, n_ea = sizes
    comps, dx, dy, dz = load_v.shape
    ecomp, enb = load_w.shape
    epad = wu.shape[1]
    cap = node.shape[2]
    per = dx * dy
    allrows = comps * per
    groups8 = allrows // 8
    edge_rows = comps * dx
    gi, gj, ek = (lax.axis_index(a) for a in AXES)
    own = {"gx": gi, "gy": gj, "ea": ek}
    count = dict(zip(AXES, sizes))

    def members(group):
        total = 1
        for a in group:
            total *= count[a]
        me = 0
        for a in group:
            me = me * count[a] + own[a]

        def target(d):
            flat = lax.rem(me + d, total)
            coords = dict(own)
            for a in reversed(group):
                coords[a] = lax.rem(flat, count[a])
                flat = lax.div(flat, count[a])
            return tuple(coords[a] for a in AXES)

        return total, me, target

    has = {
        ("gx", 1): gi < n_gx - 1, ("gx", -1): gi > 0,
        ("gy", 1): gj < n_gy - 1, ("gy", -1): gj > 0,
        ("ea", 1): ek < n_ea - 1, ("ea", -1): ek > 0,
    }
    beside = {
        ("gx", s): (gi + s, gj, ek) for s in (1, -1)
    } | {("gy", s): (gi, gj + s, ek) for s in (1, -1)} | {
        ("ea", s): (gi, gj, ek + s) for s in (1, -1)
    }
    slot = {1: 0, -1: 1}

    barrier = pltpu.get_barrier_semaphore()
    wide = n_gx - 1 > ITERS
    expected = 0
    for group in groups if wide else (("gy", "ea"),):
        total, _, target = members(group)
        for d in range(1, total):
            pl.semaphore_signal(barrier, inc=1, device_id=target(d), device_id_type=MESH)
        expected += total - 1
    if not wide:
        for s in (1, -1):
            @pl.when(has["gx", s])
            def _():
                pl.semaphore_signal(
                    barrier, inc=1, device_id=beside["gx", s], device_id_type=MESH
                )
            expected = expected + jnp.where(has["gx", s], 1, 0)

    loads = {}
    for at, (name, src, dst) in enumerate((
        ("cell", cell_h, cell), ("v", load_v, vu.at[0]), ("w", load_w, w_first),
        ("node", node_h, node), ("kind", kind_h, kind), ("coupling", coupling_h, coupling),
        ("shift", shift_h, shift), ("off", off_h, off), ("diag", diag_h, diag),
    )):
        loads[name] = pltpu.make_async_copy(src, dst, load_s.at[at])
        loads[name].start()

    for s in (1, -1):
        for name, buffer in (("gx", x_in), ("gy", y_in), ("ea", z_in)):
            @pl.when(jnp.logical_not(has[name, -s]))
            def _():
                for op in range(ITERS):
                    buffer[op, slot[s]] = jnp.zeros(buffer.shape[2:], F32)

    def partner(d):
        return lax.rem(ek + d, n_ea)

    def remote(src, dst, s_sem, r_sem, device):
        return pltpu.make_async_remote_copy(
            src_ref=src, dst_ref=dst, send_sem=s_sem, recv_sem=r_sem,
            device_id=device, device_id_type=MESH,
        )

    def x_copy(op, s):
        return remote(
            vu.at[op, :, dx - 1 if s == 1 else 0], x_in.at[op, slot[s]],
            x_s.at[op, slot[s]], x_r.at[op, slot[s]], beside["gx", s],
        )

    def y_copy(op, s):
        return remote(
            y_out.at[op, slot[s]], y_in.at[op, slot[s]],
            y_s.at[op, slot[s]], y_r.at[op, slot[s]], beside["gy", s],
        )

    def z_copy(op, s):
        return remote(
            z_out.at[op, slot[s]], z_in.at[op, slot[s]],
            z_s.at[op, slot[s]], z_r.at[op, slot[s]], beside["ea", s],
        )

    def column_copy(src, dst, s_sem, r_sem, d):
        return remote(src, dst.at[ek], s_sem.at[d], r_sem.at[d], (gi, gj, partner(d)))

    def w_copy(d):
        return column_copy(wu.at[0], w_in, w_s, w_r, d)

    def p_copy(op, d):
        return column_copy(
            p_out.at[op, partner(d)], p_in.at[op], p_s.at[op], p_r.at[op], d
        )

    def s_copy(op, d):
        return column_copy(
            s_out.at[op, partner(d)], s_in.at[op], s_s.at[op], s_r.at[op], d
        )

    def block(d):
        return pl.ds(pl.multiple_of(partner(d) * cap, cap), cap)

    def table_copies(d):
        return (
            column_copy(node, node_in, node_s, node_r, d),
            column_copy(kind, kind_in, kind_s, kind_r, d),
            column_copy(coupling.at[:, :, block(d)], coup_in, coup_s, coup_r, d),
        )

    lane_i = iota((8, dz), 1)
    lane_r = iota((1, dz), 1)
    row_i = iota((dy, dz), 0)
    lane_b = iota((dy, dz), 1)

    def columns(tile):
        full = jnp.concatenate(
            [tile.astype(F32), jnp.zeros((cap - tile.shape[0], cap), F32)], axis=0
        )
        return jnp.transpose(full).astype(jnp.int32)

    def slabs(o):
        return slice(o * cap, (o + 1) * cap)

    def halo_pack(op):
        v2 = vu[op].reshape(allrows, dz)
        for i in range(comps):
            for a in range(dx):
                at = i * dx + a
                y_out[op, 0, at : at + 1, :] = vu[op, i, a, dy - 1 : dy, :]
                y_out[op, 1, at : at + 1, :] = vu[op, i, a, 0:1, :]
        up = jnp.zeros((8, dz), F32)
        down = jnp.zeros((8, dz), F32)
        for g in range(groups8):
            part = v2[8 * g : 8 * g + 8]
            up = jnp.where(lane_i == g, part[:, dz - 1 : dz], up)
            down = jnp.where(lane_i == g, part[:, 0:1], down)
        z_out[op, 0] = up
        z_out[op, 1] = down

    def halo_send(op):
        for s in (1, -1):
            for name, copy in (("gx", x_copy), ("gy", y_copy), ("ea", z_copy)):
                @pl.when(has[name, s])
                def _():
                    copy(op, s).start()

    def halo_wait(op):
        for s in (1, -1):
            for name, copy in (("gx", x_copy), ("gy", y_copy), ("ea", z_copy)):
                @pl.when(has[name, -s])
                def _():
                    copy(op, s).wait_recv()

    def pick(op):
        v2 = vu[op].reshape(allrows, dz)
        seen = folded(jnp.dot(stacked(v2), lanes[...], preferred_element_type=F32))
        for i in range(comps):
            picked = jnp.sum(seen[i * per : (i + 1) * per] * rows[...], axis=0, keepdims=True)
            for o in range(n_ea):
                p_out[op, o, i : i + 1, :] = picked[:, slabs(o)]

    def pick_send(op):
        for d in range(1, n_ea):
            p_copy(op, d).start()

    def local(op):
        v4 = vu[op]
        v2 = v4.reshape(allrows, dz)
        zero = jnp.zeros((comps, 1, dy, dz), F32)
        near = jnp.concatenate([zero, v4[:, : dx - 1]], axis=1) + jnp.concatenate(
            [v4[:, 1:], zero], axis=1
        )
        near = near.reshape(allrows, dz)
        lane_all = iota((allrows, dz), 1)
        row_all = lax.rem(iota((allrows, dz), 0), dy)
        near = near + jnp.where(lane_all == 0, 0.0, pltpu.roll(v2, 1, 1))
        near = near + jnp.where(lane_all == dz - 1, 0.0, pltpu.roll(v2, dz - 1, 1))
        near = near + jnp.where(row_all == 0, 0.0, pltpu.roll(v2, 1, 0))
        near = near + jnp.where(row_all == dy - 1, 0.0, pltpu.roll(v2, allrows - 1, 0))
        vu[op + 1] = centre_diag[...][None] * v4 - near.reshape(v4.shape)

    def local_nodes(op):
        w = wu[op]
        acc = stiff[0] * w[0:1]
        for p in range(1, ecomp):
            acc = acc + stiff[p] * w[p : p + 1]
        wu[op + 1] = acc

    def product(op_a, op_b):
        pv = jnp.sum((vu[op_a] * vu[op_b]).reshape(groups8, 8, dz), axis=0)
        pw = jnp.sum(wu[op_a] * wu[op_b], axis=0, keepdims=True)
        total = jnp.sum(pv, axis=0, keepdims=True)
        for b in range(enb // dz):
            total = total + pw[:, b * dz : (b + 1) * dz]
        return total

    def nodes_step(op):
        p_in[op, ek] = p_out[op, ek]
        for d in range(1, n_ea):
            p_copy(op, d).wait_recv()
        terms = []
        for o in range(n_ea):
            total = None
            for i in range(comps):
                term = win[o, i] * p_in[op, o, i : i + 1, :]
                total = term if total is None else total + term
            terms.append(total)
        wu[op + 1] += folded(
            jnp.dot(
                stacked(jnp.concatenate(terms, axis=1)), nodes_recv[...],
                preferred_element_type=F32,
            )
        )

    def sums_send(op):
        values = folded(jnp.dot(stacked(wu[op]), nodes_t[...], preferred_element_type=F32))
        for o in range(n_ea):
            for i in range(comps):
                s_out[op, o, i : i + 1, :] = jnp.sum(
                    win[o, i] * values[:, slabs(o)], axis=0, keepdims=True
                )
        for d in range(1, n_ea):
            s_copy(op, d).start()

    def first_sums():
        w_in[ek] = wu[0]
        for d in range(1, n_ea):
            w_copy(d).wait_recv()
        for o in range(n_ea):
            values = folded(jnp.dot(stacked(w_in[o]), nodes_mine[o], preferred_element_type=F32))
            for i in range(comps):
                s_in[0, o, i : i + 1, :] = jnp.sum(
                    weights[o, i] * values, axis=0, keepdims=True
                )

    def sums_wait(op):
        s_in[op, ek] = s_out[op, ek]
        for d in range(1, n_ea):
            s_copy(op, d).wait_recv()

    def cells_step(op):
        spread_h, spread_l = [], []
        for i in range(comps):
            line = jnp.concatenate([s_in[op, o, i : i + 1, :] for o in range(n_ea)], axis=1)
            h, l = pieces(line)
            spread_h.append(rows_b[...] * h)
            spread_l.append(rows_b[...] * l)
        added = folded(
            jnp.dot(
                jnp.concatenate(spread_h + spread_l, axis=0), lanes_t[...],
                preferred_element_type=F32,
            )
        )
        z_low, z_high = z_in[op, 0], z_in[op, 1]
        for i in range(comps):
            for a in range(dx):
                at = i * dx + a
                low = jnp.where(row_i == 0, y_in[op, 0, at : at + 1, :], 0.0)
                high = jnp.where(row_i == dy - 1, y_in[op, 1, at : at + 1, :], 0.0)
                side = low + high
                z_l, z_h = [], []
                for b in range(dy // 8):
                    g = at * (dy // 8) + b
                    z_l.append(jnp.broadcast_to(z_low[:, g : g + 1], (8, dz)))
                    z_h.append(jnp.broadcast_to(z_high[:, g : g + 1], (8, dz)))
                side = side + jnp.where(lane_b == 0, jnp.concatenate(z_l, axis=0), 0.0)
                side = side + jnp.where(lane_b == dz - 1, jnp.concatenate(z_h, axis=0), 0.0)
                if a == 0:
                    side = side + x_in[op, 0, i]
                if a == dx - 1:
                    side = side + x_in[op, 1, i]
                vu[op + 1, i, a] += added[at * dy : (at + 1) * dy] - side

    def last_moment(op, row):
        x_low = x_in[op, 0] * vu[op, :, 0]
        x_high = x_in[op, 1] * vu[op, :, dx - 1]
        side = jnp.sum((x_low + x_high).reshape(comps * dy, dz), axis=0, keepdims=True)
        y = y_out[op, 1, :edge_rows] * y_in[op, 0, :edge_rows]
        y = y + y_out[op, 0, :edge_rows] * y_in[op, 1, :edge_rows]
        side = side + jnp.sum(y, axis=0, keepdims=True)
        z = z_out[op, 1] * z_in[op, 0] + z_out[op, 0] * z_in[op, 1]
        side = side + jnp.sum(z, axis=0, keepdims=True)
        cross = None
        for o in range(n_ea):
            term = p_out[op, o] * s_in[op, o]
            cross = term if cross is None else cross + term
        cross = jnp.sum(cross, axis=0, keepdims=True)
        return row - side + 2.0 * cross

    loads["cell"].wait()
    tile = cell[0]
    tile_row = lax.div(tile, dz)
    tile_lane = tile - tile_row * dz
    for o in range(n_ea):
        lanes[:, slabs(o)] = jnp.where(
            iota((dz, cap), 0) == tile_lane[o : o + 1], 1.0, 0.0
        ).astype(BF16)
        r = jnp.where(iota((per, cap), 0) == tile_row[o : o + 1], 1.0, 0.0)
        rows[:, slabs(o)] = r
        rows_b[:, slabs(o)] = r.astype(BF16)
    loads["v"].wait()
    halo_pack(0)
    pick(0)
    loads["w"].wait()
    wu[0] = jnp.concatenate([w_first[...], jnp.zeros((epad - ecomp, enb), F32)], axis=0)
    for name in ("node", "kind", "coupling"):
        loads[name].wait()

    pl.semaphore_wait(barrier, expected)

    for d in range(1, n_ea):
        w_copy(d).start()
    halo_send(0)
    pick_send(0)
    for d in range(1, n_ea):
        for copy in table_copies(d):
            copy.start()

    lane_columns = columns(tile_lane)
    for o in range(n_ea):
        lanes_t[slabs(o), :] = jnp.where(
            iota((cap, dz), 1) == lane_columns[:, o : o + 1], 1.0, 0.0
        ).astype(BF16)
        nodes_mine[o] = jnp.where(
            iota((enb, cap), 0) == node[0, o : o + 1, :], 1.0, 0.0
        ).astype(BF16)
    no_row = jnp.zeros((epad - ecomp, cap), F32)

    def masked(raw, k):
        heavi = jnp.where(k >= 1, 1.0, 0.0)
        tip = jnp.where(k == 2, 1.0, 0.0)
        mask = jnp.where(iota((ecomp, cap), 0) < 3, heavi, tip)
        return jnp.concatenate([raw * mask, no_row], axis=0)

    for o in range(n_ea):
        for i in range(comps):
            weights[o, i] = masked(coupling[i, :, slabs(o)], kind[0, o : o + 1, :])
    loads["off"].wait()
    loads["diag"].wait()
    for p in range(ecomp):
        whole = 0.5 * (off[p] + off[:, p, :])
        whole = jnp.where(iota((ecomp, enb), 0) == p, diag[p : p + 1, :] - CENTRE, whole)
        stiff[p] = jnp.concatenate([whole, jnp.zeros((epad - ecomp, enb), F32)], axis=0)
    loads["shift"].wait()
    centre_diag[...] = shift[...] + (6.0 - CENTRE)
    node_in[ek] = node[...]
    kind_in[ek] = kind[...]
    coup_in[ek] = coupling[:, :, block(0)]
    local(0)
    local_nodes(0)
    moments = [product(0, 0)]

    first_sums()
    halo_wait(0)
    cells_step(0)
    halo_pack(1)
    halo_send(1)
    pick(1)
    pick_send(1)

    for d in range(1, n_ea):
        for copy in table_copies(d):
            copy.wait_recv()
    own_rows = jnp.concatenate(
        [node_in[o, 0, pl.ds(ek, 1), :] for o in range(n_ea)], axis=0
    )
    node_columns = columns(own_rows)
    for o in range(n_ea):
        nodes_recv[slabs(o), :] = jnp.where(
            iota((cap, enb), 1) == node_columns[:, o : o + 1], 1.0, 0.0
        ).astype(BF16)
        nodes_t[:, slabs(o)] = jnp.where(
            iota((enb, cap), 0) == own_rows[o : o + 1, :], 1.0, 0.0
        ).astype(BF16)
        for i in range(comps):
            win[o, i] = masked(coup_in[o, i], kind_in[o, 0, pl.ds(ek, 1), :])
    nodes_step(0)
    sums_send(1)
    last = ITERS - 1
    for op in range(1, last):
        moments.append(product(op - 1, op))
        moments.append(product(op, op))
        local(op)
        local_nodes(op)
        nodes_step(op)
        sums_send(op + 1)
        halo_wait(op)
        sums_wait(op)
        cells_step(op)
        halo_pack(op + 1)
        halo_send(op + 1)
        pick(op + 1)
        pick_send(op + 1)

    moments.append(product(last - 1, last))
    moments.append(product(last, last))
    local(last)
    local_nodes(last)
    row = product(last, last + 1)
    packed = jnp.zeros((1, dz), F32)
    for n, m in enumerate(moments):
        packed = jnp.where(lane_r == n, jnp.sum(m, axis=1, keepdims=True), packed)
    halo_wait(last)
    sums_wait(last)
    row = last_moment(last, row)
    at = 2 * ITERS - 1
    packed = jnp.where(lane_r == at, jnp.sum(row, axis=1, keepdims=True), packed)

    def red_copy(stage, me, target, d):
        return remote(
            red_out.at[stage], red.at[stage, me], red_s.at[stage, d], red_r.at[stage, d],
            target(d),
        )

    for stage, group in enumerate(groups):
        total, me, target = members(group)
        red_out[stage] = packed
        for d in range(1, total):
            red_copy(stage, me, target, d).start()
        red[stage, me] = packed
        if stage == 0:
            cells_step(last)
            nodes_step(last)
            for op in range(ITERS):
                for s in (1, -1):
                    for name, copy in (("gx", x_copy), ("gy", y_copy), ("ea", z_copy)):
                        @pl.when(has[name, s])
                        def _():
                            copy(op, s).wait_send()
                for d in range(1, n_ea):
                    p_copy(op, d).wait_send()
                    if op > 0:
                        s_copy(op, d).wait_send()
            for d in range(1, n_ea):
                w_copy(d).wait_send()
                for copy in table_copies(d):
                    copy.wait_send()
        for d in range(1, total):
            red_copy(stage, me, target, d).wait_send()
        for d in range(1, total):
            red_copy(stage, me, target, d).wait_recv()
        packed = jnp.sum(red[stage, :total], axis=0)

    sol, res = cg_coefficients([packed[:, n : n + 1] for n in range(2 * ITERS)])
    tile = jnp.zeros((1, dz), F32)
    for n, c in enumerate(sol + res):
        tile = jnp.where(lane_r == n, c, tile)
    coefs[...] = tile


def combine_kernel(vu, wu, coefs, sol_v, res_v, sol_w, res_w):
    ecomp = sol_w.shape[0]
    tile = coefs[...]
    solution = [tile[:, n : n + 1] for n in range(ITERS)]
    residual = [tile[:, ITERS + n : ITERS + n + 1] for n in range(ITERS + 1)]

    def combine(factors, terms):
        out = factors[0] * terms[0]
        for f, t in zip(factors[1:], terms[1:]):
            out = out + f * t
        return out

    shape = sol_v.shape
    flat = (shape[0] * shape[1] * shape[2], shape[3])
    v_terms = [vu[n].reshape(flat) for n in range(ITERS + 1)]
    w_terms = [wu[n] for n in range(ITERS + 1)]
    sol_v[...] = combine(solution, v_terms).reshape(shape)
    res_v[...] = combine(residual, v_terms).reshape(shape)
    sol_w[...] = combine(solution, w_terms)[:ecomp]
    res_w[...] = combine(residual, w_terms)[:ecomp]


def body(sizes, *args):
    load_v, load_w, shift, diag, off, coupling, kind, cell, node = args
    n_ea = sizes[2]
    total = sizes[0] * sizes[1] * sizes[2]
    groups = (AXES,) if total <= 64 else (("gx",), ("gy", "ea"))
    widest = total if total <= 64 else max(sizes[0], sizes[1] * sizes[2])
    comps, dx, dy, dz = load_v.shape
    ecomp, enb = load_w.shape
    cap = node.shape[2]
    vmem = pltpu.VMEM
    dma = pltpu.SemaphoreType.DMA
    y_rows = -(-comps * dx // 8) * 8
    epad = -(-ecomp // 16) * 16
    slots = n_ea * cap
    scratch = [
        vmem(load_w.shape, F32), vmem(shift.shape, F32), vmem(diag.shape, F32),
        vmem(off.shape, F32), vmem(coupling.shape, F32),
        vmem(kind.shape, jnp.int32), vmem(cell.shape, jnp.int32), vmem(node.shape, jnp.int32),
        dma((9,)),
        vmem((n_ea, comps, epad, cap), F32),
        vmem((n_ea, comps, epad, cap), F32),
        vmem((ecomp, epad, enb), F32),
        vmem((dz, slots), BF16),
        vmem((slots, dz), BF16),
        vmem((dx * dy, slots), F32),
        vmem((dx * dy, slots), BF16),
        vmem((n_ea, enb, cap), BF16),
        vmem((slots, enb), BF16),
        vmem((enb, slots), BF16),
        vmem((dx, dy, dz), F32),
        vmem((n_ea,) + node.shape, jnp.int32),
        vmem((n_ea,) + kind.shape, jnp.int32),
        vmem((n_ea, comps, ecomp, cap), F32),
        vmem((ITERS, 2, comps, dy, dz), F32),
        vmem((ITERS, 2, y_rows, dz), F32),
        vmem((ITERS, 2, 8, dz), F32),
        vmem((n_ea, epad, enb), F32),
        vmem((ITERS, n_ea, comps, cap), F32),
        vmem((ITERS, n_ea, comps, cap), F32),
        vmem((ITERS, 2, y_rows, dz), F32),
        vmem((ITERS, 2, 8, dz), F32),
        vmem((ITERS, n_ea, comps, cap), F32),
        vmem((ITERS, n_ea, comps, cap), F32),
        vmem((len(groups), widest, 1, dz), F32),
        vmem((len(groups), 1, dz), F32),
        dma((n_ea,)), dma((n_ea,)),
        dma((n_ea,)), dma((n_ea,)),
        dma((n_ea,)), dma((n_ea,)),
        dma((ITERS, 2)), dma((ITERS, 2)),
        dma((ITERS, 2)), dma((ITERS, 2)),
        dma((ITERS, 2)), dma((ITERS, 2)),
        dma((n_ea,)), dma((n_ea,)),
        dma((ITERS, n_ea)), dma((ITERS, n_ea)),
        dma((ITERS, n_ea)), dma((ITERS, n_ea)),
        dma((len(groups), widest)), dma((len(groups), widest)),
    ]
    basis = pl.pallas_call(
        functools.partial(kernel, sizes, groups),
        out_shape=(
            pltpu.VMEM((ITERS + 1,) + load_v.shape, F32),
            pltpu.VMEM((ITERS + 1, epad, enb), F32),
            pltpu.VMEM((1, dz), F32),
        ),
        in_specs=[pl.BlockSpec(memory_space=pltpu.HBM)] * 9,
        out_specs=[pl.BlockSpec(memory_space=vmem)] * 3,
        scratch_shapes=scratch,
        compiler_params=pltpu.CompilerParams(
            collective_id=0, has_side_effects=True
        ),
        name="krylov",
    )(*args)
    return tuple(
        pl.pallas_call(
            combine_kernel,
            out_shape=tuple(
                jax.ShapeDtypeStruct(like.shape, F32)
                for like in (load_v, load_v, load_w, load_w)
            ),
            in_specs=[pl.BlockSpec(memory_space=vmem)] * 3,
            out_specs=[pl.BlockSpec(memory_space=vmem)] * 4,
            compiler_params=pltpu.CompilerParams(vmem_limit_bytes=8 << 20),
            name="combine",
        )(*basis)
    )


def solution(mesh):
    column = ("gx", "gy", "ea")
    placed = (
        P(None, "gx", "gy", "ea"),
        P(None, column),
        P("gx", "gy", "ea"),
        P(None, column),
        P(None, None, column),
        P(None, None, column),
        P(column, None, None),
        P(column, None, None),
        P(column, None, None),
    )
    return jax.shard_map(
        functools.partial(body, tuple(mesh.shape[a] for a in AXES)),
        mesh=mesh,
        in_specs=placed,
        out_specs=(
            P(None, "gx", "gy", "ea"),
            P(None, "gx", "gy", "ea"),
            P(None, column),
            P(None, column),
        ),
        check_vma=False,
    )
```

```python
import functools

import jax
import jax.numpy as jnp
from jax import lax
from jax.experimental import pallas as pl
from jax.experimental.pallas import tpu as pltpu
from jax.sharding import PartitionSpec as P

ITERS = 3
CENTRE = 11.5
AXES = ("gx", "gy", "ea")
MESH = pl.DeviceIdType.MESH
F32 = jnp.float32
BF16 = jnp.bfloat16


def pieces(x):
    high = x.astype(BF16)
    return high, (x - high.astype(F32)).astype(BF16)


def stacked(x):
    high, low = pieces(x)
    return jnp.concatenate([high, low], axis=0)


def folded(product):
    half = product.shape[0] // 2
    return product[:half] + product[half:]


def iota(shape, dim):
    return lax.broadcasted_iota(jnp.int32, shape, dim)


def cg_coefficients(moment):
    def inner(first, second):
        total = None
        for i, a in enumerate(first):
            for j, b in enumerate(second):
                term = a * b * moment[i + j]
                total = term if total is None else total + term
        return total

    one = jnp.ones_like(moment[0])
    residual, direction, solution = [one], [one], []
    norm = moment[0]
    for step in range(ITERS):
        image = [CENTRE * d for d in direction] + [0.0 * one]
        for i, d in enumerate(direction):
            image[i + 1] = image[i + 1] + d
        alpha = norm / inner(direction, image)
        solution = [
            (solution[i] if i < len(solution) else 0.0) + alpha * d
            for i, d in enumerate(direction)
        ]
        residual = [
            (residual[i] if i < len(residual) else 0.0) - alpha * d for i, d in enumerate(image)
        ]
        if step + 1 < ITERS:
            new = inner(residual, residual)
            ratio = new / norm
            norm = new
            direction = [
                r + (ratio * direction[i] if i < len(direction) else 0.0)
                for i, r in enumerate(residual)
            ]
    return solution, residual


def kernel(
    sizes, groups,
    load_v, load_w, shift_h, diag_h, off_h, coupling_h, kind_h, cell_h, node_h,
    vu, wu, coefs,
    w_first, shift, diag, off, coupling, cell, ids, load_s,
    weights, win, stiff, lanes, lanes_t, rows, rows_b, nodes_mine, nodes_recv, nodes_t,
    centre_diag, ids_in, coup_in,
    x_in, y_in, z_in, w_in, p_in, s_in, z_out, p_out, s_out, red, red_out,
    ids_s, ids_r, coup_s, coup_r,
    x_s, x_r, y_s, y_r, z_s, z_r, w_s, w_r, p_s, p_r, s_s, s_r, red_s, red_r,
):
    n_gx, n_gy, n_ea = sizes
    comps, dx, dy, dz = load_v.shape
    ecomp, enb = load_w.shape
    epad = wu.shape[1]
    cap = cell.shape[2]
    per = dx * dy
    allrows = comps * per
    groups8 = allrows // 8
    gi, gj, ek = (lax.axis_index(a) for a in AXES)
    own = {"gx": gi, "gy": gj, "ea": ek}
    count = dict(zip(AXES, sizes))

    def members(group):
        total = 1
        for a in group:
            total *= count[a]
        me = 0
        for a in group:
            me = me * count[a] + own[a]

        def target(d):
            flat = lax.rem(me + d, total)
            coords = dict(own)
            for a in reversed(group):
                coords[a] = lax.rem(flat, count[a])
                flat = lax.div(flat, count[a])
            return tuple(coords[a] for a in AXES)

        return total, me, target

    has = {
        ("gx", 1): gi < n_gx - 1, ("gx", -1): gi > 0,
        ("gy", 1): gj < n_gy - 1, ("gy", -1): gj > 0,
        ("ea", 1): ek < n_ea - 1, ("ea", -1): ek > 0,
    }
    beside = {
        ("gx", s): (gi + s, gj, ek) for s in (1, -1)
    } | {("gy", s): (gi, gj + s, ek) for s in (1, -1)} | {
        ("ea", s): (gi, gj, ek + s) for s in (1, -1)
    }
    slot = {1: 0, -1: 1}

    barrier = pltpu.get_barrier_semaphore()
    wide = n_gx - 1 > ITERS
    expected = 0
    for group in groups if wide else (("gy", "ea"),):
        total, _, target = members(group)
        for d in range(1, total):
            pl.semaphore_signal(barrier, inc=1, device_id=target(d), device_id_type=MESH)
        expected += total - 1
    if not wide:
        for s in (1, -1):
            @pl.when(has["gx", s])
            def _():
                pl.semaphore_signal(
                    barrier, inc=1, device_id=beside["gx", s], device_id_type=MESH
                )
            expected = expected + jnp.where(has["gx", s], 1, 0)

    loads = {}
    for at, (name, src, dst) in enumerate((
        ("w", load_w, w_first), ("node", node_h, ids.at[0]), ("kind", kind_h, ids.at[1]),
        ("v", load_v, vu.at[0]), ("cell", cell_h, cell), ("coupling", coupling_h, coupling),
        ("shift", shift_h, shift), ("off", off_h, off), ("diag", diag_h, diag),
    )):
        at = 1 if name == "kind" else at
        loads[name] = pltpu.make_async_copy(src, dst, load_s.at[at])
        loads[name].start()

    for s in (1, -1):
        for name, buffer in (("gx", x_in), ("gy", y_in), ("ea", z_in)):
            @pl.when(jnp.logical_not(has[name, -s]))
            def _():
                for op in range(ITERS):
                    buffer[op, slot[s]] = jnp.zeros(buffer.shape[2:], F32)

    def partner(d):
        return lax.rem(ek + d, n_ea)

    def remote(src, dst, s_sem, r_sem, device):
        return pltpu.make_async_remote_copy(
            src_ref=src, dst_ref=dst, send_sem=s_sem, recv_sem=r_sem,
            device_id=device, device_id_type=MESH,
        )

    sides = {
        name: jnp.where(has[name, 1], 1, 0) + jnp.where(has[name, -1], 1, 0) for name in AXES
    }

    def landed(ref, sem):
        pltpu.make_async_copy(ref, ref, sem).wait()

    def x_copy(op, s):
        return remote(
            vu.at[op, :, dx - 1 if s == 1 else 0], x_in.at[op, slot[s]],
            x_s.at[0], x_r.at[op], beside["gx", s],
        )

    def y_copy(op, s):
        edge = dy - 1 if s == 1 else 0
        return remote(
            vu.at[op, :, :, edge : edge + 1, :], y_in.at[op, slot[s]],
            y_s.at[0], y_r.at[op], beside["gy", s],
        )

    def z_copy(op, s):
        return remote(
            z_out.at[op, slot[s]], z_in.at[op, slot[s]],
            z_s.at[0], z_r.at[op], beside["ea", s],
        )

    def column_copy(src, dst, s_sem, r_sem, d):
        return remote(src, dst.at[ek], s_sem, r_sem, (gi, gj, partner(d)))

    def w_copy(d):
        return column_copy(wu.at[0], w_in, w_s.at[0], w_r.at[0], d)

    def p_copy(op, d):
        return column_copy(
            p_out.at[op, partner(d)], p_in.at[op], p_s.at[0], p_r.at[op], d
        )

    def s_copy(op, d):
        return column_copy(
            s_out.at[op, partner(d)], s_in.at[op], s_s.at[0], s_r.at[op], d
        )

    def ids_copy(d):
        return column_copy(
            ids.at[:, 0, pl.ds(partner(d), 1), :], ids_in, ids_s.at[0], ids_r.at[0], d
        )

    def block(d):
        return pl.ds(pl.multiple_of(partner(d) * cap, cap), cap)

    def coup_copy(d):
        return column_copy(
            coupling.at[:, :, block(d)], coup_in, coup_s.at[0], coup_r.at[0], d
        )

    def column_send(copy):
        for d in range(1, n_ea):
            copy(d).start()

    lane_i = iota((8, dz), 1)
    lane_r = iota((1, dz), 1)
    row_i = iota((dy, dz), 0)
    lane_b = iota((dy, dz), 1)

    def columns(tile):
        full = jnp.concatenate(
            [tile.astype(F32), jnp.zeros((cap - tile.shape[0], cap), F32)], axis=0
        )
        return jnp.transpose(full).astype(jnp.int32)

    def slabs(o):
        return slice(o * cap, (o + 1) * cap)

    def halo_send(op):
        for s in (1, -1):
            for name, copy in (("gx", x_copy), ("gy", y_copy)):
                @pl.when(has[name, s])
                def _():
                    copy(op, s).start()
        v2 = vu[op].reshape(allrows, dz)
        up = jnp.zeros((8, dz), F32)
        down = jnp.zeros((8, dz), F32)
        for g in range(groups8):
            part = v2[8 * g : 8 * g + 8]
            up = jnp.where(lane_i == g, part[:, dz - 1 : dz], up)
            down = jnp.where(lane_i == g, part[:, 0:1], down)
        z_out[op, 0] = up
        z_out[op, 1] = down
        for s in (1, -1):
            @pl.when(has["ea", s])
            def _():
                z_copy(op, s).start()

    def by_sides(name, two, one, sem):
        @pl.when(sides[name] == 2)
        def _():
            landed(two, sem)

        @pl.when(sides[name] == 1)
        def _():
            landed(one, sem)

    def halo_wait(op):
        for name, buffer, sem in (("gx", x_in, x_r), ("gy", y_in, y_r), ("ea", z_in, z_r)):
            by_sides(name, buffer.at[op], buffer.at[op, 0], sem.at[op])

    def pick(op):
        h, l = pieces(vu[op].reshape(allrows, dz))
        seen = jnp.dot(
            jnp.concatenate([h, l], axis=1), lanes[...], preferred_element_type=F32
        )
        return [
            jnp.sum(seen[i * per : (i + 1) * per] * rows[...], axis=0, keepdims=True)
            for i in range(comps)
        ]

    def pick_send(op, picked):
        for i in range(comps):
            for o in range(n_ea):
                line = picked[i][:, slabs(o)]
                if op > 0:
                    line = line + s_in[op - 1, o, i : i + 1, :]
                p_out[op, o, i : i + 1, :] = line
        column_send(functools.partial(p_copy, op))

    def local(op):
        v4 = vu[op]
        v2 = v4.reshape(allrows, dz)
        zero = jnp.zeros((comps, 1, dy, dz), F32)
        near = jnp.concatenate([zero, v4[:, : dx - 1]], axis=1) + jnp.concatenate(
            [v4[:, 1:], zero], axis=1
        )
        near = near.reshape(allrows, dz)
        lane_all = iota((allrows, dz), 1)
        row_all = lax.rem(iota((allrows, dz), 0), dy)
        near = near + jnp.where(lane_all == 0, 0.0, pltpu.roll(v2, 1, 1))
        near = near + jnp.where(lane_all == dz - 1, 0.0, pltpu.roll(v2, dz - 1, 1))
        near = near + jnp.where(row_all == 0, 0.0, pltpu.roll(v2, 1, 0))
        near = near + jnp.where(row_all == dy - 1, 0.0, pltpu.roll(v2, allrows - 1, 0))
        vu[op + 1] = centre_diag[...][None] * v4 - near.reshape(v4.shape)

    def local_nodes(op):
        w = wu[op]
        acc = stiff[0] * w[0:1]
        for p in range(1, ecomp):
            acc = acc + stiff[p] * w[p : p + 1]
        wu[op + 1] = acc

    def product(op_a, op_b):
        pv = jnp.sum((vu[op_a] * vu[op_b]).reshape(groups8, 8, dz), axis=0)
        pw = jnp.sum(wu[op_a] * wu[op_b], axis=0, keepdims=True)
        total = jnp.sum(pv, axis=0, keepdims=True)
        for b in range(enb // dz):
            total = total + pw[:, b * dz : (b + 1) * dz]
        return total

    def nodes_step(op):
        p_in[op, ek] = p_out[op, ek]
        landed(p_in.at[op, : n_ea - 1], p_r.at[op])
        terms = []
        for o in range(n_ea):
            total = None
            for i in range(comps):
                term = win[o, i] * p_in[op, o, i : i + 1, :]
                total = term if total is None else total + term
            terms.append(total)
        wu[op + 1] += folded(
            jnp.dot(
                stacked(jnp.concatenate(terms, axis=1)), nodes_recv[...],
                preferred_element_type=F32,
            )
        )

    def sums_send(op):
        values = folded(jnp.dot(stacked(wu[op]), nodes_t[...], preferred_element_type=F32))
        for o in range(n_ea):
            for i in range(comps):
                s_out[op, o, i : i + 1, :] = jnp.sum(
                    win[o, i] * values[:, slabs(o)], axis=0, keepdims=True
                )
        column_send(functools.partial(s_copy, op))

    def first_sums():
        w_in[ek] = wu[0]
        landed(w_in.at[: n_ea - 1], w_r.at[0])
        for o in range(n_ea):
            values = folded(jnp.dot(stacked(w_in[o]), nodes_mine[o], preferred_element_type=F32))
            for i in range(comps):
                s_in[0, o, i : i + 1, :] = jnp.sum(
                    weights[o, i] * values, axis=0, keepdims=True
                )

    def sums_wait(op):
        s_in[op, ek] = s_out[op, ek]
        landed(s_in.at[op, : n_ea - 1], s_r.at[op])

    def halo_apply(op):
        z_low, z_high = z_in[op, 0], z_in[op, 1]
        for i in range(comps):
            for a in range(dx):
                at = i * dx + a
                side = jnp.where(row_i == 0, y_in[op, 0, i, a], 0.0)
                side = side + jnp.where(row_i == dy - 1, y_in[op, 1, i, a], 0.0)
                z_l, z_h = [], []
                for b in range(dy // 8):
                    g = at * (dy // 8) + b
                    z_l.append(jnp.broadcast_to(z_low[:, g : g + 1], (8, dz)))
                    z_h.append(jnp.broadcast_to(z_high[:, g : g + 1], (8, dz)))
                side = side + jnp.where(lane_b == 0, jnp.concatenate(z_l, axis=0), 0.0)
                side = side + jnp.where(lane_b == dz - 1, jnp.concatenate(z_h, axis=0), 0.0)
                if a == 0:
                    side = side + x_in[op, 0, i]
                if a == dx - 1:
                    side = side + x_in[op, 1, i]
                vu[op + 1, i, a] -= side

    def cells_step(op):
        spread_h, spread_l = [], []
        for i in range(comps):
            line = jnp.concatenate([s_in[op, o, i : i + 1, :] for o in range(n_ea)], axis=1)
            h, l = pieces(line)
            spread_h.append(rows_b[...] * h)
            spread_l.append(rows_b[...] * l)
        added = folded(
            jnp.dot(
                jnp.concatenate(spread_h + spread_l, axis=0), lanes_t[...],
                preferred_element_type=F32,
            )
        )
        vu[op + 1] += added.reshape(comps, dx, dy, dz)

    def last_moment(op, row):
        x_low = x_in[op, 0] * vu[op, :, 0]
        x_high = x_in[op, 1] * vu[op, :, dx - 1]
        side = jnp.sum((x_low + x_high).reshape(comps * dy, dz), axis=0, keepdims=True)
        y = y_in[op, 0] * vu[op, :, :, 0:1] + y_in[op, 1] * vu[op, :, :, dy - 1 : dy]
        side = side + jnp.sum(y.reshape(comps * dx, dz), axis=0, keepdims=True)
        z = z_out[op, 1] * z_in[op, 0] + z_out[op, 0] * z_in[op, 1]
        side = side + jnp.sum(z, axis=0, keepdims=True)
        cross = None
        for o in range(n_ea):
            term = p_out[op, o] * s_in[op, o]
            cross = term if cross is None else cross + term
        cross = jnp.sum(cross, axis=0, keepdims=True)
        return row - side + 2.0 * cross

    loads["w"].wait()
    wu[0] = jnp.concatenate([w_first[...], jnp.zeros((epad - ecomp, enb), F32)], axis=0)
    landed(ids, load_s.at[1])
    loads["v"].wait()

    pl.semaphore_wait(barrier, expected)

    column_send(ids_copy)
    column_send(w_copy)
    halo_send(0)
    loads["cell"].wait()
    tile = cell[0]
    tile_row = lax.div(tile, dz)
    tile_lane = tile - tile_row * dz
    for o in range(n_ea):
        hot = jnp.where(
            iota((dz, cap), 0) == tile_lane[o : o + 1], 1.0, 0.0
        ).astype(BF16)
        lanes[:dz, slabs(o)] = hot
        lanes[dz:, slabs(o)] = hot
        r = jnp.where(iota((per, cap), 0) == tile_row[o : o + 1], 1.0, 0.0)
        rows[:, slabs(o)] = r
        rows_b[:, slabs(o)] = r.astype(BF16)
    pick_send(0, pick(0))
    loads["coupling"].wait()
    column_send(coup_copy)

    lane_columns = columns(tile_lane)
    for o in range(n_ea):
        lanes_t[slabs(o), :] = jnp.where(
            iota((cap, dz), 1) == lane_columns[:, o : o + 1], 1.0, 0.0
        ).astype(BF16)
        nodes_mine[o] = jnp.where(
            iota((enb, cap), 0) == ids[0, 0, o : o + 1, :], 1.0, 0.0
        ).astype(BF16)
    no_row = jnp.zeros((epad - ecomp, cap), F32)

    def masked(raw, k):
        heavi = jnp.where(k >= 1, 1.0, 0.0)
        tip = jnp.where(k == 2, 1.0, 0.0)
        mask = jnp.where(iota((ecomp, cap), 0) < 3, heavi, tip)
        return jnp.concatenate([raw * mask, no_row], axis=0)

    for o in range(n_ea):
        for i in range(comps):
            weights[o, i] = masked(coupling[i, :, slabs(o)], ids[1, 0, o : o + 1, :])
    loads["shift"].wait()
    centre_diag[...] = shift[...] + (6.0 - CENTRE)
    local(0)
    loads["off"].wait()
    loads["diag"].wait()
    for p in range(ecomp):
        whole = 0.5 * (off[p] + off[:, p, :])
        whole = jnp.where(iota((ecomp, enb), 0) == p, diag[p : p + 1, :] - CENTRE, whole)
        stiff[p] = jnp.concatenate([whole, jnp.zeros((epad - ecomp, enb), F32)], axis=0)
    local_nodes(0)
    moments = [product(0, 0)]
    ids_in[ek] = ids[:, 0, pl.ds(ek, 1), :]
    coup_in[ek] = coupling[:, :, block(0)]
    landed(ids_in.at[: n_ea - 1], ids_r.at[0])
    own_rows = jnp.concatenate([ids_in[o, 0] for o in range(n_ea)], axis=0)
    node_columns = columns(own_rows)
    for o in range(n_ea):
        nodes_recv[slabs(o), :] = jnp.where(
            iota((cap, enb), 1) == node_columns[:, o : o + 1], 1.0, 0.0
        ).astype(BF16)
        nodes_t[:, slabs(o)] = jnp.where(
            iota((enb, cap), 0) == own_rows[o : o + 1, :], 1.0, 0.0
        ).astype(BF16)

    halo_wait(0)
    halo_apply(0)
    picked = pick(1)
    first_sums()
    pick_send(1, picked)
    cells_step(0)
    halo_send(1)
    landed(coup_in.at[: n_ea - 1], coup_r.at[0])
    for o in range(n_ea):
        for i in range(comps):
            win[o, i] = masked(coup_in[o, i], ids_in[o, 1])
    nodes_step(0)
    sums_send(1)
    last = ITERS - 1
    for op in range(1, last):
        local(op)
        local_nodes(op)
        moments.append(product(op - 1, op))
        moments.append(product(op, op))
        halo_wait(op)
        halo_apply(op)
        picked = pick(op + 1)
        sums_wait(op)
        pick_send(op + 1, picked)
        cells_step(op)
        halo_send(op + 1)
        nodes_step(op)
        sums_send(op + 1)

    local(last)
    local_nodes(last)
    moments.append(product(last - 1, last))
    moments.append(product(last, last))
    row = product(last, last + 1)
    packed = jnp.zeros((1, dz), F32)
    for n, m in enumerate(moments):
        packed = jnp.where(lane_r == n, jnp.sum(m, axis=1, keepdims=True), packed)
    halo_wait(last)
    sums_wait(last)
    row = last_moment(last, row)
    at = 2 * ITERS - 1
    packed = jnp.where(lane_r == at, jnp.sum(row, axis=1, keepdims=True), packed)

    for stage, group in enumerate(groups):
        total, me, target = members(group)
        whole = group == AXES
        red_out[stage] = packed
        for d in range(total - 1):
            dst = red.at[stage, me]
            ends = (red_s.at[stage], red_r.at[stage])
            if whole:
                pltpu.make_async_remote_copy(
                    src_ref=red_out.at[stage], dst_ref=dst, send_sem=ends[0], recv_sem=ends[1],
                    device_id=d + jnp.where(me <= d, 1, 0),
                    device_id_type=pl.DeviceIdType.LOGICAL,
                ).start()
            else:
                remote(red_out.at[stage], dst, *ends, target(d + 1)).start()
        red[stage, me] = packed
        if stage == 0:
            halo_apply(last)
            cells_step(last)
            nodes_step(last)
            for name, buffer, sem in (("gx", x_in, x_s), ("gy", y_in, y_s), ("ea", z_in, z_s)):
                by_sides(name, buffer, buffer.at[:, 0], sem.at[0])
            landed(p_in.at[:, : n_ea - 1], p_s.at[0])
            landed(s_in.at[1:, : n_ea - 1], s_s.at[0])
            landed(w_in.at[: n_ea - 1], w_s.at[0])
            landed(ids_in.at[: n_ea - 1], ids_s.at[0])
            landed(coup_in.at[: n_ea - 1], coup_s.at[0])
        landed(red.at[stage, : total - 1], red_s.at[stage])
        landed(red.at[stage, : total - 1], red_r.at[stage])
        packed = jnp.sum(red[stage, :total], axis=0)

    sol, res = cg_coefficients([packed[:, n : n + 1] for n in range(2 * ITERS)])
    tile = jnp.zeros((1, dz), F32)
    for n, c in enumerate(sol + res):
        tile = jnp.where(lane_r == n, c, tile)
    coefs[...] = tile


def combine_kernel(vu, wu, coefs, sol_v, res_v, sol_w, res_w):
    ecomp = sol_w.shape[0]
    tile = coefs[...]
    solution = [tile[:, n : n + 1] for n in range(ITERS)]
    residual = [tile[:, ITERS + n : ITERS + n + 1] for n in range(ITERS + 1)]

    def combine(factors, terms):
        out = factors[0] * terms[0]
        for f, t in zip(factors[1:], terms[1:]):
            out = out + f * t
        return out

    shape = sol_v.shape
    flat = (shape[0] * shape[1] * shape[2], shape[3])
    v_terms = [vu[n].reshape(flat) for n in range(ITERS + 1)]
    w_terms = [wu[n] for n in range(ITERS + 1)]
    sol_v[...] = combine(solution, v_terms).reshape(shape)
    res_v[...] = combine(residual, v_terms).reshape(shape)
    sol_w[...] = combine(solution, w_terms)[:ecomp]
    res_w[...] = combine(residual, w_terms)[:ecomp]


def body(sizes, *args):
    load_v, load_w, shift, diag, off, coupling, kind, cell, node = args
    n_ea = sizes[2]
    total = sizes[0] * sizes[1] * sizes[2]
    groups = (AXES,) if total <= 64 else (("gx",), ("gy", "ea"))
    widest = total if total <= 64 else max(sizes[0], sizes[1] * sizes[2])
    comps, dx, dy, dz = load_v.shape
    ecomp, enb = load_w.shape
    cap = node.shape[2]
    vmem = pltpu.VMEM
    dma = pltpu.SemaphoreType.DMA
    epad = -(-ecomp // 16) * 16
    slots = n_ea * cap
    scratch = [
        vmem(load_w.shape, F32), vmem(shift.shape, F32), vmem(diag.shape, F32),
        vmem(off.shape, F32), vmem(coupling.shape, F32),
        vmem(cell.shape, jnp.int32), vmem((2,) + node.shape, jnp.int32),
        dma((9,)),
        vmem((n_ea, comps, epad, cap), F32),
        vmem((n_ea, comps, epad, cap), F32),
        vmem((ecomp, epad, enb), F32),
        vmem((2 * dz, slots), BF16),
        vmem((slots, dz), BF16),
        vmem((dx * dy, slots), F32),
        vmem((dx * dy, slots), BF16),
        vmem((n_ea, enb, cap), BF16),
        vmem((slots, enb), BF16),
        vmem((enb, slots), BF16),
        vmem((dx, dy, dz), F32),
        vmem((n_ea, 2, 1, cap), jnp.int32),
        vmem((n_ea, comps, ecomp, cap), F32),
        vmem((ITERS, 2, comps, dy, dz), F32),
        vmem((ITERS, 2, comps, dx, 1, dz), F32),
        vmem((ITERS, 2, 8, dz), F32),
        vmem((n_ea, epad, enb), F32),
        vmem((ITERS, n_ea, comps, cap), F32),
        vmem((ITERS, n_ea, comps, cap), F32),
        vmem((ITERS, 2, 8, dz), F32),
        vmem((ITERS, n_ea, comps, cap), F32),
        vmem((ITERS, n_ea, comps, cap), F32),
        vmem((len(groups), widest, 1, dz), F32),
        vmem((len(groups), 1, dz), F32),
        dma((1,)), dma((1,)),
        dma((1,)), dma((1,)),
        dma((1,)), dma((ITERS,)),
        dma((1,)), dma((ITERS,)),
        dma((1,)), dma((ITERS,)),
        dma((1,)), dma((1,)),
        dma((1,)), dma((ITERS,)),
        dma((1,)), dma((ITERS,)),
        dma((len(groups),)), dma((len(groups),)),
    ]
    basis = pl.pallas_call(
        functools.partial(kernel, sizes, groups),
        out_shape=(
            pltpu.VMEM((ITERS + 1,) + load_v.shape, F32),
            pltpu.VMEM((ITERS + 1, epad, enb), F32),
            pltpu.VMEM((1, dz), F32),
        ),
        in_specs=[pl.BlockSpec(memory_space=pltpu.HBM)] * 9,
        out_specs=[pl.BlockSpec(memory_space=vmem)] * 3,
        scratch_shapes=scratch,
        compiler_params=pltpu.CompilerParams(
            collective_id=0, has_side_effects=True
        ),
        name="krylov",
    )(*args)
    return tuple(
        pl.pallas_call(
            combine_kernel,
            out_shape=tuple(
                jax.ShapeDtypeStruct(like.shape, F32)
                for like in (load_v, load_v, load_w, load_w)
            ),
            in_specs=[pl.BlockSpec(memory_space=vmem)] * 3,
            out_specs=[pl.BlockSpec(memory_space=vmem)] * 4,
            compiler_params=pltpu.CompilerParams(vmem_limit_bytes=8 << 20),
            name="combine",
        )(*basis)
    )


def solution(mesh):
    column = ("gx", "gy", "ea")
    placed = (
        P(None, "gx", "gy", "ea"),
        P(None, column),
        P("gx", "gy", "ea"),
        P(None, column),
        P(None, None, column),
        P(None, None, column),
        P(column, None, None),
        P(column, None, None),
        P(column, None, None),
    )
    return jax.shard_map(
        functools.partial(body, tuple(mesh.shape[a] for a in AXES)),
        mesh=mesh,
        in_specs=placed,
        out_specs=(
            P(None, "gx", "gy", "ea"),
            P(None, "gx", "gy", "ea"),
            P(None, column),
            P(None, column),
        ),
        check_vma=False,
    )
```

```python
import functools

import jax
import jax.numpy as jnp
from jax import lax
from jax.experimental import pallas as pl
from jax.experimental.pallas import tpu as pltpu
from jax.sharding import PartitionSpec as P

ITERS = 3
CENTRE = 11.5
AXES = ("gx", "gy", "ea")
MESH = pl.DeviceIdType.MESH
F32 = jnp.float32
BF16 = jnp.bfloat16


def pieces(x):
    high = x.astype(BF16)
    return high, (x - high.astype(F32)).astype(BF16)


def stacked(x):
    high, low = pieces(x)
    return jnp.concatenate([high, low], axis=0)


def folded(product):
    half = product.shape[0] // 2
    return product[:half] + product[half:]


def iota(shape, dim):
    return lax.broadcasted_iota(jnp.int32, shape, dim)


def times_transposed(a, b):
    return lax.dot_general(
        a, b, (((1,), (1,)), ((), ())), preferred_element_type=F32
    )


def galerkin_coefficients(moment):
    h = [moment[k + 1] + CENTRE * moment[k] for k in range(2 * ITERS - 1)]
    first = 1.0 / h[0]
    l1, l2 = h[1] * first, h[2] * first
    d1 = h[2] - l1 * h[1]
    e = h[3] - l1 * h[2]
    g1 = moment[1] - l1 * moment[0]
    second = 1.0 / d1
    k = e * second
    d2 = h[4] - l2 * h[2] - k * e
    y2 = (moment[2] - l2 * moment[0] - k * g1) / d2
    y1 = (g1 - e * y2) * second
    y0 = (moment[0] - h[1] * y1 - h[2] * y2) * first
    solution = [y0, y1, y2]
    residual = [
        1.0 - CENTRE * y0, -(y0 + CENTRE * y1), -(y1 + CENTRE * y2), -y2
    ]
    return solution, residual


def kernel(
    sizes, groups,
    load_v, load_w, shift_h, diag_h, off_h, coupling_h, kind_h, cell_h, node_h,
    vu, wu, coefs,
    w_first, shift, diag, off, coupling, cell, ids, load_s,
    weights, win, stiff, lanes, rows, rows_b, nodes_mine, nodes_t,
    centre_diag, ids_in, coup_in,
    x_in, y_in, z_in, w_in, p_in, s_in, z_out, p_out, s_out, red, red_out,
    ids_s, ids_r, coup_s, coup_r,
    x_s, x_r, y_s, y_r, z_s, z_r, w_s, w_r, p_s, p_r, s_s, s_r, red_s, red_r,
):
    n_gx, n_gy, n_ea = sizes
    comps, dx, dy, dz = load_v.shape
    ecomp, enb = load_w.shape
    epad = wu.shape[1]
    cap = cell.shape[2]
    per = dx * dy
    allrows = comps * per
    groups8 = allrows // 8
    gi, gj, ek = (lax.axis_index(a) for a in AXES)
    own = {"gx": gi, "gy": gj, "ea": ek}
    count = dict(zip(AXES, sizes))

    def members(group):
        total = 1
        for a in group:
            total *= count[a]
        me = 0
        for a in group:
            me = me * count[a] + own[a]

        def target(d):
            flat = lax.rem(me + d, total)
            coords = dict(own)
            for a in reversed(group):
                coords[a] = lax.rem(flat, count[a])
                flat = lax.div(flat, count[a])
            return tuple(coords[a] for a in AXES)

        return total, me, target

    has = {
        ("gx", 1): gi < n_gx - 1, ("gx", -1): gi > 0,
        ("gy", 1): gj < n_gy - 1, ("gy", -1): gj > 0,
        ("ea", 1): ek < n_ea - 1, ("ea", -1): ek > 0,
    }
    beside = {
        ("gx", s): (gi + s, gj, ek) for s in (1, -1)
    } | {("gy", s): (gi, gj + s, ek) for s in (1, -1)} | {
        ("ea", s): (gi, gj, ek + s) for s in (1, -1)
    }
    slot = {1: 0, -1: 1}

    barrier = pltpu.get_barrier_semaphore()
    wide = n_gx - 1 > ITERS
    expected = 0
    for group in groups if wide else (("gy", "ea"),):
        total, _, target = members(group)
        for d in range(1, total):
            pl.semaphore_signal(barrier, inc=1, device_id=target(d), device_id_type=MESH)
        expected += total - 1
    if not wide:
        for s in (1, -1):
            @pl.when(has["gx", s])
            def _():
                pl.semaphore_signal(
                    barrier, inc=1, device_id=beside["gx", s], device_id_type=MESH
                )
            expected = expected + jnp.where(has["gx", s], 1, 0)

    loads = {}
    for at, (name, src, dst) in enumerate((
        ("w", load_w, w_first), ("node", node_h, ids.at[0]), ("kind", kind_h, ids.at[1]),
        ("v", load_v, vu.at[0]), ("cell", cell_h, cell), ("coupling", coupling_h, coupling),
        ("shift", shift_h, shift), ("off", off_h, off), ("diag", diag_h, diag),
    )):
        at = 1 if name == "kind" else at
        loads[name] = pltpu.make_async_copy(src, dst, load_s.at[at])
        loads[name].start()

    for s in (1, -1):
        for name, buffer in (("gx", x_in), ("gy", y_in), ("ea", z_in)):
            @pl.when(jnp.logical_not(has[name, -s]))
            def _():
                for op in range(ITERS):
                    buffer[op, slot[s]] = jnp.zeros(buffer.shape[2:], F32)

    def partner(d):
        return lax.rem(ek + d, n_ea)

    def remote(src, dst, s_sem, r_sem, device):
        return pltpu.make_async_remote_copy(
            src_ref=src, dst_ref=dst, send_sem=s_sem, recv_sem=r_sem,
            device_id=device, device_id_type=MESH,
        )

    sides = {
        name: jnp.where(has[name, 1], 1, 0) + jnp.where(has[name, -1], 1, 0) for name in AXES
    }

    def landed(ref, sem):
        pltpu.make_async_copy(ref, ref, sem).wait()

    def x_copy(op, s):
        return remote(
            vu.at[op, :, dx - 1 if s == 1 else 0], x_in.at[op, slot[s]],
            x_s.at[0], x_r.at[op], beside["gx", s],
        )

    def y_copy(op, s):
        edge = dy - 1 if s == 1 else 0
        return remote(
            vu.at[op, :, :, edge : edge + 1, :], y_in.at[op, slot[s]],
            y_s.at[0], y_r.at[op], beside["gy", s],
        )

    def z_copy(op, s):
        return remote(
            z_out.at[op, slot[s]], z_in.at[op, slot[s]],
            z_s.at[0], z_r.at[op], beside["ea", s],
        )

    def column_copy(src, dst, s_sem, r_sem, d):
        return remote(src, dst.at[ek], s_sem, r_sem, (gi, gj, partner(d)))

    def w_copy(d):
        return column_copy(wu.at[0], w_in, w_s.at[0], w_r.at[0], d)

    def p_copy(op, d):
        return column_copy(
            p_out.at[op, partner(d)], p_in.at[op], p_s.at[0], p_r.at[op], d
        )

    def s_copy(op, d):
        return column_copy(
            s_out.at[op, partner(d)], s_in.at[op], s_s.at[0], s_r.at[op], d
        )

    def ids_copy(d):
        return column_copy(
            ids.at[:, 0, pl.ds(partner(d), 1), :], ids_in, ids_s.at[0], ids_r.at[0], d
        )

    def block(d):
        return pl.ds(pl.multiple_of(partner(d) * cap, cap), cap)

    def coup_copy(d):
        return column_copy(
            coupling.at[:, :, block(d)], coup_in, coup_s.at[0], coup_r.at[0], d
        )

    def column_send(copy):
        for d in range(1, n_ea):
            copy(d).start()

    lane_i = iota((8, dz), 1)
    lane_r = iota((1, dz), 1)
    row_i = iota((dy, dz), 0)
    lane_b = iota((dy, dz), 1)

    def slabs(o):
        return slice(o * cap, (o + 1) * cap)

    def xy_send(op):
        for s in (1, -1):
            for name, copy in (("gx", x_copy), ("gy", y_copy)):
                @pl.when(has[name, s])
                def _():
                    copy(op, s).start()

    def z_send(op):
        v2 = vu[op].reshape(allrows, dz)
        up = jnp.zeros((8, dz), F32)
        down = jnp.zeros((8, dz), F32)
        for g in range(groups8):
            part = v2[8 * g : 8 * g + 8]
            up = jnp.where(lane_i == g, part[:, dz - 1 : dz], up)
            down = jnp.where(lane_i == g, part[:, 0:1], down)
        z_out[op, 0] = up
        z_out[op, 1] = down
        for s in (1, -1):
            @pl.when(has["ea", s])
            def _():
                z_copy(op, s).start()

    def by_sides(name, two, one, sem):
        @pl.when(sides[name] == 2)
        def _():
            landed(two, sem)

        @pl.when(sides[name] == 1)
        def _():
            landed(one, sem)

    def x_wait(op):
        by_sides("gx", x_in.at[op], x_in.at[op, 0], x_r.at[op])

    def yz_wait(op):
        by_sides("gy", y_in.at[op], y_in.at[op, 0], y_r.at[op])
        by_sides("ea", z_in.at[op], z_in.at[op, 0], z_r.at[op])

    def pick(op):
        h, l = pieces(vu[op].reshape(allrows, dz))
        seen = jnp.dot(
            jnp.concatenate([h, l], axis=1), lanes[...], preferred_element_type=F32
        )
        return [
            jnp.sum(seen[i * per : (i + 1) * per] * rows[...], axis=0, keepdims=True)
            for i in range(comps)
        ]

    def pick_send(op):
        picked = pick(op)
        for i in range(comps):
            for o in range(n_ea):
                p_out[op, o, i : i + 1, :] = picked[i][:, slabs(o)]
        column_send(functools.partial(p_copy, op))

    def local(op):
        v4 = vu[op]
        v2 = v4.reshape(allrows, dz)
        zero = jnp.zeros((comps, 1, dy, dz), F32)
        near = jnp.concatenate([zero, v4[:, : dx - 1]], axis=1) + jnp.concatenate(
            [v4[:, 1:], zero], axis=1
        )
        near = near.reshape(allrows, dz)
        lane_all = iota((allrows, dz), 1)
        row_all = lax.rem(iota((allrows, dz), 0), dy)
        near = near + jnp.where(lane_all == 0, 0.0, pltpu.roll(v2, 1, 1))
        near = near + jnp.where(lane_all == dz - 1, 0.0, pltpu.roll(v2, dz - 1, 1))
        near = near + jnp.where(row_all == 0, 0.0, pltpu.roll(v2, 1, 0))
        near = near + jnp.where(row_all == dy - 1, 0.0, pltpu.roll(v2, allrows - 1, 0))
        vu[op + 1] = centre_diag[...][None] * v4 - near.reshape(v4.shape)

    def local_nodes(op):
        w = wu[op]
        acc = stiff[0] * w[0:1]
        for p in range(1, ecomp):
            acc = acc + stiff[p] * w[p : p + 1]
        wu[op + 1] = acc

    def product(op_a, op_b):
        pv = jnp.sum((vu[op_a] * vu[op_b]).reshape(groups8, 8, dz), axis=0)
        pw = jnp.sum(wu[op_a] * wu[op_b], axis=0, keepdims=True)
        total = jnp.sum(pv, axis=0, keepdims=True)
        for b in range(enb // dz):
            total = total + pw[:, b * dz : (b + 1) * dz]
        return total

    def picks_wait(op):
        p_in[op, ek] = p_out[op, ek]
        landed(p_in.at[op, : n_ea - 1], p_r.at[op])

    def nodes_step(op):
        terms = []
        for o in range(n_ea):
            total = None
            for i in range(comps):
                term = win[o, i] * p_in[op, o, i : i + 1, :]
                total = term if total is None else total + term
            terms.append(total)
        wu[op + 1] += folded(
            times_transposed(stacked(jnp.concatenate(terms, axis=1)), nodes_t[...])
        )

    def sums_send(op):
        values = folded(jnp.dot(stacked(wu[op]), nodes_t[...], preferred_element_type=F32))
        for o in range(n_ea):
            for i in range(comps):
                s_out[op, o, i : i + 1, :] = jnp.sum(
                    win[o, i] * values[:, slabs(o)], axis=0, keepdims=True
                )
        column_send(functools.partial(s_copy, op))

    def first_sums():
        w_in[ek] = wu[0]
        landed(w_in.at[: n_ea - 1], w_r.at[0])
        for o in range(n_ea):
            values = folded(jnp.dot(stacked(w_in[o]), nodes_mine[o], preferred_element_type=F32))
            for i in range(comps):
                s_in[0, o, i : i + 1, :] = jnp.sum(
                    weights[o, i] * values, axis=0, keepdims=True
                )

    def sums_wait(op):
        s_in[op, ek] = s_out[op, ek]
        landed(s_in.at[op, : n_ea - 1], s_r.at[op])

    def cells_step(op):
        spread_h, spread_l = [], []
        for i in range(comps):
            line = jnp.concatenate([s_in[op, o, i : i + 1, :] for o in range(n_ea)], axis=1)
            h, l = pieces(line)
            spread_h.append(rows_b[...] * h)
            spread_l.append(rows_b[...] * l)
        added = folded(
            times_transposed(jnp.concatenate(spread_h + spread_l, axis=0), lanes[:dz, :])
        )
        vu[op + 1] += added.reshape(comps, dx, dy, dz)

    def yz_apply(op):
        z_low, z_high = z_in[op, 0], z_in[op, 1]
        for i in range(comps):
            for a in range(dx):
                at = i * dx + a
                side = jnp.where(row_i == 0, y_in[op, 0, i, a], 0.0)
                side = side + jnp.where(row_i == dy - 1, y_in[op, 1, i, a], 0.0)
                z_l, z_h = [], []
                for b in range(dy // 8):
                    g = at * (dy // 8) + b
                    z_l.append(jnp.broadcast_to(z_low[:, g : g + 1], (8, dz)))
                    z_h.append(jnp.broadcast_to(z_high[:, g : g + 1], (8, dz)))
                side = side + jnp.where(lane_b == 0, jnp.concatenate(z_l, axis=0), 0.0)
                side = side + jnp.where(lane_b == dz - 1, jnp.concatenate(z_h, axis=0), 0.0)
                vu[op + 1, i, a] -= side

    def x_apply(op):
        vu[op + 1, :, 0] -= x_in[op, 0]
        vu[op + 1, :, dx - 1] -= x_in[op, 1]

    def near_moment(op):
        y = y_in[op, 0] * vu[op, :, :, 0:1] + y_in[op, 1] * vu[op, :, :, dy - 1 : dy]
        z = z_out[op, 1] * z_in[op, 0] + z_out[op, 0] * z_in[op, 1]
        side = jnp.sum(y.reshape(comps * dx, dz), axis=0, keepdims=True)
        return side + jnp.sum(z, axis=0, keepdims=True)

    def slot_moment(op):
        cross = None
        for o in range(n_ea):
            term = p_in[op, o] * s_out[op, o]
            cross = term if cross is None else cross + term
        return jnp.sum(cross, axis=0, keepdims=True)

    def far_moment(op):
        x = x_in[op, 0] * vu[op, :, 0] + x_in[op, 1] * vu[op, :, dx - 1]
        return jnp.sum(x.reshape(comps * dy, dz), axis=0, keepdims=True)

    loads["w"].wait()
    wu[0] = jnp.concatenate([w_first[...], jnp.zeros((epad - ecomp, enb), F32)], axis=0)
    landed(ids, load_s.at[1])
    loads["v"].wait()

    pl.semaphore_wait(barrier, expected)

    column_send(ids_copy)
    column_send(w_copy)
    xy_send(0)
    z_send(0)
    loads["cell"].wait()
    tile = cell[0]
    tile_row = lax.div(tile, dz)
    tile_lane = tile - tile_row * dz
    for o in range(n_ea):
        hot = jnp.where(
            iota((dz, cap), 0) == tile_lane[o : o + 1], 1.0, 0.0
        ).astype(BF16)
        lanes[:dz, slabs(o)] = hot
        lanes[dz:, slabs(o)] = hot
        r = jnp.where(iota((per, cap), 0) == tile_row[o : o + 1], 1.0, 0.0)
        rows[:, slabs(o)] = r
        rows_b[:, slabs(o)] = r.astype(BF16)
    pick_send(0)
    loads["coupling"].wait()
    column_send(coup_copy)

    for o in range(n_ea):
        nodes_mine[o] = jnp.where(
            iota((enb, cap), 0) == ids[0, 0, o : o + 1, :], 1.0, 0.0
        ).astype(BF16)
    no_row = jnp.zeros((epad - ecomp, cap), F32)

    def masked(raw, k):
        heavi = jnp.where(k >= 1, 1.0, 0.0)
        tip = jnp.where(k == 2, 1.0, 0.0)
        mask = jnp.where(iota((ecomp, cap), 0) < 3, heavi, tip)
        return jnp.concatenate([raw * mask, no_row], axis=0)

    for o in range(n_ea):
        for i in range(comps):
            weights[o, i] = masked(coupling[i, :, slabs(o)], ids[1, 0, o : o + 1, :])
    loads["shift"].wait()
    centre_diag[...] = shift[...] + (6.0 - CENTRE)
    local(0)
    loads["off"].wait()
    loads["diag"].wait()
    for p in range(ecomp):
        whole = 0.5 * (off[p] + off[:, p, :])
        whole = jnp.where(iota((ecomp, enb), 0) == p, diag[p : p + 1, :] - CENTRE, whole)
        stiff[p] = jnp.concatenate([whole, jnp.zeros((epad - ecomp, enb), F32)], axis=0)
    local_nodes(0)
    moments = [product(0, 0)]
    ids_in[ek] = ids[:, 0, pl.ds(ek, 1), :]
    coup_in[ek] = coupling[:, :, block(0)]
    landed(ids_in.at[: n_ea - 1], ids_r.at[0])
    for o in range(n_ea):
        nodes_t[:, slabs(o)] = jnp.where(
            iota((enb, cap), 0) == ids_in[o, 0], 1.0, 0.0
        ).astype(BF16)
    yz_wait(0)
    yz_apply(0)
    first_sums()
    cells_step(0)
    x_wait(0)
    x_apply(0)
    xy_send(1)
    landed(coup_in.at[: n_ea - 1], coup_r.at[0])
    for o in range(n_ea):
        for i in range(comps):
            win[o, i] = masked(coup_in[o, i], ids_in[o, 1])
    picks_wait(0)
    nodes_step(0)
    sums_send(1)
    z_send(1)
    pick_send(1)
    last = ITERS - 1
    for op in range(1, last):
        local(op)
        local_nodes(op)
        moments.append(product(op - 1, op))
        moments.append(product(op, op))
        sums_wait(op)
        cells_step(op)
        yz_wait(op)
        yz_apply(op)
        x_wait(op)
        x_apply(op)
        xy_send(op + 1)
        z_send(op + 1)
        pick_send(op + 1)
        picks_wait(op)
        nodes_step(op)
        sums_send(op + 1)

    local(last)
    local_nodes(last)
    moments.append(product(last - 1, last))
    moments.append(product(last, last))
    row = product(last, last + 1)
    packed = jnp.zeros((1, dz), F32)
    for n, m in enumerate(moments):
        packed = jnp.where(lane_r == n, jnp.sum(m, axis=1, keepdims=True), packed)
    red_out[0, 0:1, :] = packed
    yz_wait(last)
    picks_wait(last)
    row = row - near_moment(last) + 2.0 * slot_moment(last)
    x_wait(last)
    red_out[0, 1:2, :] = row - far_moment(last)

    for stage, group in enumerate(groups):
        total, me, target = members(group)
        whole = group == AXES
        for d in range(total - 1):
            dst = red.at[stage, me]
            ends = (red_s.at[stage], red_r.at[stage])
            if whole:
                pltpu.make_async_remote_copy(
                    src_ref=red_out.at[stage], dst_ref=dst, send_sem=ends[0], recv_sem=ends[1],
                    device_id=d + jnp.where(me <= d, 1, 0),
                    device_id_type=pl.DeviceIdType.LOGICAL,
                ).start()
            else:
                remote(red_out.at[stage], dst, *ends, target(d + 1)).start()
        red[stage, me] = red_out[stage]
        if stage == 0:
            nodes_step(last)
            yz_apply(last)
            x_apply(last)
            sums_wait(last)
            cells_step(last)
            for name, buffer, sem in (("gx", x_in, x_s), ("gy", y_in, y_s), ("ea", z_in, z_s)):
                by_sides(name, buffer, buffer.at[:, 0], sem.at[0])
            landed(p_in.at[:, : n_ea - 1], p_s.at[0])
            landed(s_in.at[1:, : n_ea - 1], s_s.at[0])
            landed(w_in.at[: n_ea - 1], w_s.at[0])
            landed(ids_in.at[: n_ea - 1], ids_s.at[0])
            landed(coup_in.at[: n_ea - 1], coup_s.at[0])
        landed(red.at[stage, : total - 1], red_s.at[stage])
        landed(red.at[stage, : total - 1], red_r.at[stage])
        reduced = jnp.sum(red[stage, :total], axis=0)
        if stage + 1 < len(groups):
            red_out[stage + 1] = reduced

    early = [jnp.broadcast_to(reduced[0:1, n : n + 1], (1, dz)) for n in range(2 * ITERS - 1)]
    final = jnp.broadcast_to(jnp.sum(reduced[1:2], axis=1, keepdims=True), (1, dz))
    sol, res = galerkin_coefficients(early + [final])
    for n, c in enumerate(sol + res):
        coefs[n : n + 1, :] = c


def combine_kernel(vu, wu, coefs, sol_v, res_v, sol_w, res_w):
    ecomp = sol_w.shape[0]
    lane_tiles = sol_w.shape[1] // coefs.shape[1]

    def wider(factor):
        return jnp.concatenate([factor] * lane_tiles, axis=1)

    solution = [coefs[n : n + 1, :] for n in range(ITERS)]
    residual = [coefs[ITERS + n : ITERS + n + 1, :] for n in range(ITERS + 1)]

    def combine(factors, terms):
        out = factors[0] * terms[0]
        for f, t in zip(factors[1:], terms[1:]):
            out = out + f * t
        return out

    shape = sol_v.shape
    flat = (shape[0] * shape[1] * shape[2], shape[3])
    v_terms = [vu[n].reshape(flat) for n in range(ITERS + 1)]
    w_terms = [wu[n] for n in range(ITERS + 1)]
    sol_v[...] = combine(solution, v_terms).reshape(shape)
    res_v[...] = combine(residual, v_terms).reshape(shape)
    sol_w[...] = combine([wider(f) for f in solution], w_terms)[:ecomp]
    res_w[...] = combine([wider(f) for f in residual], w_terms)[:ecomp]


def body(sizes, *args):
    load_v, load_w, shift, diag, off, coupling, kind, cell, node = args
    n_ea = sizes[2]
    total = sizes[0] * sizes[1] * sizes[2]
    groups = (AXES,) if total <= 64 else (("gx",), ("gy", "ea"))
    widest = total if total <= 64 else max(sizes[0], sizes[1] * sizes[2])
    comps, dx, dy, dz = load_v.shape
    ecomp, enb = load_w.shape
    cap = node.shape[2]
    vmem = pltpu.VMEM
    dma = pltpu.SemaphoreType.DMA
    epad = -(-ecomp // 16) * 16
    slots = n_ea * cap
    scratch = [
        vmem(load_w.shape, F32), vmem(shift.shape, F32), vmem(diag.shape, F32),
        vmem(off.shape, F32), vmem(coupling.shape, F32),
        vmem(cell.shape, jnp.int32), vmem((2,) + node.shape, jnp.int32),
        dma((9,)),
        vmem((n_ea, comps, epad, cap), F32),
        vmem((n_ea, comps, epad, cap), F32),
        vmem((ecomp, epad, enb), F32),
        vmem((2 * dz, slots), BF16),
        vmem((dx * dy, slots), F32),
        vmem((dx * dy, slots), BF16),
        vmem((n_ea, enb, cap), BF16),
        vmem((enb, slots), BF16),
        vmem((dx, dy, dz), F32),
        vmem((n_ea, 2, 1, cap), jnp.int32),
        vmem((n_ea, comps, ecomp, cap), F32),
        vmem((ITERS, 2, comps, dy, dz), F32),
        vmem((ITERS, 2, comps, dx, 1, dz), F32),
        vmem((ITERS, 2, 8, dz), F32),
        vmem((n_ea, epad, enb), F32),
        vmem((ITERS, n_ea, comps, cap), F32),
        vmem((ITERS, n_ea, comps, cap), F32),
        vmem((ITERS, 2, 8, dz), F32),
        vmem((ITERS, n_ea, comps, cap), F32),
        vmem((ITERS, n_ea, comps, cap), F32),
        vmem((len(groups), widest, 2, dz), F32),
        vmem((len(groups), 2, dz), F32),
        dma((1,)), dma((1,)),
        dma((1,)), dma((1,)),
        dma((1,)), dma((ITERS,)),
        dma((1,)), dma((ITERS,)),
        dma((1,)), dma((ITERS,)),
        dma((1,)), dma((1,)),
        dma((1,)), dma((ITERS,)),
        dma((1,)), dma((ITERS,)),
        dma((len(groups),)), dma((len(groups),)),
    ]
    basis = pl.pallas_call(
        functools.partial(kernel, sizes, groups),
        out_shape=(
            pltpu.VMEM((ITERS + 1,) + load_v.shape, F32),
            pltpu.VMEM((ITERS + 1, epad, enb), F32),
            pltpu.VMEM((2 * ITERS + 2, dz), F32),
        ),
        in_specs=[pl.BlockSpec(memory_space=pltpu.HBM)] * 9,
        out_specs=[pl.BlockSpec(memory_space=vmem)] * 3,
        scratch_shapes=scratch,
        compiler_params=pltpu.CompilerParams(
            collective_id=0, has_side_effects=True
        ),
        name="krylov",
    )(*args)
    return tuple(
        pl.pallas_call(
            combine_kernel,
            out_shape=tuple(
                jax.ShapeDtypeStruct(like.shape, F32)
                for like in (load_v, load_v, load_w, load_w)
            ),
            in_specs=[pl.BlockSpec(memory_space=vmem)] * 3,
            out_specs=[pl.BlockSpec(memory_space=vmem)] * 4,
            compiler_params=pltpu.CompilerParams(vmem_limit_bytes=8 << 20),
            name="combine",
        )(*basis)
    )


def solution(mesh):
    column = ("gx", "gy", "ea")
    placed = (
        P(None, "gx", "gy", "ea"),
        P(None, column),
        P("gx", "gy", "ea"),
        P(None, column),
        P(None, None, column),
        P(None, None, column),
        P(column, None, None),
        P(column, None, None),
        P(column, None, None),
    )
    return jax.shard_map(
        functools.partial(body, tuple(mesh.shape[a] for a in AXES)),
        mesh=mesh,
        in_specs=placed,
        out_specs=(
            P(None, "gx", "gy", "ea"),
            P(None, "gx", "gy", "ea"),
            P(None, column),
            P(None, column),
        ),
        check_vma=False,
    )
```

```python
import functools

import jax
import jax.numpy as jnp
from jax import lax
from jax.experimental import pallas as pl
from jax.experimental.pallas import tpu as pltpu
from jax.sharding import PartitionSpec as P

ITERS = 3
CENTRE = 11.5
AXES = ("gx", "gy", "ea")
MESH = pl.DeviceIdType.MESH
F32 = jnp.float32
BF16 = jnp.bfloat16


def pieces(x):
    high = x.astype(BF16)
    return high, (x - high.astype(F32)).astype(BF16)


def stacked(x):
    high, low = pieces(x)
    return jnp.concatenate([high, low], axis=0)


def folded(product):
    half = product.shape[0] // 2
    return product[:half] + product[half:]


def iota(shape, dim):
    return lax.broadcasted_iota(jnp.int32, shape, dim)


def times_transposed(a, b):
    return lax.dot_general(
        a, b, (((1,), (1,)), ((), ())), preferred_element_type=F32
    )


def galerkin_coefficients(moment):
    h = [moment[k + 1] + CENTRE * moment[k] for k in range(2 * ITERS - 1)]
    first = 1.0 / h[0]
    l1, l2 = h[1] * first, h[2] * first
    d1 = h[2] - l1 * h[1]
    e = h[3] - l1 * h[2]
    g1 = moment[1] - l1 * moment[0]
    second = 1.0 / d1
    k = e * second
    d2 = h[4] - l2 * h[2] - k * e
    y2 = (moment[2] - l2 * moment[0] - k * g1) / d2
    y1 = (g1 - e * y2) * second
    y0 = (moment[0] - h[1] * y1 - h[2] * y2) * first
    solution = [y0, y1, y2]
    residual = [
        1.0 - CENTRE * y0, -(y0 + CENTRE * y1), -(y1 + CENTRE * y2), -y2
    ]
    return solution, residual


def kernel(
    sizes, groups,
    load_v, load_w, shift_h, diag_h, off_h, coupling_h, kind_h, cell_h, node_h,
    vu, wu, coefs,
    w_first, shift, diag, off, coupling, cell, ids,
    weights, win, stiff, lanes, rows, rows_b, nodes_mine, nodes_t,
    centre_diag, ids_in, coup_in,
    x_in, y_in, z_in, w_in, p_in, s_in, z_out, p_out, s_out, red, red_out,
    red_s, red_r,
):
    n_gx, n_gy, n_ea = sizes
    comps, dx, dy, dz = load_v.shape
    ecomp, enb = load_w.shape
    epad = wu.shape[1]
    cap = cell.shape[2]
    per = dx * dy
    allrows = comps * per
    groups8 = allrows // 8
    gi, gj, ek = (lax.axis_index(a) for a in AXES)
    own = {"gx": gi, "gy": gj, "ea": ek}
    count = dict(zip(AXES, sizes))

    def members(group):
        total = 1
        for a in group:
            total *= count[a]
        me = 0
        for a in group:
            me = me * count[a] + own[a]

        def target(d):
            flat = lax.rem(me + d, total)
            coords = dict(own)
            for a in reversed(group):
                coords[a] = lax.rem(flat, count[a])
                flat = lax.div(flat, count[a])
            return tuple(coords[a] for a in AXES)

        return total, me, target

    def remote(src, dst, s_sem, r_sem, device):
        return pltpu.make_async_remote_copy(
            src_ref=src, dst_ref=dst, send_sem=s_sem, recv_sem=r_sem,
            device_id=device, device_id_type=MESH,
        )

    def landed(ref, sem):
        pltpu.make_async_copy(ref, ref, sem).wait()

    def red_start(stage, group):
        total, me, target = members(group)
        for d in range(total - 1):
            dst = red.at[stage, me]
            ends = (red_s.at[stage], red_r.at[stage])
            if group == AXES:
                pltpu.make_async_remote_copy(
                    src_ref=red_out.at[stage], dst_ref=dst, send_sem=ends[0], recv_sem=ends[1],
                    device_id=d + jnp.where(me <= d, 1, 0),
                    device_id_type=pl.DeviceIdType.LOGICAL,
                ).start()
            else:
                remote(red_out.at[stage], dst, *ends, target(d + 1)).start()
        red[stage, me] = red_out[stage]

    def steps(
        load_s, ids_s, ids_r, coup_s, coup_r, x_s, x_r, y_s, y_r, z_s, z_r,
        w_s, w_r, p_s, p_r, s_s, s_r,
    ):
        has = {
            ("gx", 1): gi < n_gx - 1, ("gx", -1): gi > 0,
            ("gy", 1): gj < n_gy - 1, ("gy", -1): gj > 0,
            ("ea", 1): ek < n_ea - 1, ("ea", -1): ek > 0,
        }
        beside = {
            ("gx", s): (gi + s, gj, ek) for s in (1, -1)
        } | {("gy", s): (gi, gj + s, ek) for s in (1, -1)} | {
            ("ea", s): (gi, gj, ek + s) for s in (1, -1)
        }
        slot = {1: 0, -1: 1}
        sides = {
            name: jnp.where(has[name, 1], 1, 0) + jnp.where(has[name, -1], 1, 0) for name in AXES
        }


        barrier = pltpu.get_barrier_semaphore()
        wide = n_gx - 1 > ITERS
        expected = 0
        for group in groups if wide else (("gy", "ea"),):
            total, _, target = members(group)
            for d in range(1, total):
                pl.semaphore_signal(barrier, inc=1, device_id=target(d), device_id_type=MESH)
            expected += total - 1
        if not wide:
            for s in (1, -1):
                @pl.when(has["gx", s])
                def _():
                    pl.semaphore_signal(
                        barrier, inc=1, device_id=beside["gx", s], device_id_type=MESH
                    )
                expected = expected + jnp.where(has["gx", s], 1, 0)

        loads = {}
        for at, (name, src, dst) in enumerate((
            ("w", load_w, w_first), ("node", node_h, ids.at[0]), ("kind", kind_h, ids.at[1]),
            ("v", load_v, vu.at[0]), ("cell", cell_h, cell), ("coupling", coupling_h, coupling),
            ("shift", shift_h, shift), ("off", off_h, off), ("diag", diag_h, diag),
        )):
            at = 1 if name == "kind" else at
            loads[name] = pltpu.make_async_copy(src, dst, load_s.at[at])
            loads[name].start()

        for s in (1, -1):
            for name, buffer in (("gx", x_in), ("gy", y_in), ("ea", z_in)):
                @pl.when(jnp.logical_not(has[name, -s]))
                def _():
                    for op in range(ITERS):
                        buffer[op, slot[s]] = jnp.zeros(buffer.shape[2:], F32)

        def partner(d):
            return lax.rem(ek + d, n_ea)

        def x_copy(op, s):
            return remote(
                vu.at[op, :, dx - 1 if s == 1 else 0], x_in.at[op, slot[s]],
                x_s.at[0], x_r.at[op], beside["gx", s],
            )

        def y_copy(op, s):
            edge = dy - 1 if s == 1 else 0
            return remote(
                vu.at[op, :, :, edge : edge + 1, :], y_in.at[op, slot[s]],
                y_s.at[0], y_r.at[op], beside["gy", s],
            )

        def z_copy(op, s):
            return remote(
                z_out.at[op, slot[s]], z_in.at[op, slot[s]],
                z_s.at[0], z_r.at[op], beside["ea", s],
            )

        def column_copy(src, dst, s_sem, r_sem, d):
            return remote(src, dst.at[ek], s_sem, r_sem, (gi, gj, partner(d)))

        def w_copy(d):
            return column_copy(wu.at[0], w_in, w_s.at[0], w_r.at[0], d)

        def p_copy(op, d):
            return column_copy(
                p_out.at[op, partner(d)], p_in.at[op], p_s.at[0], p_r.at[op], d
            )

        def s_copy(op, d):
            return column_copy(
                s_out.at[op, partner(d)], s_in.at[op], s_s.at[0], s_r.at[op], d
            )

        def ids_copy(d):
            return column_copy(
                ids.at[:, 0, pl.ds(partner(d), 1), :], ids_in, ids_s.at[0], ids_r.at[0], d
            )

        def block(d):
            return pl.ds(pl.multiple_of(partner(d) * cap, cap), cap)

        def coup_copy(d):
            return column_copy(
                coupling.at[:, :, block(d)], coup_in, coup_s.at[0], coup_r.at[0], d
            )

        def column_send(copy):
            for d in range(1, n_ea):
                copy(d).start()

        lane_i = iota((8, dz), 1)
        lane_r = iota((1, dz), 1)
        row_i = iota((dy, dz), 0)
        lane_b = iota((dy, dz), 1)

        def slabs(o):
            return slice(o * cap, (o + 1) * cap)

        def xy_send(op):
            for s in (1, -1):
                for name, copy in (("gx", x_copy), ("gy", y_copy)):
                    @pl.when(has[name, s])
                    def _():
                        copy(op, s).start()

        def z_send(op):
            v2 = vu[op].reshape(allrows, dz)
            up = jnp.zeros((8, dz), F32)
            down = jnp.zeros((8, dz), F32)
            for g in range(groups8):
                part = v2[8 * g : 8 * g + 8]
                up = jnp.where(lane_i == g, part[:, dz - 1 : dz], up)
                down = jnp.where(lane_i == g, part[:, 0:1], down)
            z_out[op, 0] = up
            z_out[op, 1] = down
            for s in (1, -1):
                @pl.when(has["ea", s])
                def _():
                    z_copy(op, s).start()

        def by_sides(name, two, one, sem):
            @pl.when(sides[name] == 2)
            def _():
                landed(two, sem)

            @pl.when(sides[name] == 1)
            def _():
                landed(one, sem)

        def x_wait(op):
            by_sides("gx", x_in.at[op], x_in.at[op, 0], x_r.at[op])

        def yz_wait(op):
            by_sides("gy", y_in.at[op], y_in.at[op, 0], y_r.at[op])
            by_sides("ea", z_in.at[op], z_in.at[op, 0], z_r.at[op])

        def pick(op):
            h, l = pieces(vu[op].reshape(allrows, dz))
            seen = jnp.dot(
                jnp.concatenate([h, l], axis=1), lanes[...], preferred_element_type=F32
            )
            return [
                jnp.sum(seen[i * per : (i + 1) * per] * rows[...], axis=0, keepdims=True)
                for i in range(comps)
            ]

        def pick_send(op):
            picked = pick(op)
            for i in range(comps):
                for o in range(n_ea):
                    p_out[op, o, i : i + 1, :] = picked[i][:, slabs(o)]
            column_send(functools.partial(p_copy, op))

        def local(op):
            v4 = vu[op]
            v2 = v4.reshape(allrows, dz)
            zero = jnp.zeros((comps, 1, dy, dz), F32)
            near = jnp.concatenate([zero, v4[:, : dx - 1]], axis=1) + jnp.concatenate(
                [v4[:, 1:], zero], axis=1
            )
            near = near.reshape(allrows, dz)
            lane_all = iota((allrows, dz), 1)
            row_all = lax.rem(iota((allrows, dz), 0), dy)
            near = near + jnp.where(lane_all == 0, 0.0, pltpu.roll(v2, 1, 1))
            near = near + jnp.where(lane_all == dz - 1, 0.0, pltpu.roll(v2, dz - 1, 1))
            near = near + jnp.where(row_all == 0, 0.0, pltpu.roll(v2, 1, 0))
            near = near + jnp.where(row_all == dy - 1, 0.0, pltpu.roll(v2, allrows - 1, 0))
            vu[op + 1] = centre_diag[...][None] * v4 - near.reshape(v4.shape)

        def local_nodes(op):
            w = wu[op]
            acc = stiff[0] * w[0:1]
            for p in range(1, ecomp):
                acc = acc + stiff[p] * w[p : p + 1]
            wu[op + 1] = acc

        def product(op_a, op_b):
            pv = jnp.sum((vu[op_a] * vu[op_b]).reshape(groups8, 8, dz), axis=0)
            pw = jnp.sum(wu[op_a] * wu[op_b], axis=0, keepdims=True)
            total = jnp.sum(pv, axis=0, keepdims=True)
            for b in range(enb // dz):
                total = total + pw[:, b * dz : (b + 1) * dz]
            return total

        def picks_wait(op):
            p_in[op, ek] = p_out[op, ek]
            landed(p_in.at[op, : n_ea - 1], p_r.at[op])

        def nodes_step(op):
            terms = []
            for o in range(n_ea):
                total = None
                for i in range(comps):
                    term = win[o, i] * p_in[op, o, i : i + 1, :]
                    total = term if total is None else total + term
                terms.append(total)
            wu[op + 1] += folded(
                times_transposed(stacked(jnp.concatenate(terms, axis=1)), nodes_t[...])
            )

        def sums_send(op):
            values = folded(jnp.dot(stacked(wu[op]), nodes_t[...], preferred_element_type=F32))
            for o in range(n_ea):
                for i in range(comps):
                    s_out[op, o, i : i + 1, :] = jnp.sum(
                        win[o, i] * values[:, slabs(o)], axis=0, keepdims=True
                    )
            column_send(functools.partial(s_copy, op))

        def first_sums():
            w_in[ek] = wu[0]
            landed(w_in.at[: n_ea - 1], w_r.at[0])
            for o in range(n_ea):
                values = folded(jnp.dot(stacked(w_in[o]), nodes_mine[o], preferred_element_type=F32))
                for i in range(comps):
                    s_in[0, o, i : i + 1, :] = jnp.sum(
                        weights[o, i] * values, axis=0, keepdims=True
                    )

        def sums_wait(op):
            s_in[op, ek] = s_out[op, ek]
            landed(s_in.at[op, : n_ea - 1], s_r.at[op])

        def cells_step(op):
            spread_h, spread_l = [], []
            for i in range(comps):
                line = jnp.concatenate([s_in[op, o, i : i + 1, :] for o in range(n_ea)], axis=1)
                h, l = pieces(line)
                spread_h.append(rows_b[...] * h)
                spread_l.append(rows_b[...] * l)
            added = folded(
                times_transposed(jnp.concatenate(spread_h + spread_l, axis=0), lanes[:dz, :])
            )
            vu[op + 1] += added.reshape(comps, dx, dy, dz)

        def yz_apply(op):
            z_low, z_high = z_in[op, 0], z_in[op, 1]
            for i in range(comps):
                for a in range(dx):
                    at = i * dx + a
                    side = jnp.where(row_i == 0, y_in[op, 0, i, a], 0.0)
                    side = side + jnp.where(row_i == dy - 1, y_in[op, 1, i, a], 0.0)
                    z_l, z_h = [], []
                    for b in range(dy // 8):
                        g = at * (dy // 8) + b
                        z_l.append(jnp.broadcast_to(z_low[:, g : g + 1], (8, dz)))
                        z_h.append(jnp.broadcast_to(z_high[:, g : g + 1], (8, dz)))
                    side = side + jnp.where(lane_b == 0, jnp.concatenate(z_l, axis=0), 0.0)
                    side = side + jnp.where(lane_b == dz - 1, jnp.concatenate(z_h, axis=0), 0.0)
                    vu[op + 1, i, a] -= side

        def x_apply(op):
            vu[op + 1, :, 0] -= x_in[op, 0]
            vu[op + 1, :, dx - 1] -= x_in[op, 1]

        def near_moment(op):
            y = y_in[op, 0] * vu[op, :, :, 0:1] + y_in[op, 1] * vu[op, :, :, dy - 1 : dy]
            z = z_out[op, 1] * z_in[op, 0] + z_out[op, 0] * z_in[op, 1]
            side = jnp.sum(y.reshape(comps * dx, dz), axis=0, keepdims=True)
            return side + jnp.sum(z, axis=0, keepdims=True)

        def slot_moment(op):
            cross = None
            for o in range(n_ea):
                term = p_in[op, o] * s_out[op, o]
                cross = term if cross is None else cross + term
            return jnp.sum(cross, axis=0, keepdims=True)

        def far_moment(op):
            x = x_in[op, 0] * vu[op, :, 0] + x_in[op, 1] * vu[op, :, dx - 1]
            return jnp.sum(x.reshape(comps * dy, dz), axis=0, keepdims=True)

        loads["w"].wait()
        wu[0] = jnp.concatenate([w_first[...], jnp.zeros((epad - ecomp, enb), F32)], axis=0)
        landed(ids, load_s.at[1])
        loads["v"].wait()

        pl.semaphore_wait(barrier, expected)

        column_send(ids_copy)
        column_send(w_copy)
        xy_send(0)
        z_send(0)
        loads["coupling"].wait()
        column_send(coup_copy)
        loads["cell"].wait()
        tile = cell[0]
        tile_row = lax.div(tile, dz)
        tile_lane = tile - tile_row * dz
        for o in range(n_ea):
            hot = jnp.where(
                iota((dz, cap), 0) == tile_lane[o : o + 1], 1.0, 0.0
            ).astype(BF16)
            lanes[:dz, slabs(o)] = hot
            lanes[dz:, slabs(o)] = hot
            r = jnp.where(iota((per, cap), 0) == tile_row[o : o + 1], 1.0, 0.0)
            rows[:, slabs(o)] = r
            rows_b[:, slabs(o)] = r.astype(BF16)
        pick_send(0)

        for o in range(n_ea):
            nodes_mine[o] = jnp.where(
                iota((enb, cap), 0) == ids[0, 0, o : o + 1, :], 1.0, 0.0
            ).astype(BF16)
        no_row = jnp.zeros((epad - ecomp, cap), F32)

        def masked(raw, k):
            heavi = jnp.where(k >= 1, 1.0, 0.0)
            tip = jnp.where(k == 2, 1.0, 0.0)
            mask = jnp.where(iota((ecomp, cap), 0) < 3, heavi, tip)
            return jnp.concatenate([raw * mask, no_row], axis=0)

        for o in range(n_ea):
            for i in range(comps):
                weights[o, i] = masked(coupling[i, :, slabs(o)], ids[1, 0, o : o + 1, :])
        loads["shift"].wait()
        centre_diag[...] = shift[...] + (6.0 - CENTRE)
        local(0)
        loads["off"].wait()
        loads["diag"].wait()
        for p in range(ecomp):
            whole = 0.5 * (off[p] + off[:, p, :])
            whole = jnp.where(iota((ecomp, enb), 0) == p, diag[p : p + 1, :] - CENTRE, whole)
            stiff[p] = jnp.concatenate([whole, jnp.zeros((epad - ecomp, enb), F32)], axis=0)
        local_nodes(0)
        moments = [product(0, 0)]
        ids_in[ek] = ids[:, 0, pl.ds(ek, 1), :]
        coup_in[ek] = coupling[:, :, block(0)]
        landed(ids_in.at[: n_ea - 1], ids_r.at[0])
        for o in range(n_ea):
            nodes_t[:, slabs(o)] = jnp.where(
                iota((enb, cap), 0) == ids_in[o, 0], 1.0, 0.0
            ).astype(BF16)
        yz_wait(0)
        yz_apply(0)
        first_sums()
        cells_step(0)
        x_wait(0)
        x_apply(0)
        xy_send(1)
        landed(coup_in.at[: n_ea - 1], coup_r.at[0])
        for o in range(n_ea):
            for i in range(comps):
                win[o, i] = masked(coup_in[o, i], ids_in[o, 1])
        picks_wait(0)
        nodes_step(0)
        sums_send(1)
        pick_send(1)
        z_send(1)
        last = ITERS - 1
        for op in range(1, last):
            local(op)
            local_nodes(op)
            moments.append(product(op - 1, op))
            moments.append(product(op, op))
            yz_wait(op)
            yz_apply(op)
            sums_wait(op)
            cells_step(op)
            x_wait(op)
            x_apply(op)
            xy_send(op + 1)
            pick_send(op + 1)
            z_send(op + 1)
            picks_wait(op)
            nodes_step(op)
            sums_send(op + 1)

        local(last)
        local_nodes(last)
        moments.append(product(last - 1, last))
        moments.append(product(last, last))
        row = product(last, last + 1)
        packed = jnp.zeros((1, dz), F32)
        for n, m in enumerate(moments):
            packed = jnp.where(lane_r == n, jnp.sum(m, axis=1, keepdims=True), packed)
        red_out[0, 0:1, :] = packed
        yz_wait(last)
        picks_wait(last)
        row = row - near_moment(last) + 2.0 * slot_moment(last)
        x_wait(last)
        red_out[0, 1:2, :] = row - far_moment(last)

        red_start(0, groups[0])
        nodes_step(last)
        yz_apply(last)
        x_apply(last)
        sums_wait(last)
        cells_step(last)
        for name, buffer, sem in (("gx", x_in, x_s), ("gy", y_in, y_s), ("ea", z_in, z_s)):
            by_sides(name, buffer, buffer.at[:, 0], sem.at[0])
        landed(p_in.at[:, : n_ea - 1], p_s.at[0])
        landed(s_in.at[1:, : n_ea - 1], s_s.at[0])
        landed(w_in.at[: n_ea - 1], w_s.at[0])
        landed(ids_in.at[: n_ea - 1], ids_s.at[0])
        landed(coup_in.at[: n_ea - 1], coup_s.at[0])

    dma = pltpu.SemaphoreType.DMA
    one, each = dma((1,)), dma((ITERS,))
    pl.run_scoped(
        steps, dma((9,)), one, one, one, one, one, each, one, each, one, each,
        one, one, one, each, one, each,
    )

    for stage, group in enumerate(groups):
        total = members(group)[0]
        if stage > 0:
            red_out[stage] = reduced
            red_start(stage, group)
        landed(red.at[stage, : total - 1], red_s.at[stage])
        landed(red.at[stage, : total - 1], red_r.at[stage])
        reduced = jnp.sum(red[stage, :total], axis=0)

    early = [jnp.broadcast_to(reduced[0:1, n : n + 1], (1, dz)) for n in range(2 * ITERS - 1)]
    final = jnp.broadcast_to(jnp.sum(reduced[1:2], axis=1, keepdims=True), (1, dz))
    sol, res = galerkin_coefficients(early + [final])
    for n, c in enumerate(sol + res):
        coefs[n : n + 1, :] = c


def combine_kernel(vu, wu, coefs, sol_v, res_v, sol_w, res_w):
    ecomp = sol_w.shape[0]
    lane_tiles = sol_w.shape[1] // coefs.shape[1]

    def wider(factor):
        return jnp.concatenate([factor] * lane_tiles, axis=1)

    solution = [coefs[n : n + 1, :] for n in range(ITERS)]
    residual = [coefs[ITERS + n : ITERS + n + 1, :] for n in range(ITERS + 1)]

    def combine(factors, terms):
        out = factors[0] * terms[0]
        for f, t in zip(factors[1:], terms[1:]):
            out = out + f * t
        return out

    shape = sol_v.shape
    flat = (shape[0] * shape[1] * shape[2], shape[3])
    v_terms = [vu[n].reshape(flat) for n in range(ITERS + 1)]
    w_terms = [wu[n] for n in range(ITERS + 1)]
    sol_v[...] = combine(solution, v_terms).reshape(shape)
    res_v[...] = combine(residual, v_terms).reshape(shape)
    sol_w[...] = combine([wider(f) for f in solution], w_terms)[:ecomp]
    res_w[...] = combine([wider(f) for f in residual], w_terms)[:ecomp]


def body(sizes, *args):
    load_v, load_w, shift, diag, off, coupling, kind, cell, node = args
    n_ea = sizes[2]
    total = sizes[0] * sizes[1] * sizes[2]
    groups = (AXES,) if total <= 64 else (("gx",), ("gy", "ea"))
    widest = total if total <= 64 else max(sizes[0], sizes[1] * sizes[2])
    comps, dx, dy, dz = load_v.shape
    ecomp, enb = load_w.shape
    cap = node.shape[2]
    vmem = pltpu.VMEM
    dma = pltpu.SemaphoreType.DMA
    epad = -(-ecomp // 16) * 16
    slots = n_ea * cap
    scratch = [
        vmem(load_w.shape, F32), vmem(shift.shape, F32), vmem(diag.shape, F32),
        vmem(off.shape, F32), vmem(coupling.shape, F32),
        vmem(cell.shape, jnp.int32), vmem((2,) + node.shape, jnp.int32),
        vmem((n_ea, comps, epad, cap), F32),
        vmem((n_ea, comps, epad, cap), F32),
        vmem((ecomp, epad, enb), F32),
        vmem((2 * dz, slots), BF16),
        vmem((dx * dy, slots), F32),
        vmem((dx * dy, slots), BF16),
        vmem((n_ea, enb, cap), BF16),
        vmem((enb, slots), BF16),
        vmem((dx, dy, dz), F32),
        vmem((n_ea, 2, 1, cap), jnp.int32),
        vmem((n_ea, comps, ecomp, cap), F32),
        vmem((ITERS, 2, comps, dy, dz), F32),
        vmem((ITERS, 2, comps, dx, 1, dz), F32),
        vmem((ITERS, 2, 8, dz), F32),
        vmem((n_ea, epad, enb), F32),
        vmem((ITERS, n_ea, comps, cap), F32),
        vmem((ITERS, n_ea, comps, cap), F32),
        vmem((ITERS, 2, 8, dz), F32),
        vmem((ITERS, n_ea, comps, cap), F32),
        vmem((ITERS, n_ea, comps, cap), F32),
        vmem((len(groups), widest, 2, dz), F32),
        vmem((len(groups), 2, dz), F32),
        dma((len(groups),)), dma((len(groups),)),
    ]
    basis = pl.pallas_call(
        functools.partial(kernel, sizes, groups),
        out_shape=(
            pltpu.VMEM((ITERS + 1,) + load_v.shape, F32),
            pltpu.VMEM((ITERS + 1, epad, enb), F32),
            pltpu.VMEM((2 * ITERS + 2, dz), F32),
        ),
        in_specs=[pl.BlockSpec(memory_space=pltpu.HBM)] * 9,
        out_specs=[pl.BlockSpec(memory_space=vmem)] * 3,
        scratch_shapes=scratch,
        compiler_params=pltpu.CompilerParams(
            collective_id=0, has_side_effects=True
        ),
        name="krylov",
    )(*args)
    return tuple(
        pl.pallas_call(
            combine_kernel,
            out_shape=tuple(
                jax.ShapeDtypeStruct(like.shape, F32)
                for like in (load_v, load_v, load_w, load_w)
            ),
            in_specs=[pl.BlockSpec(memory_space=vmem)] * 3,
            out_specs=[pl.BlockSpec(memory_space=vmem)] * 4,
            compiler_params=pltpu.CompilerParams(vmem_limit_bytes=8 << 20),
            name="combine",
        )(*basis)
    )


def solution(mesh):
    column = ("gx", "gy", "ea")
    placed = (
        P(None, "gx", "gy", "ea"),
        P(None, column),
        P("gx", "gy", "ea"),
        P(None, column),
        P(None, None, column),
        P(None, None, column),
        P(column, None, None),
        P(column, None, None),
        P(column, None, None),
    )
    return jax.shard_map(
        functools.partial(body, tuple(mesh.shape[a] for a in AXES)),
        mesh=mesh,
        in_specs=placed,
        out_specs=(
            P(None, "gx", "gy", "ea"),
            P(None, "gx", "gy", "ea"),
            P(None, column),
            P(None, column),
        ),
        check_vma=False,
    )
```

```python
import functools

import jax
import jax.numpy as jnp
from jax import lax
from jax.experimental import pallas as pl
from jax.experimental.pallas import tpu as pltpu
from jax.sharding import PartitionSpec as P

ITERS = 3
CENTRE = 11.5
AXES = ("gx", "gy", "ea")
MESH = pl.DeviceIdType.MESH
F32 = jnp.float32
BF16 = jnp.bfloat16


def pieces(x):
    high = x.astype(BF16)
    return high, (x - high.astype(F32)).astype(BF16)


def stacked(x):
    high, low = pieces(x)
    return jnp.concatenate([high, low], axis=0)


def folded(product):
    half = product.shape[0] // 2
    return product[:half] + product[half:]


def iota(shape, dim):
    return lax.broadcasted_iota(jnp.int32, shape, dim)


def times_transposed(a, b):
    return lax.dot_general(
        a, b, (((1,), (1,)), ((), ())), preferred_element_type=F32
    )


def galerkin_coefficients(moment):
    h = [moment[k + 1] + CENTRE * moment[k] for k in range(2 * ITERS - 1)]
    first = 1.0 / h[0]
    l1, l2 = h[1] * first, h[2] * first
    d1 = h[2] - l1 * h[1]
    e = h[3] - l1 * h[2]
    g1 = moment[1] - l1 * moment[0]
    second = 1.0 / d1
    k = e * second
    d2 = h[4] - l2 * h[2] - k * e
    y2 = (moment[2] - l2 * moment[0] - k * g1) / d2
    y1 = (g1 - e * y2) * second
    y0 = (moment[0] - h[1] * y1 - h[2] * y2) * first
    solution = [y0, y1, y2]
    residual = [
        1.0 - CENTRE * y0, -(y0 + CENTRE * y1), -(y1 + CENTRE * y2), -y2
    ]
    return solution, residual


def kernel(
    sizes, groups,
    load_v, load_w, shift_h, diag_h, off_h, coupling_h, kind_h, cell_h, node_h,
    vu, wu, coefs,
    w_first, shift, diag, off, coupling, cell, ids,
    weights, win, stiff, lanes, rows, rows_b, nodes_mine, nodes_t, overlap,
    centre_diag, ids_in, coup_in,
    x_in, y_in, z_in, w_in, p_in, s_in, z_out, p_out, s_out, red, red_out,
    red_s, red_r,
):
    n_gx, n_gy, n_ea = sizes
    comps, dx, dy, dz = load_v.shape
    ecomp, enb = load_w.shape
    epad = wu.shape[1]
    cap = cell.shape[2]
    per = dx * dy
    allrows = comps * per
    groups8 = allrows // 8
    gi, gj, ek = (lax.axis_index(a) for a in AXES)
    own = {"gx": gi, "gy": gj, "ea": ek}
    count = dict(zip(AXES, sizes))

    def members(group):
        total = 1
        for a in group:
            total *= count[a]
        me = 0
        for a in group:
            me = me * count[a] + own[a]

        def target(d):
            flat = lax.rem(me + d, total)
            coords = dict(own)
            for a in reversed(group):
                coords[a] = lax.rem(flat, count[a])
                flat = lax.div(flat, count[a])
            return tuple(coords[a] for a in AXES)

        return total, me, target

    def remote(src, dst, s_sem, r_sem, device):
        return pltpu.make_async_remote_copy(
            src_ref=src, dst_ref=dst, send_sem=s_sem, recv_sem=r_sem,
            device_id=device, device_id_type=MESH,
        )

    def landed(ref, sem):
        pltpu.make_async_copy(ref, ref, sem).wait()

    def red_start(stage, group):
        total, me, target = members(group)
        for d in range(total - 1):
            dst = red.at[stage, me]
            ends = (red_s.at[stage], red_r.at[stage])
            if group == AXES:
                pltpu.make_async_remote_copy(
                    src_ref=red_out.at[stage], dst_ref=dst, send_sem=ends[0], recv_sem=ends[1],
                    device_id=d + jnp.where(me <= d, 1, 0),
                    device_id_type=pl.DeviceIdType.LOGICAL,
                ).start()
            else:
                remote(red_out.at[stage], dst, *ends, target(d + 1)).start()
        red[stage, me] = red_out[stage]

    def steps(
        load_s, ids_s, ids_r, coup_s, coup_r, x_s, x_r, y_s, y_r, z_s, z_r,
        w_s, w_r, p_s, p_r, s_s, s_r,
    ):
        has = {
            ("gx", 1): gi < n_gx - 1, ("gx", -1): gi > 0,
            ("gy", 1): gj < n_gy - 1, ("gy", -1): gj > 0,
            ("ea", 1): ek < n_ea - 1, ("ea", -1): ek > 0,
        }
        beside = {
            ("gx", s): (gi + s, gj, ek) for s in (1, -1)
        } | {("gy", s): (gi, gj + s, ek) for s in (1, -1)} | {
            ("ea", s): (gi, gj, ek + s) for s in (1, -1)
        }
        slot = {1: 0, -1: 1}
        sides = {
            name: jnp.where(has[name, 1], 1, 0) + jnp.where(has[name, -1], 1, 0) for name in AXES
        }


        barrier = pltpu.get_barrier_semaphore()
        wide = n_gx - 1 > ITERS
        expected = 0
        for group in groups if wide else (("gy", "ea"),):
            total, _, target = members(group)
            for d in range(1, total):
                pl.semaphore_signal(barrier, inc=1, device_id=target(d), device_id_type=MESH)
            expected += total - 1
        if not wide:
            for s in (1, -1):
                @pl.when(has["gx", s])
                def _():
                    pl.semaphore_signal(
                        barrier, inc=1, device_id=beside["gx", s], device_id_type=MESH
                    )
                expected = expected + jnp.where(has["gx", s], 1, 0)

        loads = {}
        for at, (name, src, dst) in enumerate((
            ("w", load_w, w_first), ("node", node_h, ids.at[0]), ("kind", kind_h, ids.at[1]),
            ("v", load_v, vu.at[0]), ("cell", cell_h, cell), ("coupling", coupling_h, coupling),
            ("shift", shift_h, shift), ("off", off_h, off), ("diag", diag_h, diag),
        )):
            at = 1 if name == "kind" else at
            loads[name] = pltpu.make_async_copy(src, dst, load_s.at[at])
            loads[name].start()

        for s in (1, -1):
            for name, buffer in (("gx", x_in), ("gy", y_in), ("ea", z_in)):
                @pl.when(jnp.logical_not(has[name, -s]))
                def _():
                    for op in range(ITERS):
                        buffer[op, slot[s]] = jnp.zeros(buffer.shape[2:], F32)

        def partner(d):
            return lax.rem(ek + d, n_ea)

        def x_copy(op, s):
            return remote(
                vu.at[op, :, dx - 1 if s == 1 else 0], x_in.at[op, slot[s]],
                x_s.at[0], x_r.at[op], beside["gx", s],
            )

        def y_copy(op, s):
            edge = dy - 1 if s == 1 else 0
            return remote(
                vu.at[op, :, :, edge : edge + 1, :], y_in.at[op, slot[s]],
                y_s.at[0], y_r.at[op], beside["gy", s],
            )

        def z_copy(op, s):
            return remote(
                z_out.at[op, slot[s]], z_in.at[op, slot[s]],
                z_s.at[0], z_r.at[op], beside["ea", s],
            )

        def column_copy(src, dst, s_sem, r_sem, d):
            return remote(src, dst.at[ek], s_sem, r_sem, (gi, gj, partner(d)))

        def w_copy(d):
            return column_copy(wu.at[0], w_in, w_s.at[0], w_r.at[0], d)

        def p_copy(op, d):
            return column_copy(
                p_out.at[op, partner(d)], p_in.at[op], p_s.at[0], p_r.at[op], d
            )

        def s_copy(op, d):
            return column_copy(
                s_out.at[op, partner(d)], s_in.at[op], s_s.at[0], s_r.at[op], d
            )

        def ids_copy(d):
            return column_copy(
                ids.at[:, 0, pl.ds(partner(d), 1), :], ids_in, ids_s.at[0], ids_r.at[0], d
            )

        def block(d):
            return pl.ds(pl.multiple_of(partner(d) * cap, cap), cap)

        def coup_copy(d):
            return column_copy(
                coupling.at[:, :, block(d)], coup_in, coup_s.at[0], coup_r.at[0], d
            )

        def column_send(copy):
            for d in range(1, n_ea):
                copy(d).start()

        lane_i = iota((8, dz), 1)
        lane_r = iota((1, dz), 1)
        row_i = iota((dy, dz), 0)
        lane_b = iota((dy, dz), 1)

        def slabs(o):
            return slice(o * cap, (o + 1) * cap)

        def xy_send(op):
            for s in (1, -1):
                for name, copy in (("gx", x_copy), ("gy", y_copy)):
                    @pl.when(has[name, s])
                    def _():
                        copy(op, s).start()

        def z_send(op):
            v2 = vu[op].reshape(allrows, dz)
            up = jnp.zeros((8, dz), F32)
            down = jnp.zeros((8, dz), F32)
            for g in range(groups8):
                part = v2[8 * g : 8 * g + 8]
                up = jnp.where(lane_i == g, part[:, dz - 1 : dz], up)
                down = jnp.where(lane_i == g, part[:, 0:1], down)
            z_out[op, 0] = up
            z_out[op, 1] = down
            for s in (1, -1):
                @pl.when(has["ea", s])
                def _():
                    z_copy(op, s).start()

        def by_sides(name, two, one, sem):
            @pl.when(sides[name] == 2)
            def _():
                landed(two, sem)

            @pl.when(sides[name] == 1)
            def _():
                landed(one, sem)

        def x_wait(op):
            by_sides("gx", x_in.at[op], x_in.at[op, 0], x_r.at[op])

        def yz_wait(op):
            by_sides("gy", y_in.at[op], y_in.at[op, 0], y_r.at[op])
            by_sides("ea", z_in.at[op], z_in.at[op, 0], z_r.at[op])

        def pick(op):
            h, l = pieces(vu[op].reshape(allrows, dz))
            seen = jnp.dot(
                jnp.concatenate([h, l], axis=1), lanes[...], preferred_element_type=F32
            )
            return [
                jnp.sum(seen[i * per : (i + 1) * per] * rows[...], axis=0, keepdims=True)
                for i in range(comps)
            ]

        def pick_send(op):
            picked = pick(op)
            for i in range(comps):
                for o in range(n_ea):
                    p_out[op, o, i : i + 1, :] = picked[i][:, slabs(o)]
            column_send(functools.partial(p_copy, op))

        def local(op):
            v4 = vu[op]
            v2 = v4.reshape(allrows, dz)
            zero = jnp.zeros((comps, 1, dy, dz), F32)
            near = jnp.concatenate([zero, v4[:, : dx - 1]], axis=1) + jnp.concatenate(
                [v4[:, 1:], zero], axis=1
            )
            near = near.reshape(allrows, dz)
            lane_all = iota((allrows, dz), 1)
            row_all = lax.rem(iota((allrows, dz), 0), dy)
            near = near + jnp.where(lane_all == 0, 0.0, pltpu.roll(v2, 1, 1))
            near = near + jnp.where(lane_all == dz - 1, 0.0, pltpu.roll(v2, dz - 1, 1))
            near = near + jnp.where(row_all == 0, 0.0, pltpu.roll(v2, 1, 0))
            near = near + jnp.where(row_all == dy - 1, 0.0, pltpu.roll(v2, allrows - 1, 0))
            vu[op + 1] = centre_diag[...][None] * v4 - near.reshape(v4.shape)

        def local_nodes(op):
            w = wu[op]
            acc = stiff[0] * w[0:1]
            for p in range(1, ecomp):
                acc = acc + stiff[p] * w[p : p + 1]
            wu[op + 1] = acc

        def product(op_a, op_b):
            pv = jnp.sum((vu[op_a] * vu[op_b]).reshape(groups8, 8, dz), axis=0)
            pw = jnp.sum(wu[op_a] * wu[op_b], axis=0, keepdims=True)
            total = jnp.sum(pv, axis=0, keepdims=True)
            for b in range(enb // dz):
                total = total + pw[:, b * dz : (b + 1) * dz]
            return total

        def picks_wait(op):
            p_in[op, ek] = p_out[op, ek]
            landed(p_in.at[op, : n_ea - 1], p_r.at[op])

        def slot_terms(op):
            terms = []
            for o in range(n_ea):
                total = None
                for i in range(comps):
                    term = win[o, i] * p_in[op, o, i : i + 1, :]
                    total = term if total is None else total + term
                terms.append(total)
            return stacked(jnp.concatenate(terms, axis=1))

        def nodes_step(op, terms):
            wu[op + 1] += folded(times_transposed(terms, nodes_t[...]))

        def at_slots(op):
            return folded(jnp.dot(stacked(wu[op]), nodes_t[...], preferred_element_type=F32))

        def sums_send(op, values):
            for o in range(n_ea):
                for i in range(comps):
                    s_out[op, o, i : i + 1, :] = jnp.sum(
                        win[o, i] * values[:, slabs(o)], axis=0, keepdims=True
                    )
            column_send(functools.partial(s_copy, op))

        def first_sums():
            w_in[ek] = wu[0]
            landed(w_in.at[: n_ea - 1], w_r.at[0])
            for o in range(n_ea):
                values = folded(jnp.dot(stacked(w_in[o]), nodes_mine[o], preferred_element_type=F32))
                for i in range(comps):
                    s_in[0, o, i : i + 1, :] = jnp.sum(
                        weights[o, i] * values, axis=0, keepdims=True
                    )

        def sums_wait(op):
            s_in[op, ek] = s_out[op, ek]
            landed(s_in.at[op, : n_ea - 1], s_r.at[op])

        def cells_step(op):
            spread_h, spread_l = [], []
            for i in range(comps):
                line = jnp.concatenate([s_in[op, o, i : i + 1, :] for o in range(n_ea)], axis=1)
                h, l = pieces(line)
                spread_h.append(rows_b[...] * h)
                spread_l.append(rows_b[...] * l)
            added = folded(
                times_transposed(jnp.concatenate(spread_h + spread_l, axis=0), lanes[:dz, :])
            )
            vu[op + 1] += added.reshape(comps, dx, dy, dz)

        def yz_apply(op):
            z_low, z_high = z_in[op, 0], z_in[op, 1]
            for i in range(comps):
                for a in range(dx):
                    at = i * dx + a
                    side = jnp.where(row_i == 0, y_in[op, 0, i, a], 0.0)
                    side = side + jnp.where(row_i == dy - 1, y_in[op, 1, i, a], 0.0)
                    z_l, z_h = [], []
                    for b in range(dy // 8):
                        g = at * (dy // 8) + b
                        z_l.append(jnp.broadcast_to(z_low[:, g : g + 1], (8, dz)))
                        z_h.append(jnp.broadcast_to(z_high[:, g : g + 1], (8, dz)))
                    side = side + jnp.where(lane_b == 0, jnp.concatenate(z_l, axis=0), 0.0)
                    side = side + jnp.where(lane_b == dz - 1, jnp.concatenate(z_h, axis=0), 0.0)
                    vu[op + 1, i, a] -= side

        def x_apply(op):
            vu[op + 1, :, 0] -= x_in[op, 0]
            vu[op + 1, :, dx - 1] -= x_in[op, 1]

        def near_moment(op):
            y = y_in[op, 0] * vu[op, :, :, 0:1] + y_in[op, 1] * vu[op, :, :, dy - 1 : dy]
            z = z_out[op, 1] * z_in[op, 0] + z_out[op, 0] * z_in[op, 1]
            side = jnp.sum(y.reshape(comps * dx, dz), axis=0, keepdims=True)
            return side + jnp.sum(z, axis=0, keepdims=True)

        def slot_moment(op):
            cross = None
            for o in range(n_ea):
                term = p_in[op, o] * s_out[op, o]
                cross = term if cross is None else cross + term
            return jnp.sum(cross, axis=0, keepdims=True)

        def far_moment(op):
            x = x_in[op, 0] * vu[op, :, 0] + x_in[op, 1] * vu[op, :, dx - 1]
            return jnp.sum(x.reshape(comps * dy, dz), axis=0, keepdims=True)

        loads["w"].wait()
        wu[0] = jnp.concatenate([w_first[...], jnp.zeros((epad - ecomp, enb), F32)], axis=0)
        landed(ids, load_s.at[1])

        pl.semaphore_wait(barrier, expected)

        column_send(ids_copy)
        column_send(w_copy)
        loads["v"].wait()
        xy_send(0)
        z_send(0)
        loads["cell"].wait()
        tile = cell[0]
        tile_row = lax.div(tile, dz)
        tile_lane = tile - tile_row * dz
        for o in range(n_ea):
            hot = jnp.where(
                iota((dz, cap), 0) == tile_lane[o : o + 1], 1.0, 0.0
            ).astype(BF16)
            lanes[:dz, slabs(o)] = hot
            lanes[dz:, slabs(o)] = hot
            r = jnp.where(iota((per, cap), 0) == tile_row[o : o + 1], 1.0, 0.0)
            rows[:, slabs(o)] = r
            rows_b[:, slabs(o)] = r.astype(BF16)
        pick_send(0)
        loads["coupling"].wait()
        column_send(coup_copy)

        for o in range(n_ea):
            nodes_mine[o] = jnp.where(
                iota((enb, cap), 0) == ids[0, 0, o : o + 1, :], 1.0, 0.0
            ).astype(BF16)
        no_row = jnp.zeros((epad - ecomp, cap), F32)

        def masked(raw, k):
            heavi = jnp.where(k >= 1, 1.0, 0.0)
            tip = jnp.where(k == 2, 1.0, 0.0)
            mask = jnp.where(iota((ecomp, cap), 0) < 3, heavi, tip)
            return jnp.concatenate([raw * mask, no_row], axis=0)

        for o in range(n_ea):
            for i in range(comps):
                weights[o, i] = masked(coupling[i, :, slabs(o)], ids[1, 0, o : o + 1, :])
        loads["shift"].wait()
        centre_diag[...] = shift[...] + (6.0 - CENTRE)
        local(0)
        loads["off"].wait()
        loads["diag"].wait()
        for p in range(ecomp):
            whole = 0.5 * (off[p] + off[:, p, :])
            whole = jnp.where(iota((ecomp, enb), 0) == p, diag[p : p + 1, :] - CENTRE, whole)
            stiff[p] = jnp.concatenate([whole, jnp.zeros((epad - ecomp, enb), F32)], axis=0)
        local_nodes(0)
        moments = [product(0, 0)]
        ids_in[ek] = ids[:, 0, pl.ds(ek, 1), :]
        coup_in[ek] = coupling[:, :, block(0)]
        landed(ids_in.at[: n_ea - 1], ids_r.at[0])
        for o in range(n_ea):
            nodes_t[:, slabs(o)] = jnp.where(
                iota((enb, cap), 0) == ids_in[o, 0], 1.0, 0.0
            ).astype(BF16)
        own_rows = jnp.concatenate([ids_in[o, 0] for o in range(n_ea)], axis=0)
        own_columns = jnp.transpose(
            jnp.concatenate(
                [own_rows.astype(F32), jnp.zeros((cap - n_ea, cap), F32)], axis=0
            )
        ).astype(jnp.int32)
        yz_wait(0)
        yz_apply(0)
        for a in range(n_ea):
            for b in range(n_ea):
                overlap[slabs(a), slabs(b)] = jnp.where(
                    own_columns[:, a : a + 1] == own_rows[b : b + 1, :], 1.0, 0.0
                ).astype(BF16)
        first_sums()
        cells_step(0)
        x_wait(0)
        x_apply(0)
        xy_send(1)
        pick_send(1)
        values = at_slots(1)
        landed(coup_in.at[: n_ea - 1], coup_r.at[0])
        for o in range(n_ea):
            for i in range(comps):
                win[o, i] = masked(coup_in[o, i], ids_in[o, 1])
        picks_wait(0)
        terms = slot_terms(0)
        values = values + folded(
            jnp.dot(terms, overlap[...], preferred_element_type=F32)
        )
        sums_send(1, values)
        z_send(1)
        nodes_step(0, terms)
        last = ITERS - 1
        for op in range(1, last):
            local(op)
            local_nodes(op)
            moments.append(product(op - 1, op))
            moments.append(product(op, op))
            yz_wait(op)
            yz_apply(op)
            sums_wait(op)
            cells_step(op)
            x_wait(op)
            x_apply(op)
            xy_send(op + 1)
            pick_send(op + 1)
            z_send(op + 1)
            picks_wait(op)
            nodes_step(op, slot_terms(op))
            sums_send(op + 1, at_slots(op + 1))

        local(last)
        local_nodes(last)
        moments.append(product(last - 1, last))
        moments.append(product(last, last))
        row = product(last, last + 1)
        packed = jnp.zeros((1, dz), F32)
        for n, m in enumerate(moments):
            packed = jnp.where(lane_r == n, jnp.sum(m, axis=1, keepdims=True), packed)
        red_out[0, 0:1, :] = packed
        yz_wait(last)
        picks_wait(last)
        row = row - near_moment(last) + 2.0 * slot_moment(last)
        x_wait(last)
        red_out[0, 1:2, :] = row - far_moment(last)

        red_start(0, groups[0])
        nodes_step(last, slot_terms(last))
        yz_apply(last)
        x_apply(last)
        sums_wait(last)
        cells_step(last)
        for name, buffer, sem in (("gx", x_in, x_s), ("gy", y_in, y_s), ("ea", z_in, z_s)):
            by_sides(name, buffer, buffer.at[:, 0], sem.at[0])
        landed(p_in.at[:, : n_ea - 1], p_s.at[0])
        landed(s_in.at[1:, : n_ea - 1], s_s.at[0])
        landed(w_in.at[: n_ea - 1], w_s.at[0])
        landed(ids_in.at[: n_ea - 1], ids_s.at[0])
        landed(coup_in.at[: n_ea - 1], coup_s.at[0])

    dma = pltpu.SemaphoreType.DMA
    one, each = dma((1,)), dma((ITERS,))
    pl.run_scoped(
        steps, dma((9,)), one, one, one, one, one, each, one, each, one, each,
        one, one, one, each, one, each,
    )

    for stage, group in enumerate(groups):
        total = members(group)[0]
        if stage > 0:
            red_out[stage] = reduced
            red_start(stage, group)
        landed(red.at[stage, : total - 1], red_s.at[stage])
        landed(red.at[stage, : total - 1], red_r.at[stage])
        reduced = jnp.sum(red[stage, :total], axis=0)

    early = [jnp.broadcast_to(reduced[0:1, n : n + 1], (1, dz)) for n in range(2 * ITERS - 1)]
    final = jnp.broadcast_to(jnp.sum(reduced[1:2], axis=1, keepdims=True), (1, dz))
    sol, res = galerkin_coefficients(early + [final])
    for n, c in enumerate(sol + res):
        coefs[n : n + 1, :] = c


def combine_kernel(vu, wu, coefs, sol_v, res_v, sol_w, res_w):
    ecomp = sol_w.shape[0]
    lane_tiles = sol_w.shape[1] // coefs.shape[1]

    def wider(factor):
        return jnp.concatenate([factor] * lane_tiles, axis=1)

    solution = [coefs[n : n + 1, :] for n in range(ITERS)]
    residual = [coefs[ITERS + n : ITERS + n + 1, :] for n in range(ITERS + 1)]

    def combine(factors, terms):
        out = factors[0] * terms[0]
        for f, t in zip(factors[1:], terms[1:]):
            out = out + f * t
        return out

    shape = sol_v.shape
    flat = (shape[0] * shape[1] * shape[2], shape[3])
    v_terms = [vu[n].reshape(flat) for n in range(ITERS + 1)]
    w_terms = [wu[n] for n in range(ITERS + 1)]
    sol_v[...] = combine(solution, v_terms).reshape(shape)
    res_v[...] = combine(residual, v_terms).reshape(shape)
    sol_w[...] = combine([wider(f) for f in solution], w_terms)[:ecomp]
    res_w[...] = combine([wider(f) for f in residual], w_terms)[:ecomp]


def body(sizes, *args):
    load_v, load_w, shift, diag, off, coupling, kind, cell, node = args
    n_ea = sizes[2]
    total = sizes[0] * sizes[1] * sizes[2]
    groups = (AXES,) if total <= 64 else (("gx",), ("gy", "ea"))
    widest = total if total <= 64 else max(sizes[0], sizes[1] * sizes[2])
    comps, dx, dy, dz = load_v.shape
    ecomp, enb = load_w.shape
    cap = node.shape[2]
    vmem = pltpu.VMEM
    dma = pltpu.SemaphoreType.DMA
    epad = -(-ecomp // 16) * 16
    slots = n_ea * cap
    scratch = [
        vmem(load_w.shape, F32), vmem(shift.shape, F32), vmem(diag.shape, F32),
        vmem(off.shape, F32), vmem(coupling.shape, F32),
        vmem(cell.shape, jnp.int32), vmem((2,) + node.shape, jnp.int32),
        vmem((n_ea, comps, epad, cap), F32),
        vmem((n_ea, comps, epad, cap), F32),
        vmem((ecomp, epad, enb), F32),
        vmem((2 * dz, slots), BF16),
        vmem((dx * dy, slots), F32),
        vmem((dx * dy, slots), BF16),
        vmem((n_ea, enb, cap), BF16),
        vmem((enb, slots), BF16),
        vmem((slots, slots), BF16),
        vmem((dx, dy, dz), F32),
        vmem((n_ea, 2, 1, cap), jnp.int32),
        vmem((n_ea, comps, ecomp, cap), F32),
        vmem((ITERS, 2, comps, dy, dz), F32),
        vmem((ITERS, 2, comps, dx, 1, dz), F32),
        vmem((ITERS, 2, 8, dz), F32),
        vmem((n_ea, epad, enb), F32),
        vmem((ITERS, n_ea, comps, cap), F32),
        vmem((ITERS, n_ea, comps, cap), F32),
        vmem((ITERS, 2, 8, dz), F32),
        vmem((ITERS, n_ea, comps, cap), F32),
        vmem((ITERS, n_ea, comps, cap), F32),
        vmem((len(groups), widest, 2, dz), F32),
        vmem((len(groups), 2, dz), F32),
        dma((len(groups),)), dma((len(groups),)),
    ]
    basis = pl.pallas_call(
        functools.partial(kernel, sizes, groups),
        out_shape=(
            pltpu.VMEM((ITERS + 1,) + load_v.shape, F32),
            pltpu.VMEM((ITERS + 1, epad, enb), F32),
            pltpu.VMEM((2 * ITERS + 2, dz), F32),
        ),
        in_specs=[pl.BlockSpec(memory_space=pltpu.HBM)] * 9,
        out_specs=[pl.BlockSpec(memory_space=vmem)] * 3,
        scratch_shapes=scratch,
        compiler_params=pltpu.CompilerParams(
            collective_id=0, has_side_effects=True
        ),
        name="krylov",
    )(*args)
    return tuple(
        pl.pallas_call(
            combine_kernel,
            out_shape=tuple(
                jax.ShapeDtypeStruct(like.shape, F32)
                for like in (load_v, load_v, load_w, load_w)
            ),
            in_specs=[pl.BlockSpec(memory_space=vmem)] * 3,
            out_specs=[pl.BlockSpec(memory_space=vmem)] * 4,
            compiler_params=pltpu.CompilerParams(vmem_limit_bytes=8 << 20),
            name="combine",
        )(*basis)
    )


def solution(mesh):
    column = ("gx", "gy", "ea")
    placed = (
        P(None, "gx", "gy", "ea"),
        P(None, column),
        P("gx", "gy", "ea"),
        P(None, column),
        P(None, None, column),
        P(None, None, column),
        P(column, None, None),
        P(column, None, None),
        P(column, None, None),
    )
    return jax.shard_map(
        functools.partial(body, tuple(mesh.shape[a] for a in AXES)),
        mesh=mesh,
        in_specs=placed,
        out_specs=(
            P(None, "gx", "gy", "ea"),
            P(None, "gx", "gy", "ea"),
            P(None, column),
            P(None, column),
        ),
        check_vma=False,
    )
```

```python
import functools

import jax
import jax.numpy as jnp
from jax import lax
from jax.experimental import pallas as pl
from jax.experimental.pallas import tpu as pltpu
from jax.sharding import PartitionSpec as P

ITERS = 3
CENTRE = 11.5
AXES = ("gx", "gy", "ea")
MESH = pl.DeviceIdType.MESH
F32 = jnp.float32
BF16 = jnp.bfloat16


def pieces(x):
    high = x.astype(BF16)
    return high, (x - high.astype(F32)).astype(BF16)


def stacked(x):
    high, low = pieces(x)
    return jnp.concatenate([high, low], axis=0)


def folded(product):
    half = product.shape[0] // 2
    return product[:half] + product[half:]


def iota(shape, dim):
    return lax.broadcasted_iota(jnp.int32, shape, dim)


def times_transposed(a, b):
    return lax.dot_general(
        a, b, (((1,), (1,)), ((), ())), preferred_element_type=F32
    )


def galerkin_coefficients(moment):
    h = [moment[k + 1] + CENTRE * moment[k] for k in range(2 * ITERS - 1)]
    first = 1.0 / h[0]
    l1, l2 = h[1] * first, h[2] * first
    d1 = h[2] - l1 * h[1]
    e = h[3] - l1 * h[2]
    g1 = moment[1] - l1 * moment[0]
    second = 1.0 / d1
    k = e * second
    d2 = h[4] - l2 * h[2] - k * e
    y2 = (moment[2] - l2 * moment[0] - k * g1) / d2
    y1 = (g1 - e * y2) * second
    y0 = (moment[0] - h[1] * y1 - h[2] * y2) * first
    solution = [y0, y1, y2]
    residual = [
        1.0 - CENTRE * y0, -(y0 + CENTRE * y1), -(y1 + CENTRE * y2), -y2
    ]
    return solution, residual


def kernel(
    sizes, groups,
    load_v, load_w, shift_h, diag_h, off_h, coupling_h, kind_h, cell_h, node_h,
    vu, wu, coefs,
    w_first, shift, diag, off, coupling, cell, ids,
    weights, win, stiff, lanes, rows, rows_b, nodes_mine, nodes_t, overlap,
    centre_diag, ids_in, coup_in,
    x_in, y_in, z_in, w_in, p_in, s_in, z_out, p_out, s_out, red, red_out,
    red_s, red_r,
):
    n_gx, n_gy, n_ea = sizes
    comps, dx, dy, dz = load_v.shape
    ecomp, enb = load_w.shape
    epad = wu.shape[1]
    cap = cell.shape[2]
    per = dx * dy
    half = per // 2
    allrows = comps * per
    groups8 = allrows // 8
    gi, gj, ek = (lax.axis_index(a) for a in AXES)
    own = {"gx": gi, "gy": gj, "ea": ek}
    count = dict(zip(AXES, sizes))

    def members(group):
        total = 1
        for a in group:
            total *= count[a]
        me = 0
        for a in group:
            me = me * count[a] + own[a]

        def target(d):
            flat = lax.rem(me + d, total)
            coords = dict(own)
            for a in reversed(group):
                coords[a] = lax.rem(flat, count[a])
                flat = lax.div(flat, count[a])
            return tuple(coords[a] for a in AXES)

        return total, me, target

    def remote(src, dst, s_sem, r_sem, device):
        return pltpu.make_async_remote_copy(
            src_ref=src, dst_ref=dst, send_sem=s_sem, recv_sem=r_sem,
            device_id=device, device_id_type=MESH,
        )

    def landed(ref, sem):
        pltpu.make_async_copy(ref, ref, sem).wait()

    def red_start(stage, group):
        total, me, target = members(group)
        for d in range(total - 1):
            dst = red.at[stage, me]
            ends = (red_s.at[stage], red_r.at[stage])
            if group == AXES:
                pltpu.make_async_remote_copy(
                    src_ref=red_out.at[stage], dst_ref=dst, send_sem=ends[0], recv_sem=ends[1],
                    device_id=d + jnp.where(me <= d, 1, 0),
                    device_id_type=pl.DeviceIdType.LOGICAL,
                ).start()
            else:
                remote(red_out.at[stage], dst, *ends, target(d + 1)).start()
        red[stage, me] = red_out[stage]

    def steps(
        load_s, ids_s, ids_r, coup_s, coup_r, x_s, x_r, y_s, y_r, z_s, z_r,
        w_s, w_r, p_s, p_r, s_s, s_r,
    ):
        has = {
            ("gx", 1): gi < n_gx - 1, ("gx", -1): gi > 0,
            ("gy", 1): gj < n_gy - 1, ("gy", -1): gj > 0,
            ("ea", 1): ek < n_ea - 1, ("ea", -1): ek > 0,
        }
        beside = {
            ("gx", s): (gi + s, gj, ek) for s in (1, -1)
        } | {("gy", s): (gi, gj + s, ek) for s in (1, -1)} | {
            ("ea", s): (gi, gj, ek + s) for s in (1, -1)
        }
        slot = {1: 0, -1: 1}
        sides = {
            name: jnp.where(has[name, 1], 1, 0) + jnp.where(has[name, -1], 1, 0) for name in AXES
        }


        barrier = pltpu.get_barrier_semaphore()
        wide = n_gx - 1 > ITERS
        expected = 0
        for group in groups if wide else (("gy", "ea"),):
            total, _, target = members(group)
            for d in range(1, total):
                pl.semaphore_signal(barrier, inc=1, device_id=target(d), device_id_type=MESH)
            expected += total - 1
        if not wide:
            for s in (1, -1):
                @pl.when(has["gx", s])
                def _():
                    pl.semaphore_signal(
                        barrier, inc=1, device_id=beside["gx", s], device_id_type=MESH
                    )
                expected = expected + jnp.where(has["gx", s], 1, 0)

        loads = {}
        for at, (name, src, dst) in enumerate((
            ("w", load_w, w_first), ("node", node_h, ids.at[0]), ("kind", kind_h, ids.at[1]),
            ("v", load_v, vu.at[0]), ("cell", cell_h, cell), ("coupling", coupling_h, coupling),
            ("shift", shift_h, shift), ("off", off_h, off), ("diag", diag_h, diag),
        )):
            at = 1 if name == "kind" else at
            loads[name] = pltpu.make_async_copy(src, dst, load_s.at[at])
            loads[name].start()

        for s in (1, -1):
            for name, buffer in (("gx", x_in), ("gy", y_in), ("ea", z_in)):
                @pl.when(jnp.logical_not(has[name, -s]))
                def _():
                    for op in range(ITERS):
                        buffer[op, slot[s]] = jnp.zeros(buffer.shape[2:], F32)

        def partner(d):
            return lax.rem(ek + d, n_ea)

        def x_copy(op, s):
            return remote(
                vu.at[op, :, dx - 1 if s == 1 else 0], x_in.at[op, slot[s]],
                x_s.at[0], x_r.at[op], beside["gx", s],
            )

        def y_copy(op, s):
            edge = dy - 1 if s == 1 else 0
            return remote(
                vu.at[op, :, :, edge : edge + 1, :], y_in.at[op, slot[s]],
                y_s.at[0], y_r.at[op], beside["gy", s],
            )

        def z_copy(op, s):
            return remote(
                z_out.at[op, slot[s]], z_in.at[op, slot[s]],
                z_s.at[0], z_r.at[op], beside["ea", s],
            )

        def column_copy(src, dst, s_sem, r_sem, d):
            return remote(src, dst.at[ek], s_sem, r_sem, (gi, gj, partner(d)))

        def w_copy(d):
            return column_copy(wu.at[0], w_in, w_s.at[0], w_r.at[0], d)

        def p_copy(op, d):
            return column_copy(
                p_out.at[op, partner(d)], p_in.at[op], p_s.at[0], p_r.at[op], d
            )

        def s_copy(op, d):
            return column_copy(
                s_out.at[op, partner(d)], s_in.at[op], s_s.at[0], s_r.at[op], d
            )

        def ids_copy(d):
            return column_copy(
                ids.at[:, 0, pl.ds(partner(d), 1), :], ids_in, ids_s.at[0], ids_r.at[0], d
            )

        def block(d):
            return pl.ds(pl.multiple_of(partner(d) * cap, cap), cap)

        def coup_copy(d):
            return column_copy(
                coupling.at[:, :, block(d)], coup_in, coup_s.at[0], coup_r.at[0], d
            )

        def column_send(copy):
            for d in range(1, n_ea):
                copy(d).start()

        lane_i = iota((8, dz), 1)
        lane_r = iota((1, dz), 1)
        row_i = iota((dy, dz), 0)
        lane_b = iota((dy, dz), 1)

        def slabs(o):
            return slice(o * cap, (o + 1) * cap)

        def xy_send(op):
            for s in (1, -1):
                for name, copy in (("gx", x_copy), ("gy", y_copy)):
                    @pl.when(has[name, s])
                    def _():
                        copy(op, s).start()

        def z_send(op):
            v2 = vu[op].reshape(allrows, dz)
            up = jnp.zeros((8, dz), F32)
            down = jnp.zeros((8, dz), F32)
            for g in range(groups8):
                part = v2[8 * g : 8 * g + 8]
                up = jnp.where(lane_i == g, part[:, dz - 1 : dz], up)
                down = jnp.where(lane_i == g, part[:, 0:1], down)
            z_out[op, 0] = up
            z_out[op, 1] = down
            for s in (1, -1):
                @pl.when(has["ea", s])
                def _():
                    z_copy(op, s).start()

        def by_sides(name, two, one, sem):
            @pl.when(sides[name] == 2)
            def _():
                landed(two, sem)

            @pl.when(sides[name] == 1)
            def _():
                landed(one, sem)

        def x_wait(op):
            by_sides("gx", x_in.at[op], x_in.at[op, 0], x_r.at[op])

        def yz_wait(op):
            by_sides("gy", y_in.at[op], y_in.at[op, 0], y_r.at[op])
            by_sides("ea", z_in.at[op], z_in.at[op, 0], z_r.at[op])

        def pick(op):
            v3 = vu[op].reshape(comps, per, dz)
            folds = jnp.concatenate(
                [
                    jnp.concatenate([v3[i, :half], v3[i, half:]], axis=1)
                    for i in range(comps)
                ],
                axis=0,
            )
            h, l = pieces(folds)
            seen = jnp.dot(h, lanes[...], preferred_element_type=F32) + jnp.dot(
                l, lanes[...], preferred_element_type=F32
            )
            return [
                jnp.sum(seen[i * half : (i + 1) * half] * rows[...], axis=0, keepdims=True)
                for i in range(comps)
            ]

        def pick_send(op):
            picked = pick(op)
            for i in range(comps):
                for o in range(n_ea):
                    p_out[op, o, i : i + 1, :] = picked[i][:, slabs(o)]
            column_send(functools.partial(p_copy, op))

        def local(op):
            v4 = vu[op]
            v2 = v4.reshape(allrows, dz)
            zero = jnp.zeros((comps, 1, dy, dz), F32)
            near = jnp.concatenate([zero, v4[:, : dx - 1]], axis=1) + jnp.concatenate(
                [v4[:, 1:], zero], axis=1
            )
            near = near.reshape(allrows, dz)
            lane_all = iota((allrows, dz), 1)
            row_all = lax.rem(iota((allrows, dz), 0), dy)
            near = near + jnp.where(lane_all == 0, 0.0, pltpu.roll(v2, 1, 1))
            near = near + jnp.where(lane_all == dz - 1, 0.0, pltpu.roll(v2, dz - 1, 1))
            near = near + jnp.where(row_all == 0, 0.0, pltpu.roll(v2, 1, 0))
            near = near + jnp.where(row_all == dy - 1, 0.0, pltpu.roll(v2, allrows - 1, 0))
            vu[op + 1] = centre_diag[...][None] * v4 - near.reshape(v4.shape)

        def local_nodes(op):
            w = wu[op]
            acc = stiff[0] * w[0:1]
            for p in range(1, ecomp):
                acc = acc + stiff[p] * w[p : p + 1]
            wu[op + 1] = acc

        def product(op_a, op_b):
            pv = jnp.sum((vu[op_a] * vu[op_b]).reshape(groups8, 8, dz), axis=0)
            pw = jnp.sum(wu[op_a] * wu[op_b], axis=0, keepdims=True)
            total = jnp.sum(pv, axis=0, keepdims=True)
            for b in range(enb // dz):
                total = total + pw[:, b * dz : (b + 1) * dz]
            return total

        def picks_wait(op):
            p_in[op, ek] = p_out[op, ek]
            landed(p_in.at[op, : n_ea - 1], p_r.at[op])

        def slot_terms(op):
            terms = []
            for o in range(n_ea):
                total = None
                for i in range(comps):
                    term = win[o, i] * p_in[op, o, i : i + 1, :]
                    total = term if total is None else total + term
                terms.append(total)
            return stacked(jnp.concatenate(terms, axis=1))

        def nodes_step(op, terms):
            wu[op + 1] += folded(times_transposed(terms, nodes_t[...]))

        def at_slots(op):
            return folded(jnp.dot(stacked(wu[op]), nodes_t[...], preferred_element_type=F32))

        def sums_send(op, values):
            for o in range(n_ea):
                for i in range(comps):
                    s_out[op, o, i : i + 1, :] = jnp.sum(
                        win[o, i] * values[:, slabs(o)], axis=0, keepdims=True
                    )
            column_send(functools.partial(s_copy, op))

        def first_sums():
            w_in[ek] = wu[0]
            landed(w_in.at[: n_ea - 1], w_r.at[0])
            for o in range(n_ea):
                values = folded(jnp.dot(stacked(w_in[o]), nodes_mine[o], preferred_element_type=F32))
                for i in range(comps):
                    s_in[0, o, i : i + 1, :] = jnp.sum(
                        weights[o, i] * values, axis=0, keepdims=True
                    )

        def sums_wait(op):
            s_in[op, ek] = s_out[op, ek]
            landed(s_in.at[op, : n_ea - 1], s_r.at[op])

        def cells_step(op):
            spread_h, spread_l = [], []
            for i in range(comps):
                line = jnp.concatenate([s_in[op, o, i : i + 1, :] for o in range(n_ea)], axis=1)
                h, l = pieces(line)
                spread_h.append(rows_b[...] * h)
                spread_l.append(rows_b[...] * l)
            added = times_transposed(
                jnp.concatenate(spread_h, axis=0), lanes[...]
            ) + times_transposed(jnp.concatenate(spread_l, axis=0), lanes[...])
            for i in range(comps):
                for a in range(dx):
                    at = a * dy
                    part = at // half
                    low = i * half + at - part * half
                    vu[op + 1, i, a] += added[low : low + dy, part * dz : (part + 1) * dz]

        def yz_apply(op):
            z_low, z_high = z_in[op, 0], z_in[op, 1]
            for i in range(comps):
                for a in range(dx):
                    at = i * dx + a
                    side = jnp.where(row_i == 0, y_in[op, 0, i, a], 0.0)
                    side = side + jnp.where(row_i == dy - 1, y_in[op, 1, i, a], 0.0)
                    z_l, z_h = [], []
                    for b in range(dy // 8):
                        g = at * (dy // 8) + b
                        z_l.append(jnp.broadcast_to(z_low[:, g : g + 1], (8, dz)))
                        z_h.append(jnp.broadcast_to(z_high[:, g : g + 1], (8, dz)))
                    side = side + jnp.where(lane_b == 0, jnp.concatenate(z_l, axis=0), 0.0)
                    side = side + jnp.where(lane_b == dz - 1, jnp.concatenate(z_h, axis=0), 0.0)
                    vu[op + 1, i, a] -= side

        def x_apply(op):
            vu[op + 1, :, 0] -= x_in[op, 0]
            vu[op + 1, :, dx - 1] -= x_in[op, 1]

        def near_moment(op):
            y = y_in[op, 0] * vu[op, :, :, 0:1] + y_in[op, 1] * vu[op, :, :, dy - 1 : dy]
            z = z_out[op, 1] * z_in[op, 0] + z_out[op, 0] * z_in[op, 1]
            side = jnp.sum(y.reshape(comps * dx, dz), axis=0, keepdims=True)
            return side + jnp.sum(z, axis=0, keepdims=True)

        def slot_moment(op):
            cross = None
            for o in range(n_ea):
                term = p_in[op, o] * s_out[op, o]
                cross = term if cross is None else cross + term
            return jnp.sum(cross, axis=0, keepdims=True)

        def far_moment(op):
            x = x_in[op, 0] * vu[op, :, 0] + x_in[op, 1] * vu[op, :, dx - 1]
            return jnp.sum(x.reshape(comps * dy, dz), axis=0, keepdims=True)

        loads["w"].wait()
        wu[0] = jnp.concatenate([w_first[...], jnp.zeros((epad - ecomp, enb), F32)], axis=0)
        landed(ids, load_s.at[1])

        pl.semaphore_wait(barrier, expected)

        column_send(ids_copy)
        column_send(w_copy)
        loads["v"].wait()
        xy_send(0)
        z_send(0)
        loads["cell"].wait()
        tile = cell[0]
        tile_row = lax.div(tile, dz)
        tile_lane = tile - tile_row * dz
        for o in range(n_ea):
            here = tile_lane[o : o + 1] + jnp.where(tile_row[o : o + 1] >= half, dz, 0)
            lanes[:, slabs(o)] = jnp.where(
                iota((2 * dz, cap), 0) == here, 1.0, 0.0
            ).astype(BF16)
            below = lax.rem(tile_row[o : o + 1], half)
            r = jnp.where(iota((half, cap), 0) == below, 1.0, 0.0)
            rows[:, slabs(o)] = r
            rows_b[:, slabs(o)] = r.astype(BF16)
        pick_send(0)
        loads["coupling"].wait()
        column_send(coup_copy)

        for o in range(n_ea):
            nodes_mine[o] = jnp.where(
                iota((enb, cap), 0) == ids[0, 0, o : o + 1, :], 1.0, 0.0
            ).astype(BF16)
        no_row = jnp.zeros((epad - ecomp, cap), F32)

        def masked(raw, k):
            heavi = jnp.where(k >= 1, 1.0, 0.0)
            tip = jnp.where(k == 2, 1.0, 0.0)
            mask = jnp.where(iota((ecomp, cap), 0) < 3, heavi, tip)
            return jnp.concatenate([raw * mask, no_row], axis=0)

        for o in range(n_ea):
            for i in range(comps):
                weights[o, i] = masked(coupling[i, :, slabs(o)], ids[1, 0, o : o + 1, :])
        loads["shift"].wait()
        centre_diag[...] = shift[...] + (6.0 - CENTRE)
        local(0)
        loads["off"].wait()
        loads["diag"].wait()
        for p in range(ecomp):
            whole = 0.5 * (off[p] + off[:, p, :])
            whole = jnp.where(iota((ecomp, enb), 0) == p, diag[p : p + 1, :] - CENTRE, whole)
            stiff[p] = jnp.concatenate([whole, jnp.zeros((epad - ecomp, enb), F32)], axis=0)
        local_nodes(0)
        moments = [product(0, 0)]
        ids_in[ek] = ids[:, 0, pl.ds(ek, 1), :]
        coup_in[ek] = coupling[:, :, block(0)]
        landed(ids_in.at[: n_ea - 1], ids_r.at[0])
        for o in range(n_ea):
            nodes_t[:, slabs(o)] = jnp.where(
                iota((enb, cap), 0) == ids_in[o, 0], 1.0, 0.0
            ).astype(BF16)
        own_rows = jnp.concatenate([ids_in[o, 0] for o in range(n_ea)], axis=0)
        own_columns = jnp.transpose(
            jnp.concatenate(
                [own_rows.astype(F32), jnp.zeros((cap - n_ea, cap), F32)], axis=0
            )
        ).astype(jnp.int32)
        yz_wait(0)
        yz_apply(0)
        first_sums()
        cells_step(0)
        x_wait(0)
        x_apply(0)
        xy_send(1)
        for a in range(n_ea):
            for b in range(n_ea):
                overlap[slabs(a), slabs(b)] = jnp.where(
                    own_columns[:, a : a + 1] == own_rows[b : b + 1, :], 1.0, 0.0
                ).astype(BF16)
        values = at_slots(1)
        landed(coup_in.at[: n_ea - 1], coup_r.at[0])
        for o in range(n_ea):
            for i in range(comps):
                win[o, i] = masked(coup_in[o, i], ids_in[o, 1])
        picks_wait(0)
        terms = slot_terms(0)
        values = values + folded(
            jnp.dot(terms, overlap[...], preferred_element_type=F32)
        )
        sums_send(1, values)
        z_send(1)
        pick_send(1)
        nodes_step(0, terms)
        last = ITERS - 1
        for op in range(1, last):
            local(op)
            local_nodes(op)
            moments.append(product(op - 1, op))
            moments.append(product(op, op))
            yz_wait(op)
            yz_apply(op)
            sums_wait(op)
            cells_step(op)
            x_wait(op)
            x_apply(op)
            xy_send(op + 1)
            pick_send(op + 1)
            z_send(op + 1)
            picks_wait(op)
            nodes_step(op, slot_terms(op))
            sums_send(op + 1, at_slots(op + 1))

        local(last)
        local_nodes(last)
        moments.append(product(last - 1, last))
        moments.append(product(last, last))
        row = product(last, last + 1)
        packed = jnp.zeros((1, dz), F32)
        for n, m in enumerate(moments):
            packed = jnp.where(lane_r == n, jnp.sum(m, axis=1, keepdims=True), packed)
        red_out[0, 0:1, :] = packed
        yz_wait(last)
        picks_wait(last)
        row = row - near_moment(last) + 2.0 * slot_moment(last)
        x_wait(last)
        red_out[0, 1:2, :] = row - far_moment(last)

        red_start(0, groups[0])
        nodes_step(last, slot_terms(last))
        yz_apply(last)
        x_apply(last)
        sums_wait(last)
        cells_step(last)
        for name, buffer, sem in (("gx", x_in, x_s), ("gy", y_in, y_s), ("ea", z_in, z_s)):
            by_sides(name, buffer, buffer.at[:, 0], sem.at[0])
        landed(p_in.at[:, : n_ea - 1], p_s.at[0])
        landed(s_in.at[1:, : n_ea - 1], s_s.at[0])
        landed(w_in.at[: n_ea - 1], w_s.at[0])
        landed(ids_in.at[: n_ea - 1], ids_s.at[0])
        landed(coup_in.at[: n_ea - 1], coup_s.at[0])

    dma = pltpu.SemaphoreType.DMA
    one, each = dma((1,)), dma((ITERS,))
    pl.run_scoped(
        steps, dma((9,)), one, one, one, one, one, each, one, each, one, each,
        one, one, one, each, one, each,
    )

    for stage, group in enumerate(groups):
        total = members(group)[0]
        if stage > 0:
            red_out[stage] = reduced
            red_start(stage, group)
        landed(red.at[stage, : total - 1], red_s.at[stage])
        landed(red.at[stage, : total - 1], red_r.at[stage])
        reduced = jnp.sum(red[stage, :total], axis=0)

    early = [jnp.broadcast_to(reduced[0:1, n : n + 1], (1, dz)) for n in range(2 * ITERS - 1)]
    final = jnp.broadcast_to(jnp.sum(reduced[1:2], axis=1, keepdims=True), (1, dz))
    sol, res = galerkin_coefficients(early + [final])
    for n, c in enumerate(sol + res):
        coefs[n : n + 1, :] = c


def combine_kernel(vu, wu, coefs, sol_v, res_v, sol_w, res_w):
    ecomp = sol_w.shape[0]
    lane_tiles = sol_w.shape[1] // coefs.shape[1]

    def wider(factor):
        return jnp.concatenate([factor] * lane_tiles, axis=1)

    solution = [coefs[n : n + 1, :] for n in range(ITERS)]
    residual = [coefs[ITERS + n : ITERS + n + 1, :] for n in range(ITERS + 1)]

    def combine(factors, terms):
        out = factors[0] * terms[0]
        for f, t in zip(factors[1:], terms[1:]):
            out = out + f * t
        return out

    shape = sol_v.shape
    flat = (shape[0] * shape[1] * shape[2], shape[3])
    v_terms = [vu[n].reshape(flat) for n in range(ITERS + 1)]
    w_terms = [wu[n] for n in range(ITERS + 1)]
    sol_v[...] = combine(solution, v_terms).reshape(shape)
    res_v[...] = combine(residual, v_terms).reshape(shape)
    sol_w[...] = combine([wider(f) for f in solution], w_terms)[:ecomp]
    res_w[...] = combine([wider(f) for f in residual], w_terms)[:ecomp]


def body(sizes, *args):
    load_v, load_w, shift, diag, off, coupling, kind, cell, node = args
    n_ea = sizes[2]
    total = sizes[0] * sizes[1] * sizes[2]
    groups = (AXES,) if total <= 64 else (("gx",), ("gy", "ea"))
    widest = total if total <= 64 else max(sizes[0], sizes[1] * sizes[2])
    comps, dx, dy, dz = load_v.shape
    ecomp, enb = load_w.shape
    cap = node.shape[2]
    vmem = pltpu.VMEM
    dma = pltpu.SemaphoreType.DMA
    epad = -(-ecomp // 16) * 16
    slots = n_ea * cap
    scratch = [
        vmem(load_w.shape, F32), vmem(shift.shape, F32), vmem(diag.shape, F32),
        vmem(off.shape, F32), vmem(coupling.shape, F32),
        vmem(cell.shape, jnp.int32), vmem((2,) + node.shape, jnp.int32),
        vmem((n_ea, comps, epad, cap), F32),
        vmem((n_ea, comps, epad, cap), F32),
        vmem((ecomp, epad, enb), F32),
        vmem((2 * dz, slots), BF16),
        vmem((dx * dy // 2, slots), F32),
        vmem((dx * dy // 2, slots), BF16),
        vmem((n_ea, enb, cap), BF16),
        vmem((enb, slots), BF16),
        vmem((slots, slots), BF16),
        vmem((dx, dy, dz), F32),
        vmem((n_ea, 2, 1, cap), jnp.int32),
        vmem((n_ea, comps, ecomp, cap), F32),
        vmem((ITERS, 2, comps, dy, dz), F32),
        vmem((ITERS, 2, comps, dx, 1, dz), F32),
        vmem((ITERS, 2, 8, dz), F32),
        vmem((n_ea, epad, enb), F32),
        vmem((ITERS, n_ea, comps, cap), F32),
        vmem((ITERS, n_ea, comps, cap), F32),
        vmem((ITERS, 2, 8, dz), F32),
        vmem((ITERS, n_ea, comps, cap), F32),
        vmem((ITERS, n_ea, comps, cap), F32),
        vmem((len(groups), widest, 2, dz), F32),
        vmem((len(groups), 2, dz), F32),
        dma((len(groups),)), dma((len(groups),)),
    ]
    basis = pl.pallas_call(
        functools.partial(kernel, sizes, groups),
        out_shape=(
            pltpu.VMEM((ITERS + 1,) + load_v.shape, F32),
            pltpu.VMEM((ITERS + 1, epad, enb), F32),
            pltpu.VMEM((2 * ITERS + 2, dz), F32),
        ),
        in_specs=[pl.BlockSpec(memory_space=pltpu.HBM)] * 9,
        out_specs=[pl.BlockSpec(memory_space=vmem)] * 3,
        scratch_shapes=scratch,
        compiler_params=pltpu.CompilerParams(
            collective_id=0, has_side_effects=True
        ),
        name="krylov",
    )(*args)
    return tuple(
        pl.pallas_call(
            combine_kernel,
            out_shape=tuple(
                jax.ShapeDtypeStruct(like.shape, F32)
                for like in (load_v, load_v, load_w, load_w)
            ),
            in_specs=[pl.BlockSpec(memory_space=vmem)] * 3,
            out_specs=[pl.BlockSpec(memory_space=vmem)] * 4,
            compiler_params=pltpu.CompilerParams(vmem_limit_bytes=8 << 20),
            name="combine",
        )(*basis)
    )


def solution(mesh):
    column = ("gx", "gy", "ea")
    placed = (
        P(None, "gx", "gy", "ea"),
        P(None, column),
        P("gx", "gy", "ea"),
        P(None, column),
        P(None, None, column),
        P(None, None, column),
        P(column, None, None),
        P(column, None, None),
        P(column, None, None),
    )
    return jax.shard_map(
        functools.partial(body, tuple(mesh.shape[a] for a in AXES)),
        mesh=mesh,
        in_specs=placed,
        out_specs=(
            P(None, "gx", "gy", "ea"),
            P(None, "gx", "gy", "ea"),
            P(None, column),
            P(None, column),
        ),
        check_vma=False,
    )
```

```python
import functools

import jax
import jax.numpy as jnp
from jax import lax
from jax.experimental import pallas as pl
from jax.experimental.pallas import tpu as pltpu
from jax.sharding import PartitionSpec as P

ITERS = 3
CENTRE = 11.5
AXES = ("gx", "gy", "ea")
MESH = pl.DeviceIdType.MESH
F32 = jnp.float32
BF16 = jnp.bfloat16


def pieces(x):
    high = x.astype(BF16)
    return high, (x - high.astype(F32)).astype(BF16)


def stacked(x):
    high, low = pieces(x)
    return jnp.concatenate([high, low], axis=0)


def folded(product):
    half = product.shape[0] // 2
    return product[:half] + product[half:]


def iota(shape, dim):
    return lax.broadcasted_iota(jnp.int32, shape, dim)


def times_transposed(a, b):
    return lax.dot_general(
        a, b, (((1,), (1,)), ((), ())), preferred_element_type=F32
    )


def galerkin_coefficients(moment):
    h = [moment[k + 1] + CENTRE * moment[k] for k in range(2 * ITERS - 1)]
    first = 1.0 / h[0]
    l1, l2 = h[1] * first, h[2] * first
    d1 = h[2] - l1 * h[1]
    e = h[3] - l1 * h[2]
    g1 = moment[1] - l1 * moment[0]
    second = 1.0 / d1
    k = e * second
    d2 = h[4] - l2 * h[2] - k * e
    y2 = (moment[2] - l2 * moment[0] - k * g1) / d2
    y1 = (g1 - e * y2) * second
    y0 = (moment[0] - h[1] * y1 - h[2] * y2) * first
    solution = [y0, y1, y2]
    residual = [
        1.0 - CENTRE * y0, -(y0 + CENTRE * y1), -(y1 + CENTRE * y2), -y2
    ]
    return solution, residual


def kernel(
    sizes, groups,
    load_v, load_w, shift_h, diag_h, off_h, coupling_h, kind_h, cell_h, node_h,
    vu, wu, coefs,
    w_first, shift, diag, off, coupling, cell, ids,
    weights, win, stiff, lanes, rows, rows_b, nodes_mine, nodes_t, overlap,
    centre_diag, ids_in, coup_in,
    x_in, y_in, z_in, w_in, p_in, s_in, z_out, p_out, s_out, red, red_out,
    red_s, red_r,
):
    n_gx, n_gy, n_ea = sizes
    comps, dx, dy, dz = load_v.shape
    ecomp, enb = load_w.shape
    epad = wu.shape[1]
    cap = cell.shape[2]
    per = dx * dy
    half = per // 2
    allrows = comps * per
    groups8 = allrows // 8
    gi, gj, ek = (lax.axis_index(a) for a in AXES)
    own = {"gx": gi, "gy": gj, "ea": ek}
    count = dict(zip(AXES, sizes))

    def members(group):
        total = 1
        for a in group:
            total *= count[a]
        me = 0
        for a in group:
            me = me * count[a] + own[a]

        def target(d):
            flat = lax.rem(me + d, total)
            coords = dict(own)
            for a in reversed(group):
                coords[a] = lax.rem(flat, count[a])
                flat = lax.div(flat, count[a])
            return tuple(coords[a] for a in AXES)

        return total, me, target

    def remote(src, dst, s_sem, r_sem, device):
        return pltpu.make_async_remote_copy(
            src_ref=src, dst_ref=dst, send_sem=s_sem, recv_sem=r_sem,
            device_id=device, device_id_type=MESH,
        )

    def landed(ref, sem):
        pltpu.make_async_copy(ref, ref, sem).wait()

    def red_start(stage, group):
        total, me, target = members(group)
        for d in range(total - 1):
            dst = red.at[stage, me]
            ends = (red_s.at[stage], red_r.at[stage])
            if group == AXES:
                pltpu.make_async_remote_copy(
                    src_ref=red_out.at[stage], dst_ref=dst, send_sem=ends[0], recv_sem=ends[1],
                    device_id=d + jnp.where(me <= d, 1, 0),
                    device_id_type=pl.DeviceIdType.LOGICAL,
                ).start()
            else:
                remote(red_out.at[stage], dst, *ends, target(d + 1)).start()
        red[stage, me] = red_out[stage]

    def steps(
        load_s, ids_s, ids_r, coup_s, coup_r, x_s, x_r, y_s, y_r, z_s, z_r,
        w_s, w_r, p_s, p_r, s_s, s_r, known,
    ):
        has = {
            ("gx", 1): gi < n_gx - 1, ("gx", -1): gi > 0,
            ("gy", 1): gj < n_gy - 1, ("gy", -1): gj > 0,
            ("ea", 1): ek < n_ea - 1, ("ea", -1): ek > 0,
        }
        beside = {
            ("gx", s): (gi + s, gj, ek) for s in (1, -1)
        } | {("gy", s): (gi, gj + s, ek) for s in (1, -1)} | {
            ("ea", s): (gi, gj, ek + s) for s in (1, -1)
        }
        slot = {1: 0, -1: 1}
        sides = {
            name: jnp.where(has[name, 1], 1, 0) + jnp.where(has[name, -1], 1, 0) for name in AXES
        }


        barrier = pltpu.get_barrier_semaphore()
        wide = n_gx + n_gy - 2 + (n_ea > 1) > ITERS + 2

        def greet(sem):
            for d in range(1, n_ea):
                pl.semaphore_signal(
                    sem, inc=1, device_id=(gi, gj, lax.rem(ek + d, n_ea)), device_id_type=MESH
                )
            for name in ("gx", "gy"):
                for s in (1, -1):
                    @pl.when(has[name, s])
                    def _():
                        pl.semaphore_signal(
                            sem, inc=1, device_id=beside[name, s], device_id_type=MESH
                        )

        if wide:
            expected = 0
            for group in groups:
                total, _, target = members(group)
                for d in range(1, total):
                    pl.semaphore_signal(
                        barrier, inc=1, device_id=target(d), device_id_type=MESH
                    )
                expected += total - 1
        else:
            greet(barrier)
            expected = n_ea - 1 + sides["gx"] + sides["gy"]

        loads = {}
        for at, (name, src, dst) in enumerate((
            ("w", load_w, w_first), ("node", node_h, ids.at[0]), ("kind", kind_h, ids.at[1]),
            ("v", load_v, vu.at[0]), ("cell", cell_h, cell), ("coupling", coupling_h, coupling),
            ("shift", shift_h, shift), ("off", off_h, off), ("diag", diag_h, diag),
        )):
            at = 1 if name == "kind" else at
            loads[name] = pltpu.make_async_copy(src, dst, load_s.at[at])
            loads[name].start()

        for s in (1, -1):
            for name, buffer in (("gx", x_in), ("gy", y_in), ("ea", z_in)):
                @pl.when(jnp.logical_not(has[name, -s]))
                def _():
                    for op in range(ITERS):
                        buffer[op, slot[s]] = jnp.zeros(buffer.shape[2:], F32)

        def partner(d):
            return lax.rem(ek + d, n_ea)

        def x_copy(op, s):
            return remote(
                vu.at[op, :, dx - 1 if s == 1 else 0], x_in.at[op, slot[s]],
                x_s.at[0], x_r.at[op], beside["gx", s],
            )

        def y_copy(op, s):
            edge = dy - 1 if s == 1 else 0
            return remote(
                vu.at[op, :, :, edge : edge + 1, :], y_in.at[op, slot[s]],
                y_s.at[0], y_r.at[op], beside["gy", s],
            )

        def z_copy(op, s):
            return remote(
                z_out.at[op, slot[s]], z_in.at[op, slot[s]],
                z_s.at[0], z_r.at[op], beside["ea", s],
            )

        def column_copy(src, dst, s_sem, r_sem, d):
            return remote(src, dst.at[ek], s_sem, r_sem, (gi, gj, partner(d)))

        def w_copy(d):
            return column_copy(wu.at[0], w_in, w_s.at[0], w_r.at[0], d)

        def p_copy(op, d):
            return column_copy(
                p_out.at[op, partner(d)], p_in.at[op], p_s.at[0], p_r.at[op], d
            )

        def s_copy(op, d):
            return column_copy(
                s_out.at[op, partner(d)], s_in.at[op], s_s.at[0], s_r.at[op], d
            )

        def ids_copy(d):
            return column_copy(
                ids.at[:, 0, pl.ds(partner(d), 1), :], ids_in, ids_s.at[0], ids_r.at[0], d
            )

        def block(d):
            return pl.ds(pl.multiple_of(partner(d) * cap, cap), cap)

        def coup_copy(d):
            return column_copy(
                coupling.at[:, :, block(d)], coup_in, coup_s.at[0], coup_r.at[0], d
            )

        def column_send(copy):
            for d in range(1, n_ea):
                copy(d).start()

        lane_i = iota((8, dz), 1)
        lane_r = iota((1, dz), 1)
        row_i = iota((dy, dz), 0)
        lane_b = iota((dy, dz), 1)

        def slabs(o):
            return slice(o * cap, (o + 1) * cap)

        def xy_send(op):
            for s in (1, -1):
                for name, copy in (("gx", x_copy), ("gy", y_copy)):
                    @pl.when(has[name, s])
                    def _():
                        copy(op, s).start()

        def z_send(op):
            v2 = vu[op].reshape(allrows, dz)
            up = jnp.zeros((8, dz), F32)
            down = jnp.zeros((8, dz), F32)
            for g in range(groups8):
                part = v2[8 * g : 8 * g + 8]
                up = jnp.where(lane_i == g, part[:, dz - 1 : dz], up)
                down = jnp.where(lane_i == g, part[:, 0:1], down)
            z_out[op, 0] = up
            z_out[op, 1] = down
            for s in (1, -1):
                @pl.when(has["ea", s])
                def _():
                    z_copy(op, s).start()

        def by_sides(name, two, one, sem):
            @pl.when(sides[name] == 2)
            def _():
                landed(two, sem)

            @pl.when(sides[name] == 1)
            def _():
                landed(one, sem)

        def x_wait(op):
            by_sides("gx", x_in.at[op], x_in.at[op, 0], x_r.at[op])

        def yz_wait(op):
            by_sides("gy", y_in.at[op], y_in.at[op, 0], y_r.at[op])
            by_sides("ea", z_in.at[op], z_in.at[op, 0], z_r.at[op])

        def pick(op):
            v3 = vu[op].reshape(comps, per, dz)
            folds = jnp.concatenate(
                [
                    jnp.concatenate([v3[i, :half], v3[i, half:]], axis=1)
                    for i in range(comps)
                ],
                axis=0,
            )
            seen = folded(jnp.dot(stacked(folds), lanes[...], preferred_element_type=F32))
            return [
                jnp.sum(seen[i * half : (i + 1) * half] * rows[...], axis=0, keepdims=True)
                for i in range(comps)
            ]

        def pick_send(op):
            picked = pick(op)
            for i in range(comps):
                for o in range(n_ea):
                    p_out[op, o, i : i + 1, :] = picked[i][:, slabs(o)]
            column_send(functools.partial(p_copy, op))

        def local(op):
            v4 = vu[op]
            v2 = v4.reshape(allrows, dz)
            zero = jnp.zeros((comps, 1, dy, dz), F32)
            near = jnp.concatenate([zero, v4[:, : dx - 1]], axis=1) + jnp.concatenate(
                [v4[:, 1:], zero], axis=1
            )
            near = near.reshape(allrows, dz)
            lane_all = iota((allrows, dz), 1)
            row_all = lax.rem(iota((allrows, dz), 0), dy)
            near = near + jnp.where(lane_all == 0, 0.0, pltpu.roll(v2, 1, 1))
            near = near + jnp.where(lane_all == dz - 1, 0.0, pltpu.roll(v2, dz - 1, 1))
            near = near + jnp.where(row_all == 0, 0.0, pltpu.roll(v2, 1, 0))
            near = near + jnp.where(row_all == dy - 1, 0.0, pltpu.roll(v2, allrows - 1, 0))
            vu[op + 1] = centre_diag[...][None] * v4 - near.reshape(v4.shape)

        def local_nodes(op):
            w = wu[op]
            acc = stiff[0] * w[0:1]
            for p in range(1, ecomp):
                acc = acc + stiff[p] * w[p : p + 1]
            wu[op + 1] = acc

        def product(op_a, op_b):
            pv = jnp.sum((vu[op_a] * vu[op_b]).reshape(groups8, 8, dz), axis=0)
            pw = jnp.sum(wu[op_a] * wu[op_b], axis=0, keepdims=True)
            total = jnp.sum(pv, axis=0, keepdims=True)
            for b in range(enb // dz):
                total = total + pw[:, b * dz : (b + 1) * dz]
            return total

        def picks_wait(op):
            p_in[op, ek] = p_out[op, ek]
            landed(p_in.at[op, : n_ea - 1], p_r.at[op])

        def slot_terms(op):
            terms = []
            for o in range(n_ea):
                total = None
                for i in range(comps):
                    term = win[o, i] * p_in[op, o, i : i + 1, :]
                    total = term if total is None else total + term
                terms.append(total)
            return stacked(jnp.concatenate(terms, axis=1))

        def nodes_step(op, terms):
            wu[op + 1] += folded(times_transposed(terms, nodes_t[...]))

        def at_slots(op):
            return folded(jnp.dot(stacked(wu[op]), nodes_t[...], preferred_element_type=F32))

        def sums_send(op, values):
            for o in range(n_ea):
                for i in range(comps):
                    s_out[op, o, i : i + 1, :] = jnp.sum(
                        win[o, i] * values[:, slabs(o)], axis=0, keepdims=True
                    )
            column_send(functools.partial(s_copy, op))

        def first_sums():
            w_in[ek] = wu[0]
            landed(w_in.at[: n_ea - 1], w_r.at[0])
            for o in range(n_ea):
                values = folded(jnp.dot(stacked(w_in[o]), nodes_mine[o], preferred_element_type=F32))
                for i in range(comps):
                    s_in[0, o, i : i + 1, :] = jnp.sum(
                        weights[o, i] * values, axis=0, keepdims=True
                    )

        def sums_wait(op):
            s_in[op, ek] = s_out[op, ek]
            landed(s_in.at[op, : n_ea - 1], s_r.at[op])

        def cells_step(op):
            spread_h, spread_l = [], []
            for i in range(comps):
                line = jnp.concatenate([s_in[op, o, i : i + 1, :] for o in range(n_ea)], axis=1)
                h, l = pieces(line)
                spread_h.append(rows_b[...] * h)
                spread_l.append(rows_b[...] * l)
            added = folded(
                times_transposed(jnp.concatenate(spread_h + spread_l, axis=0), lanes[...])
            )
            for i in range(comps):
                for a in range(dx):
                    at = a * dy
                    part = at // half
                    low = i * half + at - part * half
                    vu[op + 1, i, a] += added[low : low + dy, part * dz : (part + 1) * dz]

        def yz_apply(op):
            z_low, z_high = z_in[op, 0], z_in[op, 1]
            for i in range(comps):
                for a in range(dx):
                    at = i * dx + a
                    side = jnp.where(row_i == 0, y_in[op, 0, i, a], 0.0)
                    side = side + jnp.where(row_i == dy - 1, y_in[op, 1, i, a], 0.0)
                    z_l, z_h = [], []
                    for b in range(dy // 8):
                        g = at * (dy // 8) + b
                        z_l.append(jnp.broadcast_to(z_low[:, g : g + 1], (8, dz)))
                        z_h.append(jnp.broadcast_to(z_high[:, g : g + 1], (8, dz)))
                    side = side + jnp.where(lane_b == 0, jnp.concatenate(z_l, axis=0), 0.0)
                    side = side + jnp.where(lane_b == dz - 1, jnp.concatenate(z_h, axis=0), 0.0)
                    vu[op + 1, i, a] -= side

        def x_apply(op):
            vu[op + 1, :, 0] -= x_in[op, 0]
            vu[op + 1, :, dx - 1] -= x_in[op, 1]

        def near_moment(op):
            y = y_in[op, 0] * vu[op, :, :, 0:1] + y_in[op, 1] * vu[op, :, :, dy - 1 : dy]
            z = z_out[op, 1] * z_in[op, 0] + z_out[op, 0] * z_in[op, 1]
            side = jnp.sum(y.reshape(comps * dx, dz), axis=0, keepdims=True)
            return side + jnp.sum(z, axis=0, keepdims=True)

        def slot_moment(op):
            cross = None
            for o in range(n_ea):
                term = p_in[op, o] * s_out[op, o]
                cross = term if cross is None else cross + term
            return jnp.sum(cross, axis=0, keepdims=True)

        def far_moment(op):
            x = x_in[op, 0] * vu[op, :, 0] + x_in[op, 1] * vu[op, :, dx - 1]
            return jnp.sum(x.reshape(comps * dy, dz), axis=0, keepdims=True)

        loads["w"].wait()
        wu[0] = jnp.concatenate([w_first[...], jnp.zeros((epad - ecomp, enb), F32)], axis=0)
        landed(ids, load_s.at[1])

        pl.semaphore_wait(barrier, expected)

        column_send(ids_copy)
        column_send(w_copy)
        if not wide:
            greet(known.at[0])
        loads["v"].wait()
        xy_send(0)
        z_send(0)
        loads["cell"].wait()
        tile = cell[0]
        tile_row = lax.div(tile, dz)
        tile_lane = tile - tile_row * dz
        for o in range(n_ea):
            here = tile_lane[o : o + 1] + jnp.where(tile_row[o : o + 1] >= half, dz, 0)
            lanes[:, slabs(o)] = jnp.where(
                iota((2 * dz, cap), 0) == here, 1.0, 0.0
            ).astype(BF16)
            below = lax.rem(tile_row[o : o + 1], half)
            r = jnp.where(iota((half, cap), 0) == below, 1.0, 0.0)
            rows[:, slabs(o)] = r
            rows_b[:, slabs(o)] = r.astype(BF16)
        pick_send(0)
        loads["coupling"].wait()
        column_send(coup_copy)

        for o in range(n_ea):
            nodes_mine[o] = jnp.where(
                iota((enb, cap), 0) == ids[0, 0, o : o + 1, :], 1.0, 0.0
            ).astype(BF16)
        no_row = jnp.zeros((epad - ecomp, cap), F32)

        def masked(raw, k):
            heavi = jnp.where(k >= 1, 1.0, 0.0)
            tip = jnp.where(k == 2, 1.0, 0.0)
            mask = jnp.where(iota((ecomp, cap), 0) < 3, heavi, tip)
            return jnp.concatenate([raw * mask, no_row], axis=0)

        for o in range(n_ea):
            for i in range(comps):
                weights[o, i] = masked(coupling[i, :, slabs(o)], ids[1, 0, o : o + 1, :])
        loads["shift"].wait()
        centre_diag[...] = shift[...] + (6.0 - CENTRE)
        local(0)
        loads["off"].wait()
        loads["diag"].wait()
        for p in range(ecomp):
            whole = 0.5 * (off[p] + off[:, p, :])
            whole = jnp.where(iota((ecomp, enb), 0) == p, diag[p : p + 1, :] - CENTRE, whole)
            stiff[p] = jnp.concatenate([whole, jnp.zeros((epad - ecomp, enb), F32)], axis=0)
        local_nodes(0)
        moments = [product(0, 0)]
        if not wide:
            pl.semaphore_wait(known.at[0], expected)
            greet(known.at[1])
        ids_in[ek] = ids[:, 0, pl.ds(ek, 1), :]
        coup_in[ek] = coupling[:, :, block(0)]
        yz_wait(0)
        yz_apply(0)
        first_sums()
        cells_step(0)
        x_wait(0)
        x_apply(0)
        if not wide:
            pl.semaphore_wait(known.at[1], expected)
        xy_send(1)
        landed(ids_in.at[: n_ea - 1], ids_r.at[0])
        for o in range(n_ea):
            nodes_t[:, slabs(o)] = jnp.where(
                iota((enb, cap), 0) == ids_in[o, 0], 1.0, 0.0
            ).astype(BF16)
        own_rows = jnp.concatenate([ids_in[o, 0] for o in range(n_ea)], axis=0)
        own_columns = jnp.transpose(
            jnp.concatenate(
                [own_rows.astype(F32), jnp.zeros((cap - n_ea, cap), F32)], axis=0
            )
        ).astype(jnp.int32)
        for a in range(n_ea):
            for b in range(n_ea):
                overlap[slabs(a), slabs(b)] = jnp.where(
                    own_columns[:, a : a + 1] == own_rows[b : b + 1, :], 1.0, 0.0
                ).astype(BF16)
        values = at_slots(1)
        landed(coup_in.at[: n_ea - 1], coup_r.at[0])
        for o in range(n_ea):
            for i in range(comps):
                win[o, i] = masked(coup_in[o, i], ids_in[o, 1])
        picks_wait(0)
        terms = slot_terms(0)
        values = values + folded(
            jnp.dot(terms, overlap[...], preferred_element_type=F32)
        )
        sums_send(1, values)
        z_send(1)
        pick_send(1)
        nodes_step(0, terms)
        last = ITERS - 1
        for op in range(1, last):
            local(op)
            local_nodes(op)
            moments.append(product(op - 1, op))
            moments.append(product(op, op))
            yz_wait(op)
            yz_apply(op)
            sums_wait(op)
            cells_step(op)
            x_wait(op)
            x_apply(op)
            xy_send(op + 1)
            pick_send(op + 1)
            z_send(op + 1)
            picks_wait(op)
            nodes_step(op, slot_terms(op))
            sums_send(op + 1, at_slots(op + 1))

        local(last)
        local_nodes(last)
        moments.append(product(last - 1, last))
        moments.append(product(last, last))
        row = product(last, last + 1)
        packed = jnp.zeros((1, dz), F32)
        for n, m in enumerate(moments):
            packed = jnp.where(lane_r == n, jnp.sum(m, axis=1, keepdims=True), packed)
        red_out[0, 0:1, :] = packed
        yz_wait(last)
        picks_wait(last)
        row = row - near_moment(last) + 2.0 * slot_moment(last)
        x_wait(last)
        red_out[0, 1:2, :] = row - far_moment(last)

        red_start(0, groups[0])
        nodes_step(last, slot_terms(last))
        yz_apply(last)
        x_apply(last)
        sums_wait(last)
        cells_step(last)
        for name, buffer, sem in (("gx", x_in, x_s), ("gy", y_in, y_s), ("ea", z_in, z_s)):
            by_sides(name, buffer, buffer.at[:, 0], sem.at[0])
        landed(p_in.at[:, : n_ea - 1], p_s.at[0])
        landed(s_in.at[1:, : n_ea - 1], s_s.at[0])
        landed(w_in.at[: n_ea - 1], w_s.at[0])
        landed(ids_in.at[: n_ea - 1], ids_s.at[0])
        landed(coup_in.at[: n_ea - 1], coup_s.at[0])

    dma = pltpu.SemaphoreType.DMA
    one, each = dma((1,)), dma((ITERS,))
    pl.run_scoped(
        steps, dma((9,)), one, one, one, one, one, each, one, each, one, each,
        one, one, one, each, one, each, pltpu.SemaphoreType.REGULAR((2,)),
    )

    for stage, group in enumerate(groups):
        total = members(group)[0]
        if stage > 0:
            red_out[stage] = reduced
            red_start(stage, group)
        landed(red.at[stage, : total - 1], red_s.at[stage])
        landed(red.at[stage, : total - 1], red_r.at[stage])
        reduced = jnp.sum(red[stage, :total], axis=0)

    early = [jnp.broadcast_to(reduced[0:1, n : n + 1], (1, dz)) for n in range(2 * ITERS - 1)]
    final = jnp.broadcast_to(jnp.sum(reduced[1:2], axis=1, keepdims=True), (1, dz))
    sol, res = galerkin_coefficients(early + [final])
    for n, c in enumerate(sol + res):
        coefs[n : n + 1, :] = c


def combine_kernel(vu, wu, coefs, sol_v, res_v, sol_w, res_w):
    ecomp = sol_w.shape[0]
    lane_tiles = sol_w.shape[1] // coefs.shape[1]

    def wider(factor):
        return jnp.concatenate([factor] * lane_tiles, axis=1)

    solution = [coefs[n : n + 1, :] for n in range(ITERS)]
    residual = [coefs[ITERS + n : ITERS + n + 1, :] for n in range(ITERS + 1)]

    def combine(factors, terms):
        out = factors[0] * terms[0]
        for f, t in zip(factors[1:], terms[1:]):
            out = out + f * t
        return out

    shape = sol_v.shape
    flat = (shape[0] * shape[1] * shape[2], shape[3])
    v_terms = [vu[n].reshape(flat) for n in range(ITERS + 1)]
    w_terms = [wu[n] for n in range(ITERS + 1)]
    sol_v[...] = combine(solution, v_terms).reshape(shape)
    res_v[...] = combine(residual, v_terms).reshape(shape)
    sol_w[...] = combine([wider(f) for f in solution], w_terms)[:ecomp]
    res_w[...] = combine([wider(f) for f in residual], w_terms)[:ecomp]


def body(sizes, *args):
    load_v, load_w, shift, diag, off, coupling, kind, cell, node = args
    n_ea = sizes[2]
    total = sizes[0] * sizes[1] * sizes[2]
    groups = (AXES,) if total <= 64 else (("gx",), ("gy", "ea"))
    widest = total if total <= 64 else max(sizes[0], sizes[1] * sizes[2])
    comps, dx, dy, dz = load_v.shape
    ecomp, enb = load_w.shape
    cap = node.shape[2]
    vmem = pltpu.VMEM
    dma = pltpu.SemaphoreType.DMA
    epad = -(-ecomp // 16) * 16
    slots = n_ea * cap
    scratch = [
        vmem(load_w.shape, F32), vmem(shift.shape, F32), vmem(diag.shape, F32),
        vmem(off.shape, F32), vmem(coupling.shape, F32),
        vmem(cell.shape, jnp.int32), vmem((2,) + node.shape, jnp.int32),
        vmem((n_ea, comps, epad, cap), F32),
        vmem((n_ea, comps, epad, cap), F32),
        vmem((ecomp, epad, enb), F32),
        vmem((2 * dz, slots), BF16),
        vmem((dx * dy // 2, slots), F32),
        vmem((dx * dy // 2, slots), BF16),
        vmem((n_ea, enb, cap), BF16),
        vmem((enb, slots), BF16),
        vmem((slots, slots), BF16),
        vmem((dx, dy, dz), F32),
        vmem((n_ea, 2, 1, cap), jnp.int32),
        vmem((n_ea, comps, ecomp, cap), F32),
        vmem((ITERS, 2, comps, dy, dz), F32),
        vmem((ITERS, 2, comps, dx, 1, dz), F32),
        vmem((ITERS, 2, 8, dz), F32),
        vmem((n_ea, epad, enb), F32),
        vmem((ITERS, n_ea, comps, cap), F32),
        vmem((ITERS, n_ea, comps, cap), F32),
        vmem((ITERS, 2, 8, dz), F32),
        vmem((ITERS, n_ea, comps, cap), F32),
        vmem((ITERS, n_ea, comps, cap), F32),
        vmem((len(groups), widest, 2, dz), F32),
        vmem((len(groups), 2, dz), F32),
        dma((len(groups),)), dma((len(groups),)),
    ]
    basis = pl.pallas_call(
        functools.partial(kernel, sizes, groups),
        out_shape=(
            pltpu.VMEM((ITERS + 1,) + load_v.shape, F32),
            pltpu.VMEM((ITERS + 1, epad, enb), F32),
            pltpu.VMEM((2 * ITERS + 2, dz), F32),
        ),
        in_specs=[pl.BlockSpec(memory_space=pltpu.HBM)] * 9,
        out_specs=[pl.BlockSpec(memory_space=vmem)] * 3,
        scratch_shapes=scratch,
        compiler_params=pltpu.CompilerParams(
            collective_id=0, has_side_effects=True
        ),
        name="krylov",
    )(*args)
    return tuple(
        pl.pallas_call(
            combine_kernel,
            out_shape=tuple(
                jax.ShapeDtypeStruct(like.shape, F32)
                for like in (load_v, load_v, load_w, load_w)
            ),
            in_specs=[pl.BlockSpec(memory_space=vmem)] * 3,
            out_specs=[pl.BlockSpec(memory_space=vmem)] * 4,
            compiler_params=pltpu.CompilerParams(vmem_limit_bytes=8 << 20),
            name="combine",
        )(*basis)
    )


def solution(mesh):
    column = ("gx", "gy", "ea")
    placed = (
        P(None, "gx", "gy", "ea"),
        P(None, column),
        P("gx", "gy", "ea"),
        P(None, column),
        P(None, None, column),
        P(None, None, column),
        P(column, None, None),
        P(column, None, None),
        P(column, None, None),
    )
    return jax.shard_map(
        functools.partial(body, tuple(mesh.shape[a] for a in AXES)),
        mesh=mesh,
        in_specs=placed,
        out_specs=(
            P(None, "gx", "gy", "ea"),
            P(None, "gx", "gy", "ea"),
            P(None, column),
            P(None, column),
        ),
        check_vma=False,
    )
```

```python
import functools

import jax
import jax.numpy as jnp
from jax import lax
from jax.experimental import pallas as pl
from jax.experimental.pallas import tpu as pltpu
from jax.sharding import PartitionSpec as P

ITERS = 3
CENTRE = 11.5
AXES = ("gx", "gy", "ea")
MESH = pl.DeviceIdType.MESH
F32 = jnp.float32
BF16 = jnp.bfloat16


def pieces(x):
    high = x.astype(BF16)
    return high, (x - high.astype(F32)).astype(BF16)


def stacked(x):
    high, low = pieces(x)
    return jnp.concatenate([high, low], axis=0)


def folded(product):
    half = product.shape[0] // 2
    return product[:half] + product[half:]


def iota(shape, dim):
    return lax.broadcasted_iota(jnp.int32, shape, dim)


def times_transposed(a, b):
    return lax.dot_general(
        a, b, (((1,), (1,)), ((), ())), preferred_element_type=F32
    )


def galerkin_coefficients(moment):
    h = [moment[k + 1] + CENTRE * moment[k] for k in range(2 * ITERS - 1)]
    first = 1.0 / h[0]
    l1, l2 = h[1] * first, h[2] * first
    d1 = h[2] - l1 * h[1]
    e = h[3] - l1 * h[2]
    g1 = moment[1] - l1 * moment[0]
    second = 1.0 / d1
    k = e * second
    d2 = h[4] - l2 * h[2] - k * e
    y2 = (moment[2] - l2 * moment[0] - k * g1) / d2
    y1 = (g1 - e * y2) * second
    y0 = (moment[0] - h[1] * y1 - h[2] * y2) * first
    solution = [y0, y1, y2]
    residual = [
        1.0 - CENTRE * y0, -(y0 + CENTRE * y1), -(y1 + CENTRE * y2), -y2
    ]
    return solution, residual


def kernel(
    sizes, groups,
    load_v, load_w, shift_h, diag_h, off_h, coupling_h, kind_h, cell_h, node_h,
    vu, wu, coefs,
    w_first, shift, diag, off, coupling, cell, ids,
    weights, win, stiff, lanes, rows, rows_b, nodes_mine, nodes_t, overlap,
    centre_diag, ids_in, coup_in,
    x_in, y_in, z_in, w_in, p_in, s_in, z_out, p_out, s_out, red, red_out,
    red_s, red_r,
):
    n_gx, n_gy, n_ea = sizes
    comps, dx, dy, dz = load_v.shape
    ecomp, enb = load_w.shape
    epad = wu.shape[1]
    cap = cell.shape[2]
    per = dx * dy
    half = per // 2
    allrows = comps * per
    groups8 = allrows // 8
    gi, gj, ek = (lax.axis_index(a) for a in AXES)
    own = {"gx": gi, "gy": gj, "ea": ek}
    count = dict(zip(AXES, sizes))

    def members(group):
        total = 1
        for a in group:
            total *= count[a]
        me = 0
        for a in group:
            me = me * count[a] + own[a]

        def target(d):
            flat = lax.rem(me + d, total)
            coords = dict(own)
            for a in reversed(group):
                coords[a] = lax.rem(flat, count[a])
                flat = lax.div(flat, count[a])
            return tuple(coords[a] for a in AXES)

        return total, me, target

    def remote(src, dst, s_sem, r_sem, device):
        return pltpu.make_async_remote_copy(
            src_ref=src, dst_ref=dst, send_sem=s_sem, recv_sem=r_sem,
            device_id=device, device_id_type=MESH,
        )

    def landed(ref, sem):
        pltpu.make_async_copy(ref, ref, sem).wait()

    def red_start(stage, group):
        total, me, target = members(group)
        for d in range(total - 1):
            dst = red.at[stage, me]
            ends = (red_s.at[stage], red_r.at[stage])
            if group == AXES:
                pltpu.make_async_remote_copy(
                    src_ref=red_out.at[stage], dst_ref=dst, send_sem=ends[0], recv_sem=ends[1],
                    device_id=d + jnp.where(me <= d, 1, 0),
                    device_id_type=pl.DeviceIdType.LOGICAL,
                ).start()
            else:
                remote(red_out.at[stage], dst, *ends, target(d + 1)).start()
        red[stage, me] = red_out[stage]

    def steps(
        load_s, ids_s, ids_r, coup_s, coup_r, x_s, x_r, y_s, y_r, z_s, z_r,
        w_s, w_r, p_s, p_r, s_s, s_r, known,
    ):
        has = {
            ("gx", 1): gi < n_gx - 1, ("gx", -1): gi > 0,
            ("gy", 1): gj < n_gy - 1, ("gy", -1): gj > 0,
            ("ea", 1): ek < n_ea - 1, ("ea", -1): ek > 0,
        }
        beside = {
            ("gx", s): (gi + s, gj, ek) for s in (1, -1)
        } | {("gy", s): (gi, gj + s, ek) for s in (1, -1)} | {
            ("ea", s): (gi, gj, ek + s) for s in (1, -1)
        }
        slot = {1: 0, -1: 1}
        last = ITERS - 1
        sides = {
            name: jnp.where(has[name, 1], 1, 0) + jnp.where(has[name, -1], 1, 0) for name in AXES
        }


        barrier = pltpu.get_barrier_semaphore()
        wide = n_gx + n_gy - 2 + (n_ea > 1) > ITERS + 2

        def greet(sem):
            for d in range(1, n_ea):
                pl.semaphore_signal(
                    sem, inc=1, device_id=(gi, gj, lax.rem(ek + d, n_ea)), device_id_type=MESH
                )
            for name in ("gx", "gy"):
                for s in (1, -1):
                    @pl.when(has[name, s])
                    def _():
                        pl.semaphore_signal(
                            sem, inc=1, device_id=beside[name, s], device_id_type=MESH
                        )

        if wide:
            expected = 0
            for group in groups:
                total, _, target = members(group)
                for d in range(1, total):
                    pl.semaphore_signal(
                        barrier, inc=1, device_id=target(d), device_id_type=MESH
                    )
                expected += total - 1
        else:
            greet(barrier)
            expected = n_ea - 1 + sides["gx"] + sides["gy"]

        loads = {}
        for at, (name, src, dst) in enumerate((
            ("w", load_w, w_first), ("node", node_h, ids.at[0]), ("kind", kind_h, ids.at[1]),
            ("v", load_v, vu.at[0]), ("cell", cell_h, cell), ("coupling", coupling_h, coupling),
            ("shift", shift_h, shift), ("off", off_h, off), ("diag", diag_h, diag),
        )):
            at = 1 if name == "kind" else at
            loads[name] = pltpu.make_async_copy(src, dst, load_s.at[at])
            loads[name].start()

        for s in (1, -1):
            for name, buffer in (("gx", x_in), ("gy", y_in), ("ea", z_in)):
                @pl.when(jnp.logical_not(has[name, -s]))
                def _():
                    for op in range(ITERS):
                        buffer[op, slot[s]] = jnp.zeros(buffer.shape[2:], F32)

        def partner(d):
            return lax.rem(ek + d, n_ea)

        def arrival(op, s):
            return op + 1 if op == last and s == 1 else op

        def x_copy(op, s):
            return remote(
                vu.at[op, :, dx - 1 if s == 1 else 0], x_in.at[op, slot[s]],
                x_s.at[0], x_r.at[arrival(op, s)], beside["gx", s],
            )

        def y_copy(op, s):
            edge = dy - 1 if s == 1 else 0
            return remote(
                vu.at[op, :, :, edge : edge + 1, :], y_in.at[op, slot[s]],
                y_s.at[0], y_r.at[arrival(op, s)], beside["gy", s],
            )

        def z_copy(op, s):
            return remote(
                z_out.at[op, slot[s]], z_in.at[op, slot[s]],
                z_s.at[0], z_r.at[arrival(op, s)], beside["ea", s],
            )

        def column_copy(src, dst, s_sem, r_sem, d):
            return remote(src, dst.at[ek], s_sem, r_sem, (gi, gj, partner(d)))

        def w_copy(d):
            return column_copy(wu.at[0], w_in, w_s.at[0], w_r.at[0], d)

        def p_copy(op, d):
            return column_copy(
                p_out.at[op, partner(d)], p_in.at[op], p_s.at[0], p_r.at[op], d
            )

        def s_copy(op, d):
            return column_copy(
                s_out.at[op, partner(d)], s_in.at[op], s_s.at[0], s_r.at[op], d
            )

        def ids_copy(d):
            return column_copy(
                ids.at[:, 0, pl.ds(partner(d), 1), :], ids_in, ids_s.at[0], ids_r.at[0], d
            )

        def block(d):
            return pl.ds(pl.multiple_of(partner(d) * cap, cap), cap)

        def coup_copy(d):
            return column_copy(
                coupling.at[:, :, block(d)], coup_in, coup_s.at[0], coup_r.at[0], d
            )

        def column_send(copy):
            for d in range(1, n_ea):
                copy(d).start()

        lane_i = iota((8, dz), 1)
        lane_r = iota((1, dz), 1)
        row_i = iota((dy, dz), 0)
        lane_b = iota((dy, dz), 1)

        def slabs(o):
            return slice(o * cap, (o + 1) * cap)

        def xy_send(op):
            for s in (1, -1):
                for name, copy in (("gx", x_copy), ("gy", y_copy)):
                    @pl.when(has[name, s])
                    def _():
                        copy(op, s).start()

        def z_send(op):
            v2 = vu[op].reshape(allrows, dz)
            up = jnp.zeros((8, dz), F32)
            down = jnp.zeros((8, dz), F32)
            for g in range(groups8):
                part = v2[8 * g : 8 * g + 8]
                up = jnp.where(lane_i == g, part[:, dz - 1 : dz], up)
                down = jnp.where(lane_i == g, part[:, 0:1], down)
            z_out[op, 0] = up
            z_out[op, 1] = down
            for s in (1, -1):
                @pl.when(has["ea", s])
                def _():
                    z_copy(op, s).start()

        def by_sides(name, two, one, sem):
            @pl.when(sides[name] == 2)
            def _():
                landed(two, sem)

            @pl.when(sides[name] == 1)
            def _():
                landed(one, sem)

        def x_wait(op):
            by_sides("gx", x_in.at[op], x_in.at[op, 0], x_r.at[op])

        def yz_wait(op):
            by_sides("gy", y_in.at[op], y_in.at[op, 0], y_r.at[op])
            by_sides("ea", z_in.at[op], z_in.at[op, 0], z_r.at[op])

        def side_wait(name, buffer, sem, s):
            @pl.when(has[name, -s])
            def _():
                landed(buffer.at[last, slot[s]], sem.at[arrival(last, s)])

        def pick(op):
            v3 = vu[op].reshape(comps, per, dz)
            folds = jnp.concatenate(
                [
                    jnp.concatenate([v3[i, :half], v3[i, half:]], axis=1)
                    for i in range(comps)
                ],
                axis=0,
            )
            seen = folded(jnp.dot(stacked(folds), lanes[...], preferred_element_type=F32))
            return [
                jnp.sum(seen[i * half : (i + 1) * half] * rows[...], axis=0, keepdims=True)
                for i in range(comps)
            ]

        def pick_send(op, picked, added=None):
            for i in range(comps):
                for o in range(n_ea):
                    line = picked[i][:, slabs(o)]
                    if added is not None:
                        line = line + s_in[added, o, i : i + 1, :]
                    p_out[op, o, i : i + 1, :] = line
            column_send(functools.partial(p_copy, op))

        def local(op):
            v4 = vu[op]
            v2 = v4.reshape(allrows, dz)
            zero = jnp.zeros((comps, 1, dy, dz), F32)
            near = jnp.concatenate([zero, v4[:, : dx - 1]], axis=1) + jnp.concatenate(
                [v4[:, 1:], zero], axis=1
            )
            near = near.reshape(allrows, dz)
            lane_all = iota((allrows, dz), 1)
            row_all = lax.rem(iota((allrows, dz), 0), dy)
            near = near + jnp.where(lane_all == 0, 0.0, pltpu.roll(v2, 1, 1))
            near = near + jnp.where(lane_all == dz - 1, 0.0, pltpu.roll(v2, dz - 1, 1))
            near = near + jnp.where(row_all == 0, 0.0, pltpu.roll(v2, 1, 0))
            near = near + jnp.where(row_all == dy - 1, 0.0, pltpu.roll(v2, allrows - 1, 0))
            vu[op + 1] = centre_diag[...][None] * v4 - near.reshape(v4.shape)

        def local_nodes(op):
            w = wu[op]
            acc = stiff[0] * w[0:1]
            for p in range(1, ecomp):
                acc = acc + stiff[p] * w[p : p + 1]
            wu[op + 1] = acc

        def product(op_a, op_b):
            pv = jnp.sum((vu[op_a] * vu[op_b]).reshape(groups8, 8, dz), axis=0)
            pw = jnp.sum(wu[op_a] * wu[op_b], axis=0, keepdims=True)
            total = jnp.sum(pv, axis=0, keepdims=True)
            for b in range(enb // dz):
                total = total + pw[:, b * dz : (b + 1) * dz]
            return total

        def picks_wait(op):
            p_in[op, ek] = p_out[op, ek]
            landed(p_in.at[op, : n_ea - 1], p_r.at[op])

        def slot_terms(op):
            terms = []
            for o in range(n_ea):
                total = None
                for i in range(comps):
                    term = win[o, i] * p_in[op, o, i : i + 1, :]
                    total = term if total is None else total + term
                terms.append(total)
            return stacked(jnp.concatenate(terms, axis=1))

        def nodes_step(op, terms):
            wu[op + 1] += folded(times_transposed(terms, nodes_t[...]))

        def at_slots(op):
            return folded(jnp.dot(stacked(wu[op]), nodes_t[...], preferred_element_type=F32))

        def sums_send(op, values):
            for o in range(n_ea):
                for i in range(comps):
                    s_out[op, o, i : i + 1, :] = jnp.sum(
                        win[o, i] * values[:, slabs(o)], axis=0, keepdims=True
                    )
            column_send(functools.partial(s_copy, op))

        def first_sums():
            w_in[ek] = wu[0]
            landed(w_in.at[: n_ea - 1], w_r.at[0])
            for o in range(n_ea):
                values = folded(jnp.dot(stacked(w_in[o]), nodes_mine[o], preferred_element_type=F32))
                for i in range(comps):
                    s_in[0, o, i : i + 1, :] = jnp.sum(
                        weights[o, i] * values, axis=0, keepdims=True
                    )

        def sums_wait(op):
            s_in[op, ek] = s_out[op, ek]
            landed(s_in.at[op, : n_ea - 1], s_r.at[op])

        def cells_step(op):
            spread_h, spread_l = [], []
            for i in range(comps):
                line = jnp.concatenate([s_in[op, o, i : i + 1, :] for o in range(n_ea)], axis=1)
                h, l = pieces(line)
                spread_h.append(rows_b[...] * h)
                spread_l.append(rows_b[...] * l)
            added = folded(
                times_transposed(jnp.concatenate(spread_h + spread_l, axis=0), lanes[...])
            )
            for i in range(comps):
                for a in range(dx):
                    at = a * dy
                    part = at // half
                    low = i * half + at - part * half
                    vu[op + 1, i, a] += added[low : low + dy, part * dz : (part + 1) * dz]

        def yz_apply(op):
            z_low, z_high = z_in[op, 0], z_in[op, 1]
            for i in range(comps):
                for a in range(dx):
                    at = i * dx + a
                    side = jnp.where(row_i == 0, y_in[op, 0, i, a], 0.0)
                    side = side + jnp.where(row_i == dy - 1, y_in[op, 1, i, a], 0.0)
                    z_l, z_h = [], []
                    for b in range(dy // 8):
                        g = at * (dy // 8) + b
                        z_l.append(jnp.broadcast_to(z_low[:, g : g + 1], (8, dz)))
                        z_h.append(jnp.broadcast_to(z_high[:, g : g + 1], (8, dz)))
                    side = side + jnp.where(lane_b == 0, jnp.concatenate(z_l, axis=0), 0.0)
                    side = side + jnp.where(lane_b == dz - 1, jnp.concatenate(z_h, axis=0), 0.0)
                    vu[op + 1, i, a] -= side

        def x_apply(op):
            vu[op + 1, :, 0] -= x_in[op, 0]
            vu[op + 1, :, dx - 1] -= x_in[op, 1]

        def near_moment(op):
            y = y_in[op, 1] * vu[op, :, :, dy - 1 : dy]
            side = jnp.sum(y.reshape(comps * dx, dz), axis=0, keepdims=True)
            z = z_out[op, 0] * z_in[op, 1]
            return side + jnp.sum(z, axis=0, keepdims=True)

        def slot_moment(op):
            cross = None
            for o in range(n_ea):
                term = p_in[op, o] * s_out[op, o]
                cross = term if cross is None else cross + term
            return jnp.sum(cross, axis=0, keepdims=True)

        def far_moment(op):
            x = x_in[op, 1] * vu[op, :, dx - 1]
            return jnp.sum(x.reshape(comps * dy, dz), axis=0, keepdims=True)

        loads["w"].wait()
        wu[0] = jnp.concatenate([w_first[...], jnp.zeros((epad - ecomp, enb), F32)], axis=0)
        landed(ids, load_s.at[1])

        pl.semaphore_wait(barrier, expected)

        column_send(ids_copy)
        column_send(w_copy)
        if not wide:
            greet(known.at[0])
        loads["v"].wait()
        xy_send(0)
        z_send(0)
        loads["cell"].wait()
        tile = cell[0]
        tile_row = lax.div(tile, dz)
        tile_lane = tile - tile_row * dz
        for o in range(n_ea):
            here = tile_lane[o : o + 1] + jnp.where(tile_row[o : o + 1] >= half, dz, 0)
            lanes[:, slabs(o)] = jnp.where(
                iota((2 * dz, cap), 0) == here, 1.0, 0.0
            ).astype(BF16)
            below = lax.rem(tile_row[o : o + 1], half)
            r = jnp.where(iota((half, cap), 0) == below, 1.0, 0.0)
            rows[:, slabs(o)] = r
            rows_b[:, slabs(o)] = r.astype(BF16)
        pick_send(0, pick(0))
        loads["coupling"].wait()
        column_send(coup_copy)

        for o in range(n_ea):
            nodes_mine[o] = jnp.where(
                iota((enb, cap), 0) == ids[0, 0, o : o + 1, :], 1.0, 0.0
            ).astype(BF16)
        no_row = jnp.zeros((epad - ecomp, cap), F32)

        def masked(raw, k):
            heavi = jnp.where(k >= 1, 1.0, 0.0)
            tip = jnp.where(k == 2, 1.0, 0.0)
            mask = jnp.where(iota((ecomp, cap), 0) < 3, heavi, tip)
            return jnp.concatenate([raw * mask, no_row], axis=0)

        for o in range(n_ea):
            for i in range(comps):
                weights[o, i] = masked(coupling[i, :, slabs(o)], ids[1, 0, o : o + 1, :])
        loads["shift"].wait()
        centre_diag[...] = shift[...] + (6.0 - CENTRE)
        local(0)
        loads["off"].wait()
        loads["diag"].wait()
        for p in range(ecomp):
            whole = 0.5 * (off[p] + off[:, p, :])
            whole = jnp.where(iota((ecomp, enb), 0) == p, diag[p : p + 1, :] - CENTRE, whole)
            stiff[p] = jnp.concatenate([whole, jnp.zeros((epad - ecomp, enb), F32)], axis=0)
        local_nodes(0)
        moments = [product(0, 0)]
        if not wide:
            pl.semaphore_wait(known.at[0], expected)
            greet(known.at[1])
        ids_in[ek] = ids[:, 0, pl.ds(ek, 1), :]
        coup_in[ek] = coupling[:, :, block(0)]
        yz_wait(0)
        yz_apply(0)
        landed(ids_in.at[: n_ea - 1], ids_r.at[0])
        for o in range(n_ea):
            nodes_t[:, slabs(o)] = jnp.where(
                iota((enb, cap), 0) == ids_in[o, 0], 1.0, 0.0
            ).astype(BF16)
        first_sums()
        cells_step(0)
        x_wait(0)
        x_apply(0)
        if not wide:
            pl.semaphore_wait(known.at[1], expected)
        xy_send(1)
        own_rows = jnp.concatenate([ids_in[o, 0] for o in range(n_ea)], axis=0)
        own_columns = jnp.transpose(
            jnp.concatenate(
                [own_rows.astype(F32), jnp.zeros((cap - n_ea, cap), F32)], axis=0
            )
        ).astype(jnp.int32)
        for a in range(n_ea):
            for b in range(n_ea):
                overlap[slabs(a), slabs(b)] = jnp.where(
                    own_columns[:, a : a + 1] == own_rows[b : b + 1, :], 1.0, 0.0
                ).astype(BF16)
        values = at_slots(1)
        landed(coup_in.at[: n_ea - 1], coup_r.at[0])
        for o in range(n_ea):
            for i in range(comps):
                win[o, i] = masked(coup_in[o, i], ids_in[o, 1])
        picks_wait(0)
        terms = slot_terms(0)
        values = values + folded(
            jnp.dot(terms, overlap[...], preferred_element_type=F32)
        )
        sums_send(1, values)
        z_send(1)
        pick_send(1, pick(1))
        nodes_step(0, terms)
        for op in range(1, last):
            local(op)
            local_nodes(op)
            moments.append(product(op - 1, op))
            moments.append(product(op, op))
            yz_wait(op)
            yz_apply(op)
            x_wait(op)
            x_apply(op)
            picked = pick(op + 1)
            sums_wait(op)
            pick_send(op + 1, picked, added=op)
            cells_step(op)
            xy_send(op + 1)
            z_send(op + 1)
            picks_wait(op)
            nodes_step(op, slot_terms(op))
            sums_send(op + 1, at_slots(op + 1))

        local(last)
        local_nodes(last)
        moments.append(product(last - 1, last))
        moments.append(product(last, last))
        row = product(last, last + 1)
        packed = jnp.zeros((1, dz), F32)
        for n, m in enumerate(moments):
            packed = jnp.where(lane_r == n, jnp.sum(m, axis=1, keepdims=True), packed)
        red_out[0, 0:1, :] = packed
        halos = (("ea", z_in, z_r), ("gy", y_in, y_r), ("gx", x_in, x_r))
        picks_wait(last)
        row = row + 2.0 * slot_moment(last)
        for name, buffer, sem in halos[:2]:
            side_wait(name, buffer, sem, -1)
        row = row - 2.0 * near_moment(last)
        side_wait(*halos[2], -1)
        red_out[0, 1:2, :] = row - 2.0 * far_moment(last)

        red_start(0, groups[0])
        nodes_step(last, slot_terms(last))
        for name, buffer, sem in halos:
            side_wait(name, buffer, sem, 1)
        yz_apply(last)
        x_apply(last)
        sums_wait(last)
        cells_step(last)
        for name, buffer, sem in (("gx", x_in, x_s), ("gy", y_in, y_s), ("ea", z_in, z_s)):
            by_sides(name, buffer, buffer.at[:, 0], sem.at[0])
        landed(p_in.at[:, : n_ea - 1], p_s.at[0])
        landed(s_in.at[1:, : n_ea - 1], s_s.at[0])
        landed(w_in.at[: n_ea - 1], w_s.at[0])
        landed(ids_in.at[: n_ea - 1], ids_s.at[0])
        landed(coup_in.at[: n_ea - 1], coup_s.at[0])

    dma = pltpu.SemaphoreType.DMA
    one, each, more = dma((1,)), dma((ITERS,)), dma((ITERS + 1,))
    pl.run_scoped(
        steps, dma((9,)), one, one, one, one, one, more, one, more, one, more,
        one, one, one, each, one, each, pltpu.SemaphoreType.REGULAR((2,)),
    )

    for stage, group in enumerate(groups):
        total = members(group)[0]
        if stage > 0:
            red_out[stage] = reduced
            red_start(stage, group)
        landed(red.at[stage, : total - 1], red_s.at[stage])
        landed(red.at[stage, : total - 1], red_r.at[stage])
        reduced = jnp.sum(red[stage, :total], axis=0)

    early = [jnp.broadcast_to(reduced[0:1, n : n + 1], (1, dz)) for n in range(2 * ITERS - 1)]
    final = jnp.broadcast_to(jnp.sum(reduced[1:2], axis=1, keepdims=True), (1, dz))
    sol, res = galerkin_coefficients(early + [final])
    for n, c in enumerate(sol + res):
        coefs[n : n + 1, :] = c


def combine_kernel(vu, wu, coefs, sol_v, res_v, sol_w, res_w):
    ecomp = sol_w.shape[0]
    lane_tiles = sol_w.shape[1] // coefs.shape[1]

    def wider(factor):
        return jnp.concatenate([factor] * lane_tiles, axis=1)

    solution = [coefs[n : n + 1, :] for n in range(ITERS)]
    residual = [coefs[ITERS + n : ITERS + n + 1, :] for n in range(ITERS + 1)]

    def combine(factors, terms):
        out = factors[0] * terms[0]
        for f, t in zip(factors[1:], terms[1:]):
            out = out + f * t
        return out

    shape = sol_v.shape
    flat = (shape[0] * shape[1] * shape[2], shape[3])
    v_terms = [vu[n].reshape(flat) for n in range(ITERS + 1)]
    w_terms = [wu[n] for n in range(ITERS + 1)]
    sol_v[...] = combine(solution, v_terms).reshape(shape)
    res_v[...] = combine(residual, v_terms).reshape(shape)
    sol_w[...] = combine([wider(f) for f in solution], w_terms)[:ecomp]
    res_w[...] = combine([wider(f) for f in residual], w_terms)[:ecomp]


def body(sizes, *args):
    load_v, load_w, shift, diag, off, coupling, kind, cell, node = args
    n_ea = sizes[2]
    total = sizes[0] * sizes[1] * sizes[2]
    groups = (AXES,) if total <= 64 else (("gx",), ("gy", "ea"))
    widest = total if total <= 64 else max(sizes[0], sizes[1] * sizes[2])
    comps, dx, dy, dz = load_v.shape
    ecomp, enb = load_w.shape
    cap = node.shape[2]
    vmem = pltpu.VMEM
    dma = pltpu.SemaphoreType.DMA
    epad = -(-ecomp // 16) * 16
    slots = n_ea * cap
    scratch = [
        vmem(load_w.shape, F32), vmem(shift.shape, F32), vmem(diag.shape, F32),
        vmem(off.shape, F32), vmem(coupling.shape, F32),
        vmem(cell.shape, jnp.int32), vmem((2,) + node.shape, jnp.int32),
        vmem((n_ea, comps, epad, cap), F32),
        vmem((n_ea, comps, epad, cap), F32),
        vmem((ecomp, epad, enb), F32),
        vmem((2 * dz, slots), BF16),
        vmem((dx * dy // 2, slots), F32),
        vmem((dx * dy // 2, slots), BF16),
        vmem((n_ea, enb, cap), BF16),
        vmem((enb, slots), BF16),
        vmem((slots, slots), BF16),
        vmem((dx, dy, dz), F32),
        vmem((n_ea, 2, 1, cap), jnp.int32),
        vmem((n_ea, comps, ecomp, cap), F32),
        vmem((ITERS, 2, comps, dy, dz), F32),
        vmem((ITERS, 2, comps, dx, 1, dz), F32),
        vmem((ITERS, 2, 8, dz), F32),
        vmem((n_ea, epad, enb), F32),
        vmem((ITERS, n_ea, comps, cap), F32),
        vmem((ITERS, n_ea, comps, cap), F32),
        vmem((ITERS, 2, 8, dz), F32),
        vmem((ITERS, n_ea, comps, cap), F32),
        vmem((ITERS, n_ea, comps, cap), F32),
        vmem((len(groups), widest, 2, dz), F32),
        vmem((len(groups), 2, dz), F32),
        dma((len(groups),)), dma((len(groups),)),
    ]
    basis = pl.pallas_call(
        functools.partial(kernel, sizes, groups),
        out_shape=(
            pltpu.VMEM((ITERS + 1,) + load_v.shape, F32),
            pltpu.VMEM((ITERS + 1, epad, enb), F32),
            pltpu.VMEM((2 * ITERS + 2, dz), F32),
        ),
        in_specs=[pl.BlockSpec(memory_space=pltpu.HBM)] * 9,
        out_specs=[pl.BlockSpec(memory_space=vmem)] * 3,
        scratch_shapes=scratch,
        compiler_params=pltpu.CompilerParams(
            collective_id=0, has_side_effects=True
        ),
        name="krylov",
    )(*args)
    return tuple(
        pl.pallas_call(
            combine_kernel,
            out_shape=tuple(
                jax.ShapeDtypeStruct(like.shape, F32)
                for like in (load_v, load_v, load_w, load_w)
            ),
            in_specs=[pl.BlockSpec(memory_space=vmem)] * 3,
            out_specs=[pl.BlockSpec(memory_space=vmem)] * 4,
            compiler_params=pltpu.CompilerParams(vmem_limit_bytes=8 << 20),
            name="combine",
        )(*basis)
    )


def solution(mesh):
    column = ("gx", "gy", "ea")
    placed = (
        P(None, "gx", "gy", "ea"),
        P(None, column),
        P("gx", "gy", "ea"),
        P(None, column),
        P(None, None, column),
        P(None, None, column),
        P(column, None, None),
        P(column, None, None),
        P(column, None, None),
    )
    return jax.shard_map(
        functools.partial(body, tuple(mesh.shape[a] for a in AXES)),
        mesh=mesh,
        in_specs=placed,
        out_specs=(
            P(None, "gx", "gy", "ea"),
            P(None, "gx", "gy", "ea"),
            P(None, column),
            P(None, column),
        ),
        check_vma=False,
    )
```

```python
import functools

import jax
import jax.numpy as jnp
from jax import lax
from jax.experimental import pallas as pl
from jax.experimental.pallas import tpu as pltpu
from jax.sharding import PartitionSpec as P

ITERS = 3
CENTRE = 11.5
AXES = ("gx", "gy", "ea")
MESH = pl.DeviceIdType.MESH
F32 = jnp.float32
BF16 = jnp.bfloat16


def pieces(x):
    high = x.astype(BF16)
    return high, (x - high.astype(F32)).astype(BF16)


def stacked(x):
    high, low = pieces(x)
    return jnp.concatenate([high, low], axis=0)


def folded(product):
    half = product.shape[0] // 2
    return product[:half] + product[half:]


def iota(shape, dim):
    return lax.broadcasted_iota(jnp.int32, shape, dim)


def times_transposed(a, b):
    return lax.dot_general(
        a, b, (((1,), (1,)), ((), ())), preferred_element_type=F32
    )


def galerkin_coefficients(moment):
    h = [moment[k + 1] + CENTRE * moment[k] for k in range(2 * ITERS - 1)]
    first = 1.0 / h[0]
    l1, l2 = h[1] * first, h[2] * first
    d1 = h[2] - l1 * h[1]
    e = h[3] - l1 * h[2]
    g1 = moment[1] - l1 * moment[0]
    second = 1.0 / d1
    k = e * second
    d2 = h[4] - l2 * h[2] - k * e
    y2 = (moment[2] - l2 * moment[0] - k * g1) / d2
    y1 = (g1 - e * y2) * second
    y0 = (moment[0] - h[1] * y1 - h[2] * y2) * first
    solution = [y0, y1, y2]
    residual = [
        1.0 - CENTRE * y0, -(y0 + CENTRE * y1), -(y1 + CENTRE * y2), -y2
    ]
    return solution, residual


def kernel(
    sizes, groups,
    load_v, load_w, shift_h, diag_h, off_h, coupling_h, kind_h, cell_h, node_h,
    vu, wu, coefs,
    w_first, shift, diag, off, coupling, cell, ids,
    weights, win, stiff, lanes, rows, rows_b, nodes_mine, nodes_t, overlap,
    centre_diag, ids_in, coup_in,
    x_in, y_in, z_in, w_in, p_in, s_in, z_out, p_out, s_out, red, red_out,
    red_s, red_r,
):
    n_gx, n_gy, n_ea = sizes
    comps, dx, dy, dz = load_v.shape
    ecomp, enb = load_w.shape
    epad = wu.shape[1]
    cap = cell.shape[2]
    per = dx * dy
    half = per // 2
    allrows = comps * per
    groups8 = allrows // 8
    gi, gj, ek = (lax.axis_index(a) for a in AXES)
    own = {"gx": gi, "gy": gj, "ea": ek}
    count = dict(zip(AXES, sizes))

    def members(group):
        total = 1
        for a in group:
            total *= count[a]
        me = 0
        for a in group:
            me = me * count[a] + own[a]

        def target(d):
            flat = lax.rem(me + d, total)
            coords = dict(own)
            for a in reversed(group):
                coords[a] = lax.rem(flat, count[a])
                flat = lax.div(flat, count[a])
            return tuple(coords[a] for a in AXES)

        return total, me, target

    def remote(src, dst, s_sem, r_sem, device):
        return pltpu.make_async_remote_copy(
            src_ref=src, dst_ref=dst, send_sem=s_sem, recv_sem=r_sem,
            device_id=device, device_id_type=MESH,
        )

    def landed(ref, sem):
        pltpu.make_async_copy(ref, ref, sem).wait()

    def red_start(stage, group):
        total, me, target = members(group)
        for d in range(total - 1):
            dst = red.at[stage, me]
            ends = (red_s.at[stage], red_r.at[stage])
            if group == AXES:
                pltpu.make_async_remote_copy(
                    src_ref=red_out.at[stage], dst_ref=dst, send_sem=ends[0], recv_sem=ends[1],
                    device_id=d + jnp.where(me <= d, 1, 0),
                    device_id_type=pl.DeviceIdType.LOGICAL,
                ).start()
            else:
                remote(red_out.at[stage], dst, *ends, target(d + 1)).start()
        red[stage, me] = red_out[stage]

    def steps(
        load_s, ids_s, ids_r, coup_s, coup_r, x_s, x_r, y_s, y_r, z_s, z_r,
        w_s, w_r, p_s, p_r, s_s, s_r, known,
    ):
        has = {
            ("gx", 1): gi < n_gx - 1, ("gx", -1): gi > 0,
            ("gy", 1): gj < n_gy - 1, ("gy", -1): gj > 0,
            ("ea", 1): ek < n_ea - 1, ("ea", -1): ek > 0,
        }
        beside = {
            ("gx", s): (gi + s, gj, ek) for s in (1, -1)
        } | {("gy", s): (gi, gj + s, ek) for s in (1, -1)} | {
            ("ea", s): (gi, gj, ek + s) for s in (1, -1)
        }
        slot = {1: 0, -1: 1}
        last = ITERS - 1
        sides = {
            name: jnp.where(has[name, 1], 1, 0) + jnp.where(has[name, -1], 1, 0) for name in AXES
        }


        barrier = pltpu.get_barrier_semaphore()
        wide = n_gx + n_gy - 2 + (n_ea > 1) > ITERS + 2

        def greet(sem):
            for d in range(1, n_ea):
                pl.semaphore_signal(
                    sem, inc=1, device_id=(gi, gj, lax.rem(ek + d, n_ea)), device_id_type=MESH
                )
            for name in ("gx", "gy"):
                for s in (1, -1):
                    @pl.when(has[name, s])
                    def _():
                        pl.semaphore_signal(
                            sem, inc=1, device_id=beside[name, s], device_id_type=MESH
                        )

        if wide:
            expected = 0
            for group in groups:
                total, _, target = members(group)
                for d in range(1, total):
                    pl.semaphore_signal(
                        barrier, inc=1, device_id=target(d), device_id_type=MESH
                    )
                expected += total - 1
        else:
            greet(barrier)
            expected = n_ea - 1 + sides["gx"] + sides["gy"]

        loads = {}
        for at, (name, src, dst) in enumerate((
            ("w", load_w, w_first), ("node", node_h, ids.at[0]), ("kind", kind_h, ids.at[1]),
            ("v", load_v, vu.at[0]), ("cell", cell_h, cell), ("coupling", coupling_h, coupling),
            ("shift", shift_h, shift), ("off", off_h, off), ("diag", diag_h, diag),
        )):
            at = 1 if name == "kind" else at
            loads[name] = pltpu.make_async_copy(src, dst, load_s.at[at])
            loads[name].start()

        for s in (1, -1):
            for name, buffer in (("gx", x_in), ("gy", y_in), ("ea", z_in)):
                @pl.when(jnp.logical_not(has[name, -s]))
                def _():
                    for op in range(ITERS):
                        buffer[op, slot[s]] = jnp.zeros(buffer.shape[2:], F32)

        def partner(d):
            return lax.rem(ek + d, n_ea)

        def arrival(op, s):
            return op + 1 if op == last and s == 1 else op

        def x_copy(op, s):
            return remote(
                vu.at[op, :, dx - 1 if s == 1 else 0], x_in.at[op, slot[s]],
                x_s.at[0], x_r.at[arrival(op, s)], beside["gx", s],
            )

        def y_copy(op, s):
            edge = dy - 1 if s == 1 else 0
            return remote(
                vu.at[op, :, :, edge : edge + 1, :], y_in.at[op, slot[s]],
                y_s.at[0], y_r.at[arrival(op, s)], beside["gy", s],
            )

        def z_copy(op, s):
            return remote(
                z_out.at[op, slot[s]], z_in.at[op, slot[s]],
                z_s.at[0], z_r.at[arrival(op, s)], beside["ea", s],
            )

        def column_copy(src, dst, s_sem, r_sem, d):
            return remote(src, dst.at[ek], s_sem, r_sem, (gi, gj, partner(d)))

        def w_copy(d):
            return column_copy(wu.at[0], w_in, w_s.at[0], w_r.at[0], d)

        def p_copy(op, d):
            return column_copy(
                p_out.at[op, partner(d)], p_in.at[op], p_s.at[0], p_r.at[op], d
            )

        def s_copy(op, d):
            return column_copy(
                s_out.at[op, partner(d)], s_in.at[op], s_s.at[0], s_r.at[op], d
            )

        def ids_copy(d):
            return column_copy(
                ids.at[:, 0, pl.ds(partner(d), 1), :], ids_in, ids_s.at[0], ids_r.at[0], d
            )

        def block(d):
            return pl.ds(pl.multiple_of(partner(d) * cap, cap), cap)

        def coup_copy(d):
            return column_copy(
                coupling.at[:, :, block(d)], coup_in, coup_s.at[0], coup_r.at[0], d
            )

        def column_send(copy):
            for d in range(1, n_ea):
                copy(d).start()

        lane_i = iota((8, dz), 1)
        lane_r = iota((1, dz), 1)
        row_i = iota((dy, dz), 0)
        lane_b = iota((dy, dz), 1)

        def slabs(o):
            return slice(o * cap, (o + 1) * cap)

        def xy_send(op):
            for s in (1, -1):
                for name, copy in (("gx", x_copy), ("gy", y_copy)):
                    @pl.when(has[name, s])
                    def _():
                        copy(op, s).start()

        def z_send(op):
            v2 = vu[op].reshape(allrows, dz)
            up = jnp.zeros((8, dz), F32)
            down = jnp.zeros((8, dz), F32)
            for g in range(groups8):
                part = v2[8 * g : 8 * g + 8]
                up = jnp.where(lane_i == g, part[:, dz - 1 : dz], up)
                down = jnp.where(lane_i == g, part[:, 0:1], down)
            z_out[op, 0] = up
            z_out[op, 1] = down
            for s in (1, -1):
                @pl.when(has["ea", s])
                def _():
                    z_copy(op, s).start()

        def by_sides(name, two, one, sem):
            @pl.when(sides[name] == 2)
            def _():
                landed(two, sem)

            @pl.when(sides[name] == 1)
            def _():
                landed(one, sem)

        def x_wait(op):
            by_sides("gx", x_in.at[op], x_in.at[op, 0], x_r.at[op])

        def yz_wait(op):
            by_sides("gy", y_in.at[op], y_in.at[op, 0], y_r.at[op])
            by_sides("ea", z_in.at[op], z_in.at[op, 0], z_r.at[op])

        def side_wait(name, buffer, sem, s):
            @pl.when(has[name, -s])
            def _():
                landed(buffer.at[last, slot[s]], sem.at[arrival(last, s)])

        def pick(op):
            v3 = vu[op].reshape(comps, per, dz)
            folds = jnp.concatenate(
                [
                    jnp.concatenate([v3[i, :half], v3[i, half:]], axis=1)
                    for i in range(comps)
                ],
                axis=0,
            )
            seen = folded(jnp.dot(stacked(folds), lanes[...], preferred_element_type=F32))
            return [
                jnp.sum(seen[i * half : (i + 1) * half] * rows[...], axis=0, keepdims=True)
                for i in range(comps)
            ]

        def pick_send(op, picked, added=None):
            for i in range(comps):
                for o in range(n_ea):
                    line = picked[i][:, slabs(o)]
                    if added is not None:
                        line = line + s_in[added, o, i : i + 1, :]
                    p_out[op, o, i : i + 1, :] = line
            column_send(functools.partial(p_copy, op))

        def local(op):
            v4 = vu[op]
            v2 = v4.reshape(allrows, dz)
            zero = jnp.zeros((comps, 1, dy, dz), F32)
            near = jnp.concatenate([zero, v4[:, : dx - 1]], axis=1) + jnp.concatenate(
                [v4[:, 1:], zero], axis=1
            )
            near = near.reshape(allrows, dz)
            lane_all = iota((allrows, dz), 1)
            row_all = lax.rem(iota((allrows, dz), 0), dy)
            near = near + jnp.where(lane_all == 0, 0.0, pltpu.roll(v2, 1, 1))
            near = near + jnp.where(lane_all == dz - 1, 0.0, pltpu.roll(v2, dz - 1, 1))
            near = near + jnp.where(row_all == 0, 0.0, pltpu.roll(v2, 1, 0))
            near = near + jnp.where(row_all == dy - 1, 0.0, pltpu.roll(v2, allrows - 1, 0))
            vu[op + 1] = centre_diag[...][None] * v4 - near.reshape(v4.shape)

        def local_nodes(op):
            w = wu[op]
            acc = stiff[0] * w[0:1]
            for p in range(1, ecomp):
                acc = acc + stiff[p] * w[p : p + 1]
            wu[op + 1] = acc

        def product(op_a, op_b):
            pv = jnp.sum((vu[op_a] * vu[op_b]).reshape(groups8, 8, dz), axis=0)
            pw = jnp.sum(wu[op_a] * wu[op_b], axis=0, keepdims=True)
            total = jnp.sum(pv, axis=0, keepdims=True)
            for b in range(enb // dz):
                total = total + pw[:, b * dz : (b + 1) * dz]
            return total

        def picks_wait(op):
            p_in[op, ek] = p_out[op, ek]
            landed(p_in.at[op, : n_ea - 1], p_r.at[op])

        def slot_terms(op):
            terms = []
            for o in range(n_ea):
                total = None
                for i in range(comps):
                    term = win[o, i] * p_in[op, o, i : i + 1, :]
                    total = term if total is None else total + term
                terms.append(total)
            return stacked(jnp.concatenate(terms, axis=1))

        def nodes_step(op, terms):
            wu[op + 1] += folded(times_transposed(terms, nodes_t[...]))

        def at_slots(op):
            return folded(jnp.dot(stacked(wu[op]), nodes_t[...], preferred_element_type=F32))

        def sums_send(op, values):
            for o in range(n_ea):
                for i in range(comps):
                    s_out[op, o, i : i + 1, :] = jnp.sum(
                        win[o, i] * values[:, slabs(o)], axis=0, keepdims=True
                    )
            column_send(functools.partial(s_copy, op))

        def first_sums():
            w_in[ek] = wu[0]
            landed(w_in.at[: n_ea - 1], w_r.at[0])
            for o in range(n_ea):
                values = folded(jnp.dot(stacked(w_in[o]), nodes_mine[o], preferred_element_type=F32))
                for i in range(comps):
                    s_in[0, o, i : i + 1, :] = jnp.sum(
                        weights[o, i] * values, axis=0, keepdims=True
                    )

        def sums_wait(op):
            s_in[op, ek] = s_out[op, ek]
            landed(s_in.at[op, : n_ea - 1], s_r.at[op])

        def cells_step(op):
            spread_h, spread_l = [], []
            for i in range(comps):
                line = jnp.concatenate([s_in[op, o, i : i + 1, :] for o in range(n_ea)], axis=1)
                h, l = pieces(line)
                spread_h.append(rows_b[...] * h)
                spread_l.append(rows_b[...] * l)
            added = folded(
                times_transposed(jnp.concatenate(spread_h + spread_l, axis=0), lanes[...])
            )
            for i in range(comps):
                for a in range(dx):
                    at = a * dy
                    part = at // half
                    low = i * half + at - part * half
                    vu[op + 1, i, a] += added[low : low + dy, part * dz : (part + 1) * dz]

        def yz_apply(op):
            z_low, z_high = z_in[op, 0], z_in[op, 1]
            for i in range(comps):
                for a in range(dx):
                    at = i * dx + a
                    side = jnp.where(row_i == 0, y_in[op, 0, i, a], 0.0)
                    side = side + jnp.where(row_i == dy - 1, y_in[op, 1, i, a], 0.0)
                    z_l, z_h = [], []
                    for b in range(dy // 8):
                        g = at * (dy // 8) + b
                        z_l.append(jnp.broadcast_to(z_low[:, g : g + 1], (8, dz)))
                        z_h.append(jnp.broadcast_to(z_high[:, g : g + 1], (8, dz)))
                    side = side + jnp.where(lane_b == 0, jnp.concatenate(z_l, axis=0), 0.0)
                    side = side + jnp.where(lane_b == dz - 1, jnp.concatenate(z_h, axis=0), 0.0)
                    vu[op + 1, i, a] -= side

        def x_apply(op):
            vu[op + 1, :, 0] -= x_in[op, 0]
            vu[op + 1, :, dx - 1] -= x_in[op, 1]

        def near_moment(op):
            y = y_in[op, 1] * vu[op, :, :, dy - 1 : dy]
            side = jnp.sum(y.reshape(comps * dx, dz), axis=0, keepdims=True)
            z = z_out[op, 0] * z_in[op, 1]
            return side + jnp.sum(z, axis=0, keepdims=True)

        def slot_moment(op):
            cross = None
            for o in range(n_ea):
                term = p_in[op, o] * s_out[op, o]
                cross = term if cross is None else cross + term
            return jnp.sum(cross, axis=0, keepdims=True)

        def far_moment(op):
            x = x_in[op, 1] * vu[op, :, dx - 1]
            return jnp.sum(x.reshape(comps * dy, dz), axis=0, keepdims=True)

        loads["w"].wait()
        wu[0] = jnp.concatenate([w_first[...], jnp.zeros((epad - ecomp, enb), F32)], axis=0)
        landed(ids, load_s.at[1])

        pl.semaphore_wait(barrier, expected)

        column_send(ids_copy)
        column_send(w_copy)
        if not wide:
            greet(known.at[0])
        loads["v"].wait()
        xy_send(0)
        z_send(0)
        loads["cell"].wait()
        tile = cell[0]
        tile_row = lax.div(tile, dz)
        tile_lane = tile - tile_row * dz
        for o in range(n_ea):
            here = tile_lane[o : o + 1] + jnp.where(tile_row[o : o + 1] >= half, dz, 0)
            lanes[:, slabs(o)] = jnp.where(
                iota((2 * dz, cap), 0) == here, 1.0, 0.0
            ).astype(BF16)
            below = lax.rem(tile_row[o : o + 1], half)
            r = jnp.where(iota((half, cap), 0) == below, 1.0, 0.0)
            rows[:, slabs(o)] = r
            rows_b[:, slabs(o)] = r.astype(BF16)
        pick_send(0, pick(0))
        loads["coupling"].wait()
        column_send(coup_copy)

        for o in range(n_ea):
            nodes_mine[o] = jnp.where(
                iota((enb, cap), 0) == ids[0, 0, o : o + 1, :], 1.0, 0.0
            ).astype(BF16)
        no_row = jnp.zeros((epad - ecomp, cap), F32)

        def masked(raw, k):
            heavi = jnp.where(k >= 1, 1.0, 0.0)
            tip = jnp.where(k == 2, 1.0, 0.0)
            mask = jnp.where(iota((ecomp, cap), 0) < 3, heavi, tip)
            return jnp.concatenate([raw * mask, no_row], axis=0)

        for o in range(n_ea):
            for i in range(comps):
                weights[o, i] = masked(coupling[i, :, slabs(o)], ids[1, 0, o : o + 1, :])
        loads["shift"].wait()
        centre_diag[...] = shift[...] + (6.0 - CENTRE)
        local(0)
        loads["off"].wait()
        loads["diag"].wait()
        for p in range(ecomp):
            whole = 0.5 * (off[p] + off[:, p, :])
            whole = jnp.where(iota((ecomp, enb), 0) == p, diag[p : p + 1, :] - CENTRE, whole)
            stiff[p] = jnp.concatenate([whole, jnp.zeros((epad - ecomp, enb), F32)], axis=0)
        local_nodes(0)
        moments = [product(0, 0)]
        if not wide:
            pl.semaphore_wait(known.at[0], expected)
            greet(known.at[1])
        ids_in[ek] = ids[:, 0, pl.ds(ek, 1), :]
        coup_in[ek] = coupling[:, :, block(0)]
        yz_wait(0)
        yz_apply(0)
        landed(ids_in.at[: n_ea - 1], ids_r.at[0])
        own_rows = jnp.concatenate([ids_in[o, 0] for o in range(n_ea)], axis=0)
        own_columns = jnp.transpose(
            jnp.concatenate(
                [own_rows.astype(F32), jnp.zeros((cap - n_ea, cap), F32)], axis=0
            )
        ).astype(jnp.int32)
        for o in range(n_ea):
            nodes_t[:, slabs(o)] = jnp.where(
                iota((enb, cap), 0) == ids_in[o, 0], 1.0, 0.0
            ).astype(BF16)
        first_sums()
        cells_step(0)
        x_wait(0)
        x_apply(0)
        if not wide:
            pl.semaphore_wait(known.at[1], expected)
        xy_send(1)
        for a in range(n_ea):
            for b in range(n_ea):
                overlap[slabs(a), slabs(b)] = jnp.where(
                    own_columns[:, a : a + 1] == own_rows[b : b + 1, :], 1.0, 0.0
                ).astype(BF16)
        values = at_slots(1)
        landed(coup_in.at[: n_ea - 1], coup_r.at[0])
        for o in range(n_ea):
            for i in range(comps):
                win[o, i] = masked(coup_in[o, i], ids_in[o, 1])
        picks_wait(0)
        terms = slot_terms(0)
        values = values + folded(
            jnp.dot(terms, overlap[...], preferred_element_type=F32)
        )
        sums_send(1, values)
        z_send(1)
        pick_send(1, pick(1))
        nodes_step(0, terms)
        for op in range(1, last):
            local(op)
            local_nodes(op)
            moments.append(product(op - 1, op))
            moments.append(product(op, op))
            yz_wait(op)
            yz_apply(op)
            x_wait(op)
            x_apply(op)
            late = ek == n_ea // 2

            @pl.when(late)
            def _():
                sums_wait(op)
                cells_step(op)
                xy_send(op + 1)
                pick_send(op + 1, pick(op + 1))

            @pl.when(jnp.logical_not(late))
            def _():
                picked = pick(op + 1)
                sums_wait(op)
                pick_send(op + 1, picked, added=op)
                cells_step(op)
                xy_send(op + 1)

            z_send(op + 1)
            picks_wait(op)
            nodes_step(op, slot_terms(op))
            sums_send(op + 1, at_slots(op + 1))

        local(last)
        local_nodes(last)
        moments.append(product(last - 1, last))
        moments.append(product(last, last))
        row = product(last, last + 1)
        packed = jnp.zeros((1, dz), F32)
        for n, m in enumerate(moments):
            packed = jnp.where(lane_r == n, jnp.sum(m, axis=1, keepdims=True), packed)
        red_out[0, 0:1, :] = packed
        halos = (("ea", z_in, z_r), ("gy", y_in, y_r), ("gx", x_in, x_r))
        picks_wait(last)
        row = row + 2.0 * slot_moment(last)
        for name, buffer, sem in halos[:2]:
            side_wait(name, buffer, sem, -1)
        row = row - 2.0 * near_moment(last)
        side_wait(*halos[2], -1)
        red_out[0, 1:2, :] = row - 2.0 * far_moment(last)

        red_start(0, groups[0])
        nodes_step(last, slot_terms(last))
        for name, buffer, sem in halos:
            side_wait(name, buffer, sem, 1)
        yz_apply(last)
        x_apply(last)
        sums_wait(last)
        cells_step(last)
        for name, buffer, sem in (("gx", x_in, x_s), ("gy", y_in, y_s), ("ea", z_in, z_s)):
            by_sides(name, buffer, buffer.at[:, 0], sem.at[0])
        landed(p_in.at[:, : n_ea - 1], p_s.at[0])
        landed(s_in.at[1:, : n_ea - 1], s_s.at[0])
        landed(w_in.at[: n_ea - 1], w_s.at[0])
        landed(ids_in.at[: n_ea - 1], ids_s.at[0])
        landed(coup_in.at[: n_ea - 1], coup_s.at[0])

    dma = pltpu.SemaphoreType.DMA
    one, each, more = dma((1,)), dma((ITERS,)), dma((ITERS + 1,))
    pl.run_scoped(
        steps, dma((9,)), one, one, one, one, one, more, one, more, one, more,
        one, one, one, each, one, each, pltpu.SemaphoreType.REGULAR((2,)),
    )

    for stage, group in enumerate(groups):
        total = members(group)[0]
        if stage > 0:
            red_out[stage] = reduced
            red_start(stage, group)
        landed(red.at[stage, : total - 1], red_s.at[stage])
        landed(red.at[stage, : total - 1], red_r.at[stage])
        reduced = jnp.sum(red[stage, :total], axis=0)

    early = [jnp.broadcast_to(reduced[0:1, n : n + 1], (1, dz)) for n in range(2 * ITERS - 1)]
    final = jnp.broadcast_to(jnp.sum(reduced[1:2], axis=1, keepdims=True), (1, dz))
    sol, res = galerkin_coefficients(early + [final])
    for n, c in enumerate(sol + res):
        coefs[n : n + 1, :] = c


def combine_kernel(vu, wu, coefs, sol_v, res_v, sol_w, res_w):
    ecomp = sol_w.shape[0]
    lane_tiles = sol_w.shape[1] // coefs.shape[1]

    def wider(factor):
        return jnp.concatenate([factor] * lane_tiles, axis=1)

    solution = [coefs[n : n + 1, :] for n in range(ITERS)]
    residual = [coefs[ITERS + n : ITERS + n + 1, :] for n in range(ITERS + 1)]

    def combine(factors, terms):
        out = factors[0] * terms[0]
        for f, t in zip(factors[1:], terms[1:]):
            out = out + f * t
        return out

    shape = sol_v.shape
    flat = (shape[0] * shape[1] * shape[2], shape[3])
    v_terms = [vu[n].reshape(flat) for n in range(ITERS + 1)]
    w_terms = [wu[n] for n in range(ITERS + 1)]
    sol_v[...] = combine(solution, v_terms).reshape(shape)
    res_v[...] = combine(residual, v_terms).reshape(shape)
    sol_w[...] = combine([wider(f) for f in solution], w_terms)[:ecomp]
    res_w[...] = combine([wider(f) for f in residual], w_terms)[:ecomp]


def body(sizes, *args):
    load_v, load_w, shift, diag, off, coupling, kind, cell, node = args
    n_ea = sizes[2]
    total = sizes[0] * sizes[1] * sizes[2]
    groups = (AXES,) if total <= 64 else (("gx",), ("gy", "ea"))
    widest = total if total <= 64 else max(sizes[0], sizes[1] * sizes[2])
    comps, dx, dy, dz = load_v.shape
    ecomp, enb = load_w.shape
    cap = node.shape[2]
    vmem = pltpu.VMEM
    dma = pltpu.SemaphoreType.DMA
    epad = -(-ecomp // 16) * 16
    slots = n_ea * cap
    scratch = [
        vmem(load_w.shape, F32), vmem(shift.shape, F32), vmem(diag.shape, F32),
        vmem(off.shape, F32), vmem(coupling.shape, F32),
        vmem(cell.shape, jnp.int32), vmem((2,) + node.shape, jnp.int32),
        vmem((n_ea, comps, epad, cap), F32),
        vmem((n_ea, comps, epad, cap), F32),
        vmem((ecomp, epad, enb), F32),
        vmem((2 * dz, slots), BF16),
        vmem((dx * dy // 2, slots), F32),
        vmem((dx * dy // 2, slots), BF16),
        vmem((n_ea, enb, cap), BF16),
        vmem((enb, slots), BF16),
        vmem((slots, slots), BF16),
        vmem((dx, dy, dz), F32),
        vmem((n_ea, 2, 1, cap), jnp.int32),
        vmem((n_ea, comps, ecomp, cap), F32),
        vmem((ITERS, 2, comps, dy, dz), F32),
        vmem((ITERS, 2, comps, dx, 1, dz), F32),
        vmem((ITERS, 2, 8, dz), F32),
        vmem((n_ea, epad, enb), F32),
        vmem((ITERS, n_ea, comps, cap), F32),
        vmem((ITERS, n_ea, comps, cap), F32),
        vmem((ITERS, 2, 8, dz), F32),
        vmem((ITERS, n_ea, comps, cap), F32),
        vmem((ITERS, n_ea, comps, cap), F32),
        vmem((len(groups), widest, 2, dz), F32),
        vmem((len(groups), 2, dz), F32),
        dma((len(groups),)), dma((len(groups),)),
    ]
    basis = pl.pallas_call(
        functools.partial(kernel, sizes, groups),
        out_shape=(
            pltpu.VMEM((ITERS + 1,) + load_v.shape, F32),
            pltpu.VMEM((ITERS + 1, epad, enb), F32),
            pltpu.VMEM((2 * ITERS + 2, dz), F32),
        ),
        in_specs=[pl.BlockSpec(memory_space=pltpu.HBM)] * 9,
        out_specs=[pl.BlockSpec(memory_space=vmem)] * 3,
        scratch_shapes=scratch,
        compiler_params=pltpu.CompilerParams(
            collective_id=0, has_side_effects=True
        ),
        name="krylov",
    )(*args)
    return tuple(
        pl.pallas_call(
            combine_kernel,
            out_shape=tuple(
                jax.ShapeDtypeStruct(like.shape, F32)
                for like in (load_v, load_v, load_w, load_w)
            ),
            in_specs=[pl.BlockSpec(memory_space=vmem)] * 3,
            out_specs=[pl.BlockSpec(memory_space=vmem)] * 4,
            compiler_params=pltpu.CompilerParams(vmem_limit_bytes=8 << 20),
            name="combine",
        )(*basis)
    )


def solution(mesh):
    column = ("gx", "gy", "ea")
    placed = (
        P(None, "gx", "gy", "ea"),
        P(None, column),
        P("gx", "gy", "ea"),
        P(None, column),
        P(None, None, column),
        P(None, None, column),
        P(column, None, None),
        P(column, None, None),
        P(column, None, None),
    )
    return jax.shard_map(
        functools.partial(body, tuple(mesh.shape[a] for a in AXES)),
        mesh=mesh,
        in_specs=placed,
        out_specs=(
            P(None, "gx", "gy", "ea"),
            P(None, "gx", "gy", "ea"),
            P(None, column),
            P(None, column),
        ),
        check_vma=False,
    )
```

```python
import functools

import jax
import jax.numpy as jnp
from jax import lax
from jax.experimental import pallas as pl
from jax.experimental.pallas import tpu as pltpu
from jax.sharding import PartitionSpec as P

ITERS = 3
CENTRE = 11.5
AXES = ("gx", "gy", "ea")
MESH = pl.DeviceIdType.MESH
F32 = jnp.float32
BF16 = jnp.bfloat16


def pieces(x):
    high = x.astype(BF16)
    return high, (x - high.astype(F32)).astype(BF16)


def stacked(x):
    high, low = pieces(x)
    return jnp.concatenate([high, low], axis=0)


def folded(product):
    half = product.shape[0] // 2
    return product[:half] + product[half:]


def iota(shape, dim):
    return lax.broadcasted_iota(jnp.int32, shape, dim)


def times_transposed(a, b):
    return lax.dot_general(
        a, b, (((1,), (1,)), ((), ())), preferred_element_type=F32
    )


def galerkin_coefficients(moment):
    h = [moment[k + 1] + CENTRE * moment[k] for k in range(2 * ITERS - 1)]
    first = 1.0 / h[0]
    l1, l2 = h[1] * first, h[2] * first
    d1 = h[2] - l1 * h[1]
    e = h[3] - l1 * h[2]
    g1 = moment[1] - l1 * moment[0]
    second = 1.0 / d1
    k = e * second
    d2 = h[4] - l2 * h[2] - k * e
    y2 = (moment[2] - l2 * moment[0] - k * g1) / d2
    y1 = (g1 - e * y2) * second
    y0 = (moment[0] - h[1] * y1 - h[2] * y2) * first
    solution = [y0, y1, y2]
    residual = [
        1.0 - CENTRE * y0, -(y0 + CENTRE * y1), -(y1 + CENTRE * y2), -y2
    ]
    return solution, residual


def kernel(
    sizes, groups,
    load_v, load_w, shift_h, diag_h, off_h, coupling_h, kind_h, cell_h, node_h,
    vu, wu, coefs,
    w_first, shift, diag, off, coupling, cell, ids,
    weights, win, stiff, lanes, rows, rows_b, nodes_mine, nodes_t, overlap,
    centre_diag, ids_in, coup_in,
    x_in, y_in, z_in, w_in, p_in, s_in, z_out, p_out, s_out, red, red_out,
    red_s, red_r,
):
    n_gx, n_gy, n_ea = sizes
    comps, dx, dy, dz = load_v.shape
    ecomp, enb = load_w.shape
    epad = wu.shape[1]
    cap = cell.shape[2]
    per = dx * dy
    half = per // 2
    allrows = comps * per
    groups8 = allrows // 8
    gi, gj, ek = (lax.axis_index(a) for a in AXES)
    own = {"gx": gi, "gy": gj, "ea": ek}
    count = dict(zip(AXES, sizes))

    def members(group):
        total = 1
        for a in group:
            total *= count[a]
        me = 0
        for a in group:
            me = me * count[a] + own[a]

        def target(d):
            flat = lax.rem(me + d, total)
            coords = dict(own)
            for a in reversed(group):
                coords[a] = lax.rem(flat, count[a])
                flat = lax.div(flat, count[a])
            return tuple(coords[a] for a in AXES)

        return total, me, target

    def remote(src, dst, s_sem, r_sem, device):
        return pltpu.make_async_remote_copy(
            src_ref=src, dst_ref=dst, send_sem=s_sem, recv_sem=r_sem,
            device_id=device, device_id_type=MESH,
        )

    def landed(ref, sem):
        pltpu.make_async_copy(ref, ref, sem).wait()

    def red_start(stage, group):
        total, me, target = members(group)
        for d in range(total - 1):
            dst = red.at[stage, me]
            ends = (red_s.at[stage], red_r.at[stage])
            if group == AXES:
                pltpu.make_async_remote_copy(
                    src_ref=red_out.at[stage], dst_ref=dst, send_sem=ends[0], recv_sem=ends[1],
                    device_id=d + jnp.where(me <= d, 1, 0),
                    device_id_type=pl.DeviceIdType.LOGICAL,
                ).start()
            else:
                remote(red_out.at[stage], dst, *ends, target(d + 1)).start()
        red[stage, me] = red_out[stage]

    def steps(
        load_s, ids_s, ids_r, coup_s, coup_r, x_s, x_r, y_s, y_r, z_s, z_r,
        w_s, w_r, p_s, p_r, s_s, s_r, known,
    ):
        has = {
            ("gx", 1): gi < n_gx - 1, ("gx", -1): gi > 0,
            ("gy", 1): gj < n_gy - 1, ("gy", -1): gj > 0,
            ("ea", 1): ek < n_ea - 1, ("ea", -1): ek > 0,
        }
        beside = {
            ("gx", s): (gi + s, gj, ek) for s in (1, -1)
        } | {("gy", s): (gi, gj + s, ek) for s in (1, -1)} | {
            ("ea", s): (gi, gj, ek + s) for s in (1, -1)
        }
        slot = {1: 0, -1: 1}
        last = ITERS - 1
        sides = {
            name: jnp.where(has[name, 1], 1, 0) + jnp.where(has[name, -1], 1, 0) for name in AXES
        }


        barrier = pltpu.get_barrier_semaphore()
        wide = n_gx + n_gy - 2 + (n_ea > 1) > ITERS + 2

        def greet(sem):
            for d in range(1, n_ea):
                pl.semaphore_signal(
                    sem, inc=1, device_id=(gi, gj, lax.rem(ek + d, n_ea)), device_id_type=MESH
                )
            for name in ("gx", "gy"):
                for s in (1, -1):
                    @pl.when(has[name, s])
                    def _():
                        pl.semaphore_signal(
                            sem, inc=1, device_id=beside[name, s], device_id_type=MESH
                        )

        if wide:
            expected = 0
            for group in groups:
                total, _, target = members(group)
                for d in range(1, total):
                    pl.semaphore_signal(
                        barrier, inc=1, device_id=target(d), device_id_type=MESH
                    )
                expected += total - 1
        else:
            greet(barrier)
            expected = n_ea - 1 + sides["gx"] + sides["gy"]

        loads = {}
        for at, (name, src, dst) in enumerate((
            ("w", load_w, w_first), ("node", node_h, ids.at[0]), ("kind", kind_h, ids.at[1]),
            ("v", load_v, vu.at[0]), ("cell", cell_h, cell), ("coupling", coupling_h, coupling),
            ("shift", shift_h, shift), ("off", off_h, off), ("diag", diag_h, diag),
        )):
            at = 1 if name == "kind" else at
            loads[name] = pltpu.make_async_copy(src, dst, load_s.at[at])
            loads[name].start()

        for s in (1, -1):
            for name, buffer in (("gx", x_in), ("gy", y_in), ("ea", z_in)):
                @pl.when(jnp.logical_not(has[name, -s]))
                def _():
                    for op in range(ITERS):
                        buffer[op, slot[s]] = jnp.zeros(buffer.shape[2:], F32)

        def partner(d):
            return lax.rem(ek + d, n_ea)

        def arrival(op, s):
            return op + 1 if op == last and s == 1 else op

        def x_copy(op, s):
            return remote(
                vu.at[op, :, dx - 1 if s == 1 else 0], x_in.at[op, slot[s]],
                x_s.at[0], x_r.at[arrival(op, s)], beside["gx", s],
            )

        def y_copy(op, s):
            edge = dy - 1 if s == 1 else 0
            return remote(
                vu.at[op, :, :, edge : edge + 1, :], y_in.at[op, slot[s]],
                y_s.at[0], y_r.at[arrival(op, s)], beside["gy", s],
            )

        def z_copy(op, s):
            return remote(
                z_out.at[op, slot[s]], z_in.at[op, slot[s]],
                z_s.at[0], z_r.at[arrival(op, s)], beside["ea", s],
            )

        def column_copy(src, dst, s_sem, r_sem, d):
            return remote(src, dst.at[ek], s_sem, r_sem, (gi, gj, partner(d)))

        def w_copy(d):
            return column_copy(wu.at[0], w_in, w_s.at[0], w_r.at[0], d)

        def p_copy(op, d):
            return column_copy(
                p_out.at[op, partner(d)], p_in.at[op], p_s.at[0], p_r.at[op], d
            )

        def s_copy(op, d):
            return column_copy(
                s_out.at[op, partner(d)], s_in.at[op], s_s.at[0], s_r.at[op], d
            )

        def ids_copy(d):
            return column_copy(
                ids.at[:, 0, pl.ds(partner(d), 1), :], ids_in, ids_s.at[0], ids_r.at[0], d
            )

        def block(d):
            return pl.ds(pl.multiple_of(partner(d) * cap, cap), cap)

        def coup_copy(d):
            return column_copy(
                coupling.at[:, :, block(d)], coup_in, coup_s.at[0], coup_r.at[0], d
            )

        def column_send(copy):
            for d in range(1, n_ea):
                copy(d).start()

        lane_i = iota((8, dz), 1)
        lane_r = iota((1, dz), 1)
        row_i = iota((dy, dz), 0)
        lane_b = iota((dy, dz), 1)

        def slabs(o):
            return slice(o * cap, (o + 1) * cap)

        def xy_send(op):
            for s in (1, -1):
                for name, copy in (("gx", x_copy), ("gy", y_copy)):
                    @pl.when(has[name, s])
                    def _():
                        copy(op, s).start()

        def z_send(op):
            v2 = vu[op].reshape(allrows, dz)
            up = jnp.zeros((8, dz), F32)
            down = jnp.zeros((8, dz), F32)
            for g in range(groups8):
                part = v2[8 * g : 8 * g + 8]
                up = jnp.where(lane_i == g, part[:, dz - 1 : dz], up)
                down = jnp.where(lane_i == g, part[:, 0:1], down)
            z_out[op, 0] = up
            z_out[op, 1] = down
            for s in (1, -1):
                @pl.when(has["ea", s])
                def _():
                    z_copy(op, s).start()

        def by_sides(name, two, one, sem):
            @pl.when(sides[name] == 2)
            def _():
                landed(two, sem)

            @pl.when(sides[name] == 1)
            def _():
                landed(one, sem)

        def x_wait(op):
            by_sides("gx", x_in.at[op], x_in.at[op, 0], x_r.at[op])

        def yz_wait(op):
            by_sides("gy", y_in.at[op], y_in.at[op, 0], y_r.at[op])
            by_sides("ea", z_in.at[op], z_in.at[op, 0], z_r.at[op])

        def side_wait(name, buffer, sem, s):
            @pl.when(has[name, -s])
            def _():
                landed(buffer.at[last, slot[s]], sem.at[arrival(last, s)])

        def pick(op):
            v3 = vu[op].reshape(comps, per, dz)
            folds = jnp.concatenate(
                [
                    jnp.concatenate([v3[i, :half], v3[i, half:]], axis=1)
                    for i in range(comps)
                ],
                axis=0,
            )
            seen = folded(jnp.dot(stacked(folds), lanes[...], preferred_element_type=F32))
            return [
                jnp.sum(seen[i * half : (i + 1) * half] * rows[...], axis=0, keepdims=True)
                for i in range(comps)
            ]

        def pick_send(op, picked, added=None):
            for i in range(comps):
                for o in range(n_ea):
                    line = picked[i][:, slabs(o)]
                    if added is not None:
                        line = line + s_in[added, o, i : i + 1, :]
                    p_out[op, o, i : i + 1, :] = line
            column_send(functools.partial(p_copy, op))

        def local(op):
            v4 = vu[op]
            v2 = v4.reshape(allrows, dz)
            zero = jnp.zeros((comps, 1, dy, dz), F32)
            near = jnp.concatenate([zero, v4[:, : dx - 1]], axis=1) + jnp.concatenate(
                [v4[:, 1:], zero], axis=1
            )
            near = near.reshape(allrows, dz)
            lane_all = iota((allrows, dz), 1)
            row_all = lax.rem(iota((allrows, dz), 0), dy)
            near = near + jnp.where(lane_all == 0, 0.0, pltpu.roll(v2, 1, 1))
            near = near + jnp.where(lane_all == dz - 1, 0.0, pltpu.roll(v2, dz - 1, 1))
            near = near + jnp.where(row_all == 0, 0.0, pltpu.roll(v2, 1, 0))
            near = near + jnp.where(row_all == dy - 1, 0.0, pltpu.roll(v2, allrows - 1, 0))
            vu[op + 1] = centre_diag[...][None] * v4 - near.reshape(v4.shape)

        def local_nodes(op):
            w = wu[op]
            acc = stiff[0] * w[0:1]
            for p in range(1, ecomp):
                acc = acc + stiff[p] * w[p : p + 1]
            wu[op + 1] = acc

        def product(op_a, op_b):
            pv = jnp.sum((vu[op_a] * vu[op_b]).reshape(groups8, 8, dz), axis=0)
            pw = jnp.sum(wu[op_a] * wu[op_b], axis=0, keepdims=True)
            total = jnp.sum(pv, axis=0, keepdims=True)
            for b in range(enb // dz):
                total = total + pw[:, b * dz : (b + 1) * dz]
            return total

        def picks_wait(op):
            p_in[op, ek] = p_out[op, ek]
            landed(p_in.at[op, : n_ea - 1], p_r.at[op])

        def slot_terms(op):
            terms = []
            for o in range(n_ea):
                total = None
                for i in range(comps):
                    term = win[o, i] * p_in[op, o, i : i + 1, :]
                    total = term if total is None else total + term
                terms.append(total)
            return stacked(jnp.concatenate(terms, axis=1))

        def nodes_step(op, terms):
            wu[op + 1] += folded(times_transposed(terms, nodes_t[...]))

        def at_slots(op):
            return folded(jnp.dot(stacked(wu[op]), nodes_t[...], preferred_element_type=F32))

        def sums_send(op, values):
            for o in range(n_ea):
                for i in range(comps):
                    s_out[op, o, i : i + 1, :] = jnp.sum(
                        win[o, i] * values[:, slabs(o)], axis=0, keepdims=True
                    )
            column_send(functools.partial(s_copy, op))

        def first_sums():
            w_in[ek] = wu[0]
            landed(w_in.at[: n_ea - 1], w_r.at[0])
            for o in range(n_ea):
                values = folded(jnp.dot(stacked(w_in[o]), nodes_mine[o], preferred_element_type=F32))
                for i in range(comps):
                    s_in[0, o, i : i + 1, :] = jnp.sum(
                        weights[o, i] * values, axis=0, keepdims=True
                    )

        def sums_wait(op):
            s_in[op, ek] = s_out[op, ek]
            landed(s_in.at[op, : n_ea - 1], s_r.at[op])

        def cells_step(op):
            spread_h, spread_l = [], []
            for i in range(comps):
                line = jnp.concatenate([s_in[op, o, i : i + 1, :] for o in range(n_ea)], axis=1)
                h, l = pieces(line)
                spread_h.append(rows_b[...] * h)
                spread_l.append(rows_b[...] * l)
            added = folded(
                times_transposed(jnp.concatenate(spread_h + spread_l, axis=0), lanes[...])
            )
            for i in range(comps):
                for a in range(dx):
                    at = a * dy
                    part = at // half
                    low = i * half + at - part * half
                    vu[op + 1, i, a] += added[low : low + dy, part * dz : (part + 1) * dz]

        def yz_apply(op):
            z_low, z_high = z_in[op, 0], z_in[op, 1]
            for i in range(comps):
                for a in range(dx):
                    at = i * dx + a
                    side = jnp.where(row_i == 0, y_in[op, 0, i, a], 0.0)
                    side = side + jnp.where(row_i == dy - 1, y_in[op, 1, i, a], 0.0)
                    z_l, z_h = [], []
                    for b in range(dy // 8):
                        g = at * (dy // 8) + b
                        z_l.append(jnp.broadcast_to(z_low[:, g : g + 1], (8, dz)))
                        z_h.append(jnp.broadcast_to(z_high[:, g : g + 1], (8, dz)))
                    side = side + jnp.where(lane_b == 0, jnp.concatenate(z_l, axis=0), 0.0)
                    side = side + jnp.where(lane_b == dz - 1, jnp.concatenate(z_h, axis=0), 0.0)
                    vu[op + 1, i, a] -= side

        def x_apply(op):
            vu[op + 1, :, 0] -= x_in[op, 0]
            vu[op + 1, :, dx - 1] -= x_in[op, 1]

        def near_moment(op):
            y = y_in[op, 1] * vu[op, :, :, dy - 1 : dy]
            side = jnp.sum(y.reshape(comps * dx, dz), axis=0, keepdims=True)
            z = z_out[op, 0] * z_in[op, 1]
            return side + jnp.sum(z, axis=0, keepdims=True)

        def slot_moment(op):
            cross = None
            for o in range(n_ea):
                term = p_in[op, o] * s_out[op, o]
                cross = term if cross is None else cross + term
            return jnp.sum(cross, axis=0, keepdims=True)

        def far_moment(op):
            x = x_in[op, 1] * vu[op, :, dx - 1]
            return jnp.sum(x.reshape(comps * dy, dz), axis=0, keepdims=True)

        loads["w"].wait()
        wu[0] = jnp.concatenate([w_first[...], jnp.zeros((epad - ecomp, enb), F32)], axis=0)
        landed(ids, load_s.at[1])

        pl.semaphore_wait(barrier, expected)

        column_send(ids_copy)
        column_send(w_copy)
        if not wide:
            greet(known.at[0])
        loads["v"].wait()
        xy_send(0)
        z_send(0)
        loads["cell"].wait()
        tile = cell[0]
        tile_row = lax.div(tile, dz)
        tile_lane = tile - tile_row * dz
        for o in range(n_ea):
            here = tile_lane[o : o + 1] + jnp.where(tile_row[o : o + 1] >= half, dz, 0)
            lanes[:, slabs(o)] = jnp.where(
                iota((2 * dz, cap), 0) == here, 1.0, 0.0
            ).astype(BF16)
            below = lax.rem(tile_row[o : o + 1], half)
            r = jnp.where(iota((half, cap), 0) == below, 1.0, 0.0)
            rows[:, slabs(o)] = r
            rows_b[:, slabs(o)] = r.astype(BF16)
        pick_send(0, pick(0))
        loads["coupling"].wait()
        column_send(coup_copy)

        for o in range(n_ea):
            nodes_mine[o] = jnp.where(
                iota((enb, cap), 0) == ids[0, 0, o : o + 1, :], 1.0, 0.0
            ).astype(BF16)
        no_row = jnp.zeros((epad - ecomp, cap), F32)

        def masked(raw, k):
            heavi = jnp.where(k >= 1, 1.0, 0.0)
            tip = jnp.where(k == 2, 1.0, 0.0)
            mask = jnp.where(iota((ecomp, cap), 0) < 3, heavi, tip)
            return jnp.concatenate([raw * mask, no_row], axis=0)

        for o in range(n_ea):
            for i in range(comps):
                weights[o, i] = masked(coupling[i, :, slabs(o)], ids[1, 0, o : o + 1, :])
        loads["shift"].wait()
        centre_diag[...] = shift[...] + (6.0 - CENTRE)
        local(0)
        loads["off"].wait()
        loads["diag"].wait()
        for p in range(ecomp):
            whole = 0.5 * (off[p] + off[:, p, :])
            whole = jnp.where(iota((ecomp, enb), 0) == p, diag[p : p + 1, :] - CENTRE, whole)
            stiff[p] = jnp.concatenate([whole, jnp.zeros((epad - ecomp, enb), F32)], axis=0)
        local_nodes(0)
        moments = [product(0, 0)]
        if not wide:
            pl.semaphore_wait(known.at[0], expected)
            greet(known.at[1])
        ids_in[ek] = ids[:, 0, pl.ds(ek, 1), :]
        coup_in[ek] = coupling[:, :, block(0)]
        def tables():
            landed(ids_in.at[: n_ea - 1], ids_r.at[0])
            own_rows = jnp.concatenate([ids_in[o, 0] for o in range(n_ea)], axis=0)
            own_columns = jnp.transpose(
                jnp.concatenate(
                    [own_rows.astype(F32), jnp.zeros((cap - n_ea, cap), F32)], axis=0
                )
            ).astype(jnp.int32)
            for o in range(n_ea):
                nodes_t[:, slabs(o)] = jnp.where(
                    iota((enb, cap), 0) == ids_in[o, 0], 1.0, 0.0
                ).astype(BF16)
            for a in range(n_ea):
                for b in range(n_ea):
                    overlap[slabs(a), slabs(b)] = jnp.where(
                        own_columns[:, a : a + 1] == own_rows[b : b + 1, :], 1.0, 0.0
                    ).astype(BF16)

        def layers():
            yz_wait(0)
            yz_apply(0)

        orders = {1: (tables, first_sums, layers), n_ea - 1: (layers, tables, first_sums)}
        usual = ek >= 0
        for place, order in orders.items():
            usual = jnp.logical_and(usual, ek != place)

            @pl.when(ek == place)
            def _():
                for step in order:
                    step()

        @pl.when(usual)
        def _():
            tables()
            layers()
            first_sums()

        cells_step(0)
        x_wait(0)
        x_apply(0)
        if not wide:
            pl.semaphore_wait(known.at[1], expected)
        xy_send(1)
        values = at_slots(1)
        landed(coup_in.at[: n_ea - 1], coup_r.at[0])
        for o in range(n_ea):
            for i in range(comps):
                win[o, i] = masked(coup_in[o, i], ids_in[o, 1])
        picks_wait(0)
        terms = slot_terms(0)
        values = values + folded(
            jnp.dot(terms, overlap[...], preferred_element_type=F32)
        )
        sums_send(1, values)
        z_send(1)
        pick_send(1, pick(1))
        nodes_step(0, terms)
        for op in range(1, last):
            local(op)
            local_nodes(op)
            moments.append(product(op - 1, op))
            moments.append(product(op, op))
            yz_wait(op)
            yz_apply(op)
            x_wait(op)
            x_apply(op)
            late = ek == n_ea // 2

            @pl.when(late)
            def _():
                sums_wait(op)
                cells_step(op)
                xy_send(op + 1)
                pick_send(op + 1, pick(op + 1))

            @pl.when(jnp.logical_not(late))
            def _():
                picked = pick(op + 1)
                sums_wait(op)
                pick_send(op + 1, picked, added=op)
                cells_step(op)
                xy_send(op + 1)

            z_send(op + 1)
            picks_wait(op)
            nodes_step(op, slot_terms(op))
            sums_send(op + 1, at_slots(op + 1))

        local(last)
        local_nodes(last)
        moments.append(product(last - 1, last))
        moments.append(product(last, last))
        row = product(last, last + 1)
        packed = jnp.zeros((1, dz), F32)
        for n, m in enumerate(moments):
            packed = jnp.where(lane_r == n, jnp.sum(m, axis=1, keepdims=True), packed)
        red_out[0, 0:1, :] = packed
        halos = (("ea", z_in, z_r), ("gy", y_in, y_r), ("gx", x_in, x_r))
        picks_wait(last)
        row = row + 2.0 * slot_moment(last)
        for name, buffer, sem in halos[:2]:
            side_wait(name, buffer, sem, -1)
        row = row - 2.0 * near_moment(last)
        side_wait(*halos[2], -1)
        red_out[0, 1:2, :] = row - 2.0 * far_moment(last)

        red_start(0, groups[0])
        nodes_step(last, slot_terms(last))
        for name, buffer, sem in halos:
            side_wait(name, buffer, sem, 1)
        yz_apply(last)
        x_apply(last)
        sums_wait(last)
        cells_step(last)
        for name, buffer, sem in (("gx", x_in, x_s), ("gy", y_in, y_s), ("ea", z_in, z_s)):
            by_sides(name, buffer, buffer.at[:, 0], sem.at[0])
        landed(p_in.at[:, : n_ea - 1], p_s.at[0])
        landed(s_in.at[1:, : n_ea - 1], s_s.at[0])
        landed(w_in.at[: n_ea - 1], w_s.at[0])
        landed(ids_in.at[: n_ea - 1], ids_s.at[0])
        landed(coup_in.at[: n_ea - 1], coup_s.at[0])

    dma = pltpu.SemaphoreType.DMA
    one, each, more = dma((1,)), dma((ITERS,)), dma((ITERS + 1,))
    pl.run_scoped(
        steps, dma((9,)), one, one, one, one, one, more, one, more, one, more,
        one, one, one, each, one, each, pltpu.SemaphoreType.REGULAR((2,)),
    )

    for stage, group in enumerate(groups):
        total = members(group)[0]
        if stage > 0:
            red_out[stage] = reduced
            red_start(stage, group)
        landed(red.at[stage, : total - 1], red_s.at[stage])
        landed(red.at[stage, : total - 1], red_r.at[stage])
        reduced = jnp.sum(red[stage, :total], axis=0)

    early = [jnp.broadcast_to(reduced[0:1, n : n + 1], (1, dz)) for n in range(2 * ITERS - 1)]
    final = jnp.broadcast_to(jnp.sum(reduced[1:2], axis=1, keepdims=True), (1, dz))
    sol, res = galerkin_coefficients(early + [final])
    for n, c in enumerate(sol + res):
        coefs[n : n + 1, :] = c


def combine_kernel(vu, wu, coefs, sol_v, res_v, sol_w, res_w):
    ecomp = sol_w.shape[0]
    lane_tiles = sol_w.shape[1] // coefs.shape[1]

    def wider(factor):
        return jnp.concatenate([factor] * lane_tiles, axis=1)

    solution = [coefs[n : n + 1, :] for n in range(ITERS)]
    residual = [coefs[ITERS + n : ITERS + n + 1, :] for n in range(ITERS + 1)]

    def combine(factors, terms):
        out = factors[0] * terms[0]
        for f, t in zip(factors[1:], terms[1:]):
            out = out + f * t
        return out

    shape = sol_v.shape
    flat = (shape[0] * shape[1] * shape[2], shape[3])
    v_terms = [vu[n].reshape(flat) for n in range(ITERS + 1)]
    w_terms = [wu[n] for n in range(ITERS + 1)]
    sol_v[...] = combine(solution, v_terms).reshape(shape)
    res_v[...] = combine(residual, v_terms).reshape(shape)
    sol_w[...] = combine([wider(f) for f in solution], w_terms)[:ecomp]
    res_w[...] = combine([wider(f) for f in residual], w_terms)[:ecomp]


def body(sizes, *args):
    load_v, load_w, shift, diag, off, coupling, kind, cell, node = args
    n_ea = sizes[2]
    total = sizes[0] * sizes[1] * sizes[2]
    groups = (AXES,) if total <= 64 else (("gx",), ("gy", "ea"))
    widest = total if total <= 64 else max(sizes[0], sizes[1] * sizes[2])
    comps, dx, dy, dz = load_v.shape
    ecomp, enb = load_w.shape
    cap = node.shape[2]
    vmem = pltpu.VMEM
    dma = pltpu.SemaphoreType.DMA
    epad = -(-ecomp // 16) * 16
    slots = n_ea * cap
    scratch = [
        vmem(load_w.shape, F32), vmem(shift.shape, F32), vmem(diag.shape, F32),
        vmem(off.shape, F32), vmem(coupling.shape, F32),
        vmem(cell.shape, jnp.int32), vmem((2,) + node.shape, jnp.int32),
        vmem((n_ea, comps, epad, cap), F32),
        vmem((n_ea, comps, epad, cap), F32),
        vmem((ecomp, epad, enb), F32),
        vmem((2 * dz, slots), BF16),
        vmem((dx * dy // 2, slots), F32),
        vmem((dx * dy // 2, slots), BF16),
        vmem((n_ea, enb, cap), BF16),
        vmem((enb, slots), BF16),
        vmem((slots, slots), BF16),
        vmem((dx, dy, dz), F32),
        vmem((n_ea, 2, 1, cap), jnp.int32),
        vmem((n_ea, comps, ecomp, cap), F32),
        vmem((ITERS, 2, comps, dy, dz), F32),
        vmem((ITERS, 2, comps, dx, 1, dz), F32),
        vmem((ITERS, 2, 8, dz), F32),
        vmem((n_ea, epad, enb), F32),
        vmem((ITERS, n_ea, comps, cap), F32),
        vmem((ITERS, n_ea, comps, cap), F32),
        vmem((ITERS, 2, 8, dz), F32),
        vmem((ITERS, n_ea, comps, cap), F32),
        vmem((ITERS, n_ea, comps, cap), F32),
        vmem((len(groups), widest, 2, dz), F32),
        vmem((len(groups), 2, dz), F32),
        dma((len(groups),)), dma((len(groups),)),
    ]
    basis = pl.pallas_call(
        functools.partial(kernel, sizes, groups),
        out_shape=(
            pltpu.VMEM((ITERS + 1,) + load_v.shape, F32),
            pltpu.VMEM((ITERS + 1, epad, enb), F32),
            pltpu.VMEM((2 * ITERS + 2, dz), F32),
        ),
        in_specs=[pl.BlockSpec(memory_space=pltpu.HBM)] * 9,
        out_specs=[pl.BlockSpec(memory_space=vmem)] * 3,
        scratch_shapes=scratch,
        compiler_params=pltpu.CompilerParams(
            collective_id=0, has_side_effects=True
        ),
        name="krylov",
    )(*args)
    return tuple(
        pl.pallas_call(
            combine_kernel,
            out_shape=tuple(
                jax.ShapeDtypeStruct(like.shape, F32)
                for like in (load_v, load_v, load_w, load_w)
            ),
            in_specs=[pl.BlockSpec(memory_space=vmem)] * 3,
            out_specs=[pl.BlockSpec(memory_space=vmem)] * 4,
            compiler_params=pltpu.CompilerParams(vmem_limit_bytes=8 << 20),
            name="combine",
        )(*basis)
    )


def solution(mesh):
    column = ("gx", "gy", "ea")
    placed = (
        P(None, "gx", "gy", "ea"),
        P(None, column),
        P("gx", "gy", "ea"),
        P(None, column),
        P(None, None, column),
        P(None, None, column),
        P(column, None, None),
        P(column, None, None),
        P(column, None, None),
    )
    return jax.shard_map(
        functools.partial(body, tuple(mesh.shape[a] for a in AXES)),
        mesh=mesh,
        in_specs=placed,
        out_specs=(
            P(None, "gx", "gy", "ea"),
            P(None, "gx", "gy", "ea"),
            P(None, column),
            P(None, column),
        ),
        check_vma=False,
    )
```

```python
import functools

import jax
import jax.numpy as jnp
from jax import lax
from jax.experimental import pallas as pl
from jax.experimental.pallas import tpu as pltpu
from jax.sharding import PartitionSpec as P

ITERS = 3
CENTRE = 11.5
AXES = ("gx", "gy", "ea")
MESH = pl.DeviceIdType.MESH
F32 = jnp.float32
BF16 = jnp.bfloat16


def pieces(x):
    high = x.astype(BF16)
    return high, (x - high.astype(F32)).astype(BF16)


def stacked(x):
    high, low = pieces(x)
    return jnp.concatenate([high, low], axis=0)


def folded(product):
    half = product.shape[0] // 2
    return product[:half] + product[half:]


def iota(shape, dim):
    return lax.broadcasted_iota(jnp.int32, shape, dim)


def times_transposed(a, b):
    return lax.dot_general(
        a, b, (((1,), (1,)), ((), ())), preferred_element_type=F32
    )


def galerkin_coefficients(moment):
    h = [moment[k + 1] + CENTRE * moment[k] for k in range(2 * ITERS - 1)]
    first = 1.0 / h[0]
    l1, l2 = h[1] * first, h[2] * first
    d1 = h[2] - l1 * h[1]
    e = h[3] - l1 * h[2]
    g1 = moment[1] - l1 * moment[0]
    second = 1.0 / d1
    k = e * second
    d2 = h[4] - l2 * h[2] - k * e
    y2 = (moment[2] - l2 * moment[0] - k * g1) / d2
    y1 = (g1 - e * y2) * second
    y0 = (moment[0] - h[1] * y1 - h[2] * y2) * first
    solution = [y0, y1, y2]
    residual = [
        1.0 - CENTRE * y0, -(y0 + CENTRE * y1), -(y1 + CENTRE * y2), -y2
    ]
    return solution, residual


def kernel(
    sizes, groups,
    load_v, load_w, shift_h, diag_h, off_h, coupling_h, kind_h, cell_h, node_h,
    vu, wu, coefs,
    w_first, shift, diag, off, coupling, cell, ids,
    weights, win, stiff, lanes, rows, rows_b, nodes_mine, nodes_t, overlap, turned,
    centre_diag, ids_in, coup_in,
    x_in, y_in, z_in, w_in, p_in, s_in, z_out, p_out, s_out, red, red_out,
    red_s, red_r,
):
    n_gx, n_gy, n_ea = sizes
    comps, dx, dy, dz = load_v.shape
    ecomp, enb = load_w.shape
    epad = wu.shape[1]
    cap = cell.shape[2]
    per = dx * dy
    half = per // 2
    allrows = comps * per
    groups8 = allrows // 8
    gi, gj, ek = (lax.axis_index(a) for a in AXES)
    own = {"gx": gi, "gy": gj, "ea": ek}
    count = dict(zip(AXES, sizes))

    def members(group):
        total = 1
        for a in group:
            total *= count[a]
        me = 0
        for a in group:
            me = me * count[a] + own[a]

        def target(d):
            flat = lax.rem(me + d, total)
            coords = dict(own)
            for a in reversed(group):
                coords[a] = lax.rem(flat, count[a])
                flat = lax.div(flat, count[a])
            return tuple(coords[a] for a in AXES)

        return total, me, target

    def remote(src, dst, s_sem, r_sem, device):
        return pltpu.make_async_remote_copy(
            src_ref=src, dst_ref=dst, send_sem=s_sem, recv_sem=r_sem,
            device_id=device, device_id_type=MESH,
        )

    def landed(ref, sem):
        pltpu.make_async_copy(ref, ref, sem).wait()

    def red_start(stage, group):
        total, me, target = members(group)
        for d in range(total - 1):
            dst = red.at[stage, me]
            ends = (red_s.at[stage], red_r.at[stage])
            if group == AXES:
                pltpu.make_async_remote_copy(
                    src_ref=red_out.at[stage], dst_ref=dst, send_sem=ends[0], recv_sem=ends[1],
                    device_id=d + jnp.where(me <= d, 1, 0),
                    device_id_type=pl.DeviceIdType.LOGICAL,
                ).start()
            else:
                remote(red_out.at[stage], dst, *ends, target(d + 1)).start()
        red[stage, me] = red_out[stage]

    def steps(
        load_s, ids_s, ids_r, coup_s, coup_r, x_s, x_r, y_s, y_r, z_s, z_r,
        w_s, w_r, p_s, p_r, s_s, s_r, known,
    ):
        has = {
            ("gx", 1): gi < n_gx - 1, ("gx", -1): gi > 0,
            ("gy", 1): gj < n_gy - 1, ("gy", -1): gj > 0,
            ("ea", 1): ek < n_ea - 1, ("ea", -1): ek > 0,
        }
        beside = {
            ("gx", s): (gi + s, gj, ek) for s in (1, -1)
        } | {("gy", s): (gi, gj + s, ek) for s in (1, -1)} | {
            ("ea", s): (gi, gj, ek + s) for s in (1, -1)
        }
        slot = {1: 0, -1: 1}
        last = ITERS - 1
        sides = {
            name: jnp.where(has[name, 1], 1, 0) + jnp.where(has[name, -1], 1, 0) for name in AXES
        }


        barrier = pltpu.get_barrier_semaphore()
        wide = n_gx + n_gy - 2 + (n_ea > 1) > ITERS + 2

        def greet(sem):
            for d in range(1, n_ea):
                pl.semaphore_signal(
                    sem, inc=1, device_id=(gi, gj, lax.rem(ek + d, n_ea)), device_id_type=MESH
                )
            for name in ("gx", "gy"):
                for s in (1, -1):
                    @pl.when(has[name, s])
                    def _():
                        pl.semaphore_signal(
                            sem, inc=1, device_id=beside[name, s], device_id_type=MESH
                        )

        if wide:
            expected = 0
            for group in groups:
                total, _, target = members(group)
                for d in range(1, total):
                    pl.semaphore_signal(
                        barrier, inc=1, device_id=target(d), device_id_type=MESH
                    )
                expected += total - 1
        else:
            greet(barrier)
            expected = n_ea - 1 + sides["gx"] + sides["gy"]

        loads = {}
        for at, (name, src, dst) in enumerate((
            ("w", load_w, w_first), ("node", node_h, ids.at[0]), ("kind", kind_h, ids.at[1]),
            ("v", load_v, vu.at[0]), ("cell", cell_h, cell), ("coupling", coupling_h, coupling),
            ("shift", shift_h, shift), ("off", off_h, off), ("diag", diag_h, diag),
        )):
            at = 1 if name == "kind" else at
            loads[name] = pltpu.make_async_copy(src, dst, load_s.at[at])
            loads[name].start()

        for s in (1, -1):
            for name, buffer in (("gx", x_in), ("gy", y_in), ("ea", z_in)):
                @pl.when(jnp.logical_not(has[name, -s]))
                def _():
                    for op in range(ITERS):
                        buffer[op, slot[s]] = jnp.zeros(buffer.shape[2:], F32)

        def partner(d):
            return lax.rem(ek + d, n_ea)

        def arrival(op, s):
            return op + 1 if op == last and s == 1 else op

        def x_copy(op, s):
            return remote(
                vu.at[op, :, dx - 1 if s == 1 else 0], x_in.at[op, slot[s]],
                x_s.at[0], x_r.at[arrival(op, s)], beside["gx", s],
            )

        def y_copy(op, s):
            edge = dy - 1 if s == 1 else 0
            return remote(
                vu.at[op, :, :, edge : edge + 1, :], y_in.at[op, slot[s]],
                y_s.at[0], y_r.at[arrival(op, s)], beside["gy", s],
            )

        def z_copy(op, s):
            return remote(
                z_out.at[op, slot[s]], z_in.at[op, slot[s]],
                z_s.at[0], z_r.at[arrival(op, s)], beside["ea", s],
            )

        def column_copy(src, dst, s_sem, r_sem, d):
            return remote(src, dst.at[ek], s_sem, r_sem, (gi, gj, partner(d)))

        def w_copy(d):
            return column_copy(wu.at[0], w_in, w_s.at[0], w_r.at[0], d)

        def p_copy(op, d):
            return column_copy(
                p_out.at[op, partner(d)], p_in.at[op], p_s.at[0], p_r.at[op], d
            )

        def s_copy(op, d):
            return column_copy(
                s_out.at[op, partner(d)], s_in.at[op], s_s.at[0], s_r.at[op], d
            )

        def ids_copy(d):
            return column_copy(
                ids.at[:, 0, pl.ds(partner(d), 1), :], ids_in, ids_s.at[0], ids_r.at[0], d
            )

        def block(d):
            return pl.ds(pl.multiple_of(partner(d) * cap, cap), cap)

        def coup_copy(d):
            return column_copy(
                coupling.at[:, :, block(d)], coup_in, coup_s.at[0], coup_r.at[0], d
            )

        def column_send(copy):
            for d in range(1, n_ea):
                copy(d).start()

        lane_i = iota((8, dz), 1)
        lane_r = iota((1, dz), 1)
        row_i = iota((dy, dz), 0)
        lane_b = iota((dy, dz), 1)

        def slabs(o):
            return slice(o * cap, (o + 1) * cap)

        def xy_send(op):
            for s in (1, -1):
                for name, copy in (("gx", x_copy), ("gy", y_copy)):
                    @pl.when(has[name, s])
                    def _():
                        copy(op, s).start()

        def z_send(op):
            v2 = vu[op].reshape(allrows, dz)
            up = jnp.zeros((8, dz), F32)
            down = jnp.zeros((8, dz), F32)
            for g in range(groups8):
                part = v2[8 * g : 8 * g + 8]
                up = jnp.where(lane_i == g, part[:, dz - 1 : dz], up)
                down = jnp.where(lane_i == g, part[:, 0:1], down)
            z_out[op, 0] = up
            z_out[op, 1] = down
            for s in (1, -1):
                @pl.when(has["ea", s])
                def _():
                    z_copy(op, s).start()

        def by_sides(name, two, one, sem):
            @pl.when(sides[name] == 2)
            def _():
                landed(two, sem)

            @pl.when(sides[name] == 1)
            def _():
                landed(one, sem)

        def x_wait(op):
            by_sides("gx", x_in.at[op], x_in.at[op, 0], x_r.at[op])

        def yz_wait(op):
            by_sides("gy", y_in.at[op], y_in.at[op, 0], y_r.at[op])
            by_sides("ea", z_in.at[op], z_in.at[op, 0], z_r.at[op])

        def side_wait(name, buffer, sem, s):
            @pl.when(has[name, -s])
            def _():
                landed(buffer.at[last, slot[s]], sem.at[arrival(last, s)])

        def pick(op):
            v3 = vu[op].reshape(comps, per, dz)
            folds = jnp.concatenate(
                [
                    jnp.concatenate([v3[i, :half], v3[i, half:]], axis=1)
                    for i in range(comps)
                ],
                axis=0,
            )
            seen = folded(jnp.dot(stacked(folds), lanes[...], preferred_element_type=F32))
            return [
                jnp.sum(seen[i * half : (i + 1) * half] * rows[...], axis=0, keepdims=True)
                for i in range(comps)
            ]

        def pick_send(op, picked, added=None):
            for i in range(comps):
                for o in range(n_ea):
                    line = picked[i][:, slabs(o)]
                    if added is not None:
                        line = line + s_in[added, o, i : i + 1, :]
                    p_out[op, o, i : i + 1, :] = line
            column_send(functools.partial(p_copy, op))

        def local(op):
            v4 = vu[op]
            v2 = v4.reshape(allrows, dz)
            zero = jnp.zeros((comps, 1, dy, dz), F32)
            near = jnp.concatenate([zero, v4[:, : dx - 1]], axis=1) + jnp.concatenate(
                [v4[:, 1:], zero], axis=1
            )
            near = near.reshape(allrows, dz)
            lane_all = iota((allrows, dz), 1)
            row_all = lax.rem(iota((allrows, dz), 0), dy)
            near = near + jnp.where(lane_all == 0, 0.0, pltpu.roll(v2, 1, 1))
            near = near + jnp.where(lane_all == dz - 1, 0.0, pltpu.roll(v2, dz - 1, 1))
            near = near + jnp.where(row_all == 0, 0.0, pltpu.roll(v2, 1, 0))
            near = near + jnp.where(row_all == dy - 1, 0.0, pltpu.roll(v2, allrows - 1, 0))
            vu[op + 1] = centre_diag[...][None] * v4 - near.reshape(v4.shape)

        def local_nodes(op):
            w = wu[op]
            acc = stiff[0] * w[0:1]
            for p in range(1, ecomp):
                acc = acc + stiff[p] * w[p : p + 1]
            wu[op + 1] = acc

        def product(op_a, op_b):
            pv = jnp.sum((vu[op_a] * vu[op_b]).reshape(groups8, 8, dz), axis=0)
            pw = jnp.sum(wu[op_a] * wu[op_b], axis=0, keepdims=True)
            total = jnp.sum(pv, axis=0, keepdims=True)
            for b in range(enb // dz):
                total = total + pw[:, b * dz : (b + 1) * dz]
            return total

        def picks_wait(op):
            p_in[op, ek] = p_out[op, ek]
            landed(p_in.at[op, : n_ea - 1], p_r.at[op])

        def slot_terms(op):
            terms = []
            for o in range(n_ea):
                total = None
                for i in range(comps):
                    term = win[o, i] * p_in[op, o, i : i + 1, :]
                    total = term if total is None else total + term
                terms.append(total)
            return stacked(jnp.concatenate(terms, axis=1))

        def nodes_step(op, terms):
            wu[op + 1] += folded(times_transposed(terms, nodes_t[...]))

        def at_slots(op):
            return folded(jnp.dot(stacked(wu[op]), nodes_t[...], preferred_element_type=F32))

        def sums_send(op, values):
            for o in range(n_ea):
                for i in range(comps):
                    s_out[op, o, i : i + 1, :] = jnp.sum(
                        win[o, i] * values[:, slabs(o)], axis=0, keepdims=True
                    )
            column_send(functools.partial(s_copy, op))

        def first_sums():
            w_in[ek] = wu[0]
            landed(w_in.at[: n_ea - 1], w_r.at[0])
            for o in range(n_ea):
                values = folded(jnp.dot(stacked(w_in[o]), nodes_mine[o], preferred_element_type=F32))
                for i in range(comps):
                    s_in[0, o, i : i + 1, :] = jnp.sum(
                        weights[o, i] * values, axis=0, keepdims=True
                    )

        def sums_wait(op):
            s_in[op, ek] = s_out[op, ek]
            landed(s_in.at[op, : n_ea - 1], s_r.at[op])

        def cells_step(op):
            spread_h, spread_l = [], []
            for i in range(comps):
                line = jnp.concatenate([s_in[op, o, i : i + 1, :] for o in range(n_ea)], axis=1)
                h, l = pieces(line)
                spread_h.append(rows_b[...] * h)
                spread_l.append(rows_b[...] * l)
            added = folded(
                times_transposed(jnp.concatenate(spread_h + spread_l, axis=0), lanes[...])
            )
            for i in range(comps):
                for a in range(dx):
                    at = a * dy
                    part = at // half
                    low = i * half + at - part * half
                    vu[op + 1, i, a] += added[low : low + dy, part * dz : (part + 1) * dz]

        def yz_apply(op):
            z_low, z_high = z_in[op, 0], z_in[op, 1]
            for i in range(comps):
                for a in range(dx):
                    at = i * dx + a
                    side = jnp.where(row_i == 0, y_in[op, 0, i, a], 0.0)
                    side = side + jnp.where(row_i == dy - 1, y_in[op, 1, i, a], 0.0)
                    z_l, z_h = [], []
                    for b in range(dy // 8):
                        g = at * (dy // 8) + b
                        z_l.append(jnp.broadcast_to(z_low[:, g : g + 1], (8, dz)))
                        z_h.append(jnp.broadcast_to(z_high[:, g : g + 1], (8, dz)))
                    side = side + jnp.where(lane_b == 0, jnp.concatenate(z_l, axis=0), 0.0)
                    side = side + jnp.where(lane_b == dz - 1, jnp.concatenate(z_h, axis=0), 0.0)
                    vu[op + 1, i, a] -= side

        def x_apply(op):
            vu[op + 1, :, 0] -= x_in[op, 0]
            vu[op + 1, :, dx - 1] -= x_in[op, 1]

        def near_moment(op):
            y = y_in[op, 1] * vu[op, :, :, dy - 1 : dy]
            side = jnp.sum(y.reshape(comps * dx, dz), axis=0, keepdims=True)
            z = z_out[op, 0] * z_in[op, 1]
            return side + jnp.sum(z, axis=0, keepdims=True)

        def slot_moment(op):
            cross = None
            for o in range(n_ea):
                term = p_in[op, o] * s_out[op, o]
                cross = term if cross is None else cross + term
            return jnp.sum(cross, axis=0, keepdims=True)

        def far_moment(op):
            x = x_in[op, 1] * vu[op, :, dx - 1]
            return jnp.sum(x.reshape(comps * dy, dz), axis=0, keepdims=True)

        loads["w"].wait()
        wu[0] = jnp.concatenate([w_first[...], jnp.zeros((epad - ecomp, enb), F32)], axis=0)
        landed(ids, load_s.at[1])

        pl.semaphore_wait(barrier, expected)

        column_send(ids_copy)
        column_send(w_copy)
        if not wide:
            greet(known.at[0])
        loads["v"].wait()
        xy_send(0)
        z_send(0)
        loads["cell"].wait()
        tile = cell[0]
        tile_row = lax.div(tile, dz)
        tile_lane = tile - tile_row * dz
        for o in range(n_ea):
            here = tile_lane[o : o + 1] + jnp.where(tile_row[o : o + 1] >= half, dz, 0)
            lanes[:, slabs(o)] = jnp.where(
                iota((2 * dz, cap), 0) == here, 1.0, 0.0
            ).astype(BF16)
            below = lax.rem(tile_row[o : o + 1], half)
            r = jnp.where(iota((half, cap), 0) == below, 1.0, 0.0)
            rows[:, slabs(o)] = r
            rows_b[:, slabs(o)] = r.astype(BF16)
        pick_send(0, pick(0))
        loads["coupling"].wait()
        column_send(coup_copy)

        for o in range(n_ea):
            nodes_mine[o] = jnp.where(
                iota((enb, cap), 0) == ids[0, 0, o : o + 1, :], 1.0, 0.0
            ).astype(BF16)
        no_row = jnp.zeros((epad - ecomp, cap), F32)

        def masked(raw, k):
            heavi = jnp.where(k >= 1, 1.0, 0.0)
            tip = jnp.where(k == 2, 1.0, 0.0)
            mask = jnp.where(iota((ecomp, cap), 0) < 3, heavi, tip)
            return jnp.concatenate([raw * mask, no_row], axis=0)

        for o in range(n_ea):
            for i in range(comps):
                weights[o, i] = masked(coupling[i, :, slabs(o)], ids[1, 0, o : o + 1, :])
        loads["shift"].wait()
        centre_diag[...] = shift[...] + (6.0 - CENTRE)
        local(0)
        loads["off"].wait()
        loads["diag"].wait()
        for p in range(ecomp):
            whole = 0.5 * (off[p] + off[:, p, :])
            whole = jnp.where(iota((ecomp, enb), 0) == p, diag[p : p + 1, :] - CENTRE, whole)
            stiff[p] = jnp.concatenate([whole, jnp.zeros((epad - ecomp, enb), F32)], axis=0)
        local_nodes(0)
        moments = [product(0, 0)]
        if not wide:
            pl.semaphore_wait(known.at[0], expected)
            greet(known.at[1])
        ids_in[ek] = ids[:, 0, pl.ds(ek, 1), :]
        coup_in[ek] = coupling[:, :, block(0)]
        late = ek == n_ea // 2

        def tables():
            landed(ids_in.at[: n_ea - 1], ids_r.at[0])
            own_rows = jnp.concatenate([ids_in[o, 0] for o in range(n_ea)], axis=0)
            turned[...] = jnp.transpose(
                jnp.concatenate(
                    [own_rows.astype(F32), jnp.zeros((cap - n_ea, cap), F32)], axis=0
                )
            ).astype(jnp.int32)
            for o in range(n_ea):
                nodes_t[:, slabs(o)] = jnp.where(
                    iota((enb, cap), 0) == ids_in[o, 0], 1.0, 0.0
                ).astype(BF16)

        def layers():
            yz_wait(0)
            yz_apply(0)

        def finish_first():
            cells_step(0)
            x_wait(0)
            x_apply(0)
            xy_send(1)

        def sums_first():
            own_rows = jnp.concatenate([ids_in[o, 0] for o in range(n_ea)], axis=0)
            own_columns = turned[...]
            for a in range(n_ea):
                for b in range(n_ea):
                    overlap[slabs(a), slabs(b)] = jnp.where(
                        own_columns[:, a : a + 1] == own_rows[b : b + 1, :], 1.0, 0.0
                    ).astype(BF16)
            values = at_slots(1)
            landed(coup_in.at[: n_ea - 1], coup_r.at[0])
            for o in range(n_ea):
                for i in range(comps):
                    win[o, i] = masked(coup_in[o, i], ids_in[o, 1])
            picks_wait(0)
            terms = slot_terms(0)
            values = values + folded(
                jnp.dot(terms, overlap[...], preferred_element_type=F32)
            )
            sums_send(1, values)

        @pl.when(ek == 1)
        def _():
            tables()
            first_sums()
            layers()

        @pl.when(ek != 1)
        def _():
            layers()
            tables()
            first_sums()

        if not wide:
            pl.semaphore_wait(known.at[1], expected)

        @pl.when(late)
        def _():
            sums_first()
            finish_first()

        @pl.when(jnp.logical_not(late))
        def _():
            finish_first()
            sums_first()

        z_send(1)
        pick_send(1, pick(1))
        nodes_step(0, slot_terms(0))
        for op in range(1, last):
            local(op)
            local_nodes(op)
            moments.append(product(op - 1, op))
            moments.append(product(op, op))
            yz_wait(op)
            yz_apply(op)
            x_wait(op)
            x_apply(op)
            @pl.when(late)
            def _():
                sums_wait(op)
                cells_step(op)
                xy_send(op + 1)
                pick_send(op + 1, pick(op + 1))

            @pl.when(jnp.logical_not(late))
            def _():
                picked = pick(op + 1)
                sums_wait(op)
                pick_send(op + 1, picked, added=op)
                cells_step(op)
                xy_send(op + 1)

            z_send(op + 1)
            picks_wait(op)
            nodes_step(op, slot_terms(op))
            sums_send(op + 1, at_slots(op + 1))

        local(last)
        local_nodes(last)
        moments.append(product(last - 1, last))
        moments.append(product(last, last))
        row = product(last, last + 1)
        packed = jnp.zeros((1, dz), F32)
        for n, m in enumerate(moments):
            packed = jnp.where(lane_r == n, jnp.sum(m, axis=1, keepdims=True), packed)
        red_out[0, 0:1, :] = packed
        halos = (("ea", z_in, z_r), ("gy", y_in, y_r), ("gx", x_in, x_r))
        picks_wait(last)
        row = row + 2.0 * slot_moment(last)
        for name, buffer, sem in halos[:2]:
            side_wait(name, buffer, sem, -1)
        row = row - 2.0 * near_moment(last)
        side_wait(*halos[2], -1)
        red_out[0, 1:2, :] = row - 2.0 * far_moment(last)

        red_start(0, groups[0])
        nodes_step(last, slot_terms(last))
        for name, buffer, sem in halos:
            side_wait(name, buffer, sem, 1)
        yz_apply(last)
        x_apply(last)
        sums_wait(last)
        cells_step(last)
        for name, buffer, sem in (("gx", x_in, x_s), ("gy", y_in, y_s), ("ea", z_in, z_s)):
            by_sides(name, buffer, buffer.at[:, 0], sem.at[0])
        landed(p_in.at[:, : n_ea - 1], p_s.at[0])
        landed(s_in.at[1:, : n_ea - 1], s_s.at[0])
        landed(w_in.at[: n_ea - 1], w_s.at[0])
        landed(ids_in.at[: n_ea - 1], ids_s.at[0])
        landed(coup_in.at[: n_ea - 1], coup_s.at[0])

    dma = pltpu.SemaphoreType.DMA
    one, each, more = dma((1,)), dma((ITERS,)), dma((ITERS + 1,))
    pl.run_scoped(
        steps, dma((9,)), one, one, one, one, one, more, one, more, one, more,
        one, one, one, each, one, each, pltpu.SemaphoreType.REGULAR((2,)),
    )

    for stage, group in enumerate(groups):
        total = members(group)[0]
        if stage > 0:
            red_out[stage] = reduced
            red_start(stage, group)
        landed(red.at[stage, : total - 1], red_s.at[stage])
        landed(red.at[stage, : total - 1], red_r.at[stage])
        reduced = jnp.sum(red[stage, :total], axis=0)

    early = [jnp.broadcast_to(reduced[0:1, n : n + 1], (1, dz)) for n in range(2 * ITERS - 1)]
    final = jnp.broadcast_to(jnp.sum(reduced[1:2], axis=1, keepdims=True), (1, dz))
    sol, res = galerkin_coefficients(early + [final])
    for n, c in enumerate(sol + res):
        coefs[n : n + 1, :] = c


def combine_kernel(vu, wu, coefs, sol_v, res_v, sol_w, res_w):
    ecomp = sol_w.shape[0]
    lane_tiles = sol_w.shape[1] // coefs.shape[1]

    def wider(factor):
        return jnp.concatenate([factor] * lane_tiles, axis=1)

    solution = [coefs[n : n + 1, :] for n in range(ITERS)]
    residual = [coefs[ITERS + n : ITERS + n + 1, :] for n in range(ITERS + 1)]

    def combine(factors, terms):
        out = factors[0] * terms[0]
        for f, t in zip(factors[1:], terms[1:]):
            out = out + f * t
        return out

    shape = sol_v.shape
    flat = (shape[0] * shape[1] * shape[2], shape[3])
    v_terms = [vu[n].reshape(flat) for n in range(ITERS + 1)]
    w_terms = [wu[n] for n in range(ITERS + 1)]
    sol_v[...] = combine(solution, v_terms).reshape(shape)
    res_v[...] = combine(residual, v_terms).reshape(shape)
    sol_w[...] = combine([wider(f) for f in solution], w_terms)[:ecomp]
    res_w[...] = combine([wider(f) for f in residual], w_terms)[:ecomp]


def body(sizes, *args):
    load_v, load_w, shift, diag, off, coupling, kind, cell, node = args
    n_ea = sizes[2]
    total = sizes[0] * sizes[1] * sizes[2]
    groups = (AXES,) if total <= 64 else (("gx",), ("gy", "ea"))
    widest = total if total <= 64 else max(sizes[0], sizes[1] * sizes[2])
    comps, dx, dy, dz = load_v.shape
    ecomp, enb = load_w.shape
    cap = node.shape[2]
    vmem = pltpu.VMEM
    dma = pltpu.SemaphoreType.DMA
    epad = -(-ecomp // 16) * 16
    slots = n_ea * cap
    scratch = [
        vmem(load_w.shape, F32), vmem(shift.shape, F32), vmem(diag.shape, F32),
        vmem(off.shape, F32), vmem(coupling.shape, F32),
        vmem(cell.shape, jnp.int32), vmem((2,) + node.shape, jnp.int32),
        vmem((n_ea, comps, epad, cap), F32),
        vmem((n_ea, comps, epad, cap), F32),
        vmem((ecomp, epad, enb), F32),
        vmem((2 * dz, slots), BF16),
        vmem((dx * dy // 2, slots), F32),
        vmem((dx * dy // 2, slots), BF16),
        vmem((n_ea, enb, cap), BF16),
        vmem((enb, slots), BF16),
        vmem((slots, slots), BF16),
        vmem((cap, cap), jnp.int32),
        vmem((dx, dy, dz), F32),
        vmem((n_ea, 2, 1, cap), jnp.int32),
        vmem((n_ea, comps, ecomp, cap), F32),
        vmem((ITERS, 2, comps, dy, dz), F32),
        vmem((ITERS, 2, comps, dx, 1, dz), F32),
        vmem((ITERS, 2, 8, dz), F32),
        vmem((n_ea, epad, enb), F32),
        vmem((ITERS, n_ea, comps, cap), F32),
        vmem((ITERS, n_ea, comps, cap), F32),
        vmem((ITERS, 2, 8, dz), F32),
        vmem((ITERS, n_ea, comps, cap), F32),
        vmem((ITERS, n_ea, comps, cap), F32),
        vmem((len(groups), widest, 2, dz), F32),
        vmem((len(groups), 2, dz), F32),
        dma((len(groups),)), dma((len(groups),)),
    ]
    basis = pl.pallas_call(
        functools.partial(kernel, sizes, groups),
        out_shape=(
            pltpu.VMEM((ITERS + 1,) + load_v.shape, F32),
            pltpu.VMEM((ITERS + 1, epad, enb), F32),
            pltpu.VMEM((2 * ITERS + 2, dz), F32),
        ),
        in_specs=[pl.BlockSpec(memory_space=pltpu.HBM)] * 9,
        out_specs=[pl.BlockSpec(memory_space=vmem)] * 3,
        scratch_shapes=scratch,
        compiler_params=pltpu.CompilerParams(
            collective_id=0, has_side_effects=True
        ),
        name="krylov",
    )(*args)
    return tuple(
        pl.pallas_call(
            combine_kernel,
            out_shape=tuple(
                jax.ShapeDtypeStruct(like.shape, F32)
                for like in (load_v, load_v, load_w, load_w)
            ),
            in_specs=[pl.BlockSpec(memory_space=vmem)] * 3,
            out_specs=[pl.BlockSpec(memory_space=vmem)] * 4,
            compiler_params=pltpu.CompilerParams(vmem_limit_bytes=8 << 20),
            name="combine",
        )(*basis)
    )


def solution(mesh):
    column = ("gx", "gy", "ea")
    placed = (
        P(None, "gx", "gy", "ea"),
        P(None, column),
        P("gx", "gy", "ea"),
        P(None, column),
        P(None, None, column),
        P(None, None, column),
        P(column, None, None),
        P(column, None, None),
        P(column, None, None),
    )
    return jax.shard_map(
        functools.partial(body, tuple(mesh.shape[a] for a in AXES)),
        mesh=mesh,
        in_specs=placed,
        out_specs=(
            P(None, "gx", "gy", "ea"),
            P(None, "gx", "gy", "ea"),
            P(None, column),
            P(None, column),
        ),
        check_vma=False,
    )
```

```python
import functools

import jax
import jax.numpy as jnp
from jax import lax
from jax.experimental import pallas as pl
from jax.experimental.pallas import tpu as pltpu
from jax.sharding import PartitionSpec as P

ITERS = 3
CENTRE = 11.5
AXES = ("gx", "gy", "ea")
MESH = pl.DeviceIdType.MESH
F32 = jnp.float32
BF16 = jnp.bfloat16


def pieces(x):
    high = x.astype(BF16)
    return high, (x - high.astype(F32)).astype(BF16)


def stacked(x):
    high, low = pieces(x)
    return jnp.concatenate([high, low], axis=0)


def folded(product):
    half = product.shape[0] // 2
    return product[:half] + product[half:]


def iota(shape, dim):
    return lax.broadcasted_iota(jnp.int32, shape, dim)


def times_transposed(a, b):
    return lax.dot_general(
        a, b, (((1,), (1,)), ((), ())), preferred_element_type=F32
    )


def cg_coefficients(moment):
    def inner(first, second):
        total = None
        for i, a in enumerate(first):
            for j, b in enumerate(second):
                term = a * b * moment[i + j]
                total = term if total is None else total + term
        return total

    one = jnp.ones_like(moment[0])
    residual, direction, solution = [one], [one], []
    norm = moment[0]
    for step in range(ITERS):
        image = [CENTRE * d for d in direction] + [0.0 * one]
        for i, d in enumerate(direction):
            image[i + 1] = image[i + 1] + d
        alpha = norm / inner(direction, image)
        solution = [
            (solution[i] if i < len(solution) else 0.0) + alpha * d
            for i, d in enumerate(direction)
        ]
        residual = [
            (residual[i] if i < len(residual) else 0.0) - alpha * d for i, d in enumerate(image)
        ]
        if step + 1 < ITERS:
            new = inner(residual, residual)
            ratio = new / norm
            norm = new
            direction = [
                r + (ratio * direction[i] if i < len(direction) else 0.0)
                for i, r in enumerate(residual)
            ]
    return solution, residual


def kernel(
    sizes, groups,
    load_v, load_w, shift_h, diag_h, off_h, coupling_h, kind_h, cell_h, node_h,
    vu, wu, coefs,
    w_first, shift, diag, off, coupling, cell, ids,
    weights, win, stiff, lanes, rows, rows_b, nodes_mine, nodes_t, overlap,
    centre_diag, ids_in, coup_in,
    x_in, y_in, z_in, w_in, p_in, s_in, z_out, p_out, s_out, red, red_out,
    red_s, red_r,
):
    n_gx, n_gy, n_ea = sizes
    comps, dx, dy, dz = load_v.shape
    ecomp, enb = load_w.shape
    epad = wu.shape[1]
    cap = cell.shape[2]
    per = dx * dy
    half = per // 2
    allrows = comps * per
    groups8 = allrows // 8
    gi, gj, ek = (lax.axis_index(a) for a in AXES)
    own = {"gx": gi, "gy": gj, "ea": ek}
    count = dict(zip(AXES, sizes))

    def members(group):
        total = 1
        for a in group:
            total *= count[a]
        me = 0
        for a in group:
            me = me * count[a] + own[a]

        def target(d):
            flat = lax.rem(me + d, total)
            coords = dict(own)
            for a in reversed(group):
                coords[a] = lax.rem(flat, count[a])
                flat = lax.div(flat, count[a])
            return tuple(coords[a] for a in AXES)

        return total, me, target

    def remote(src, dst, s_sem, r_sem, device):
        return pltpu.make_async_remote_copy(
            src_ref=src, dst_ref=dst, send_sem=s_sem, recv_sem=r_sem,
            device_id=device, device_id_type=MESH,
        )

    def landed(ref, sem):
        pltpu.make_async_copy(ref, ref, sem).wait()

    def red_start(stage, group):
        total, me, target = members(group)
        for d in range(total - 1):
            dst = red.at[stage, me]
            ends = (red_s.at[stage], red_r.at[stage])
            if group == AXES:
                pltpu.make_async_remote_copy(
                    src_ref=red_out.at[stage], dst_ref=dst, send_sem=ends[0], recv_sem=ends[1],
                    device_id=d + jnp.where(me <= d, 1, 0),
                    device_id_type=pl.DeviceIdType.LOGICAL,
                ).start()
            else:
                remote(red_out.at[stage], dst, *ends, target(d + 1)).start()
        red[stage, me] = red_out[stage]

    def steps(
        load_s, ids_s, ids_r, coup_s, coup_r, x_s, x_r, y_s, y_r, z_s, z_r,
        w_s, w_r, p_s, p_r, s_s, s_r, known,
    ):
        has = {
            ("gx", 1): gi < n_gx - 1, ("gx", -1): gi > 0,
            ("gy", 1): gj < n_gy - 1, ("gy", -1): gj > 0,
            ("ea", 1): ek < n_ea - 1, ("ea", -1): ek > 0,
        }
        beside = {
            ("gx", s): (gi + s, gj, ek) for s in (1, -1)
        } | {("gy", s): (gi, gj + s, ek) for s in (1, -1)} | {
            ("ea", s): (gi, gj, ek + s) for s in (1, -1)
        }
        slot = {1: 0, -1: 1}
        last = ITERS - 1
        sides = {
            name: jnp.where(has[name, 1], 1, 0) + jnp.where(has[name, -1], 1, 0) for name in AXES
        }


        barrier = pltpu.get_barrier_semaphore()
        wide = n_gx + n_gy - 2 + (n_ea > 1) > ITERS + 2

        def greet(sem):
            for d in range(1, n_ea):
                pl.semaphore_signal(
                    sem, inc=1, device_id=(gi, gj, lax.rem(ek + d, n_ea)), device_id_type=MESH
                )
            for name in ("gx", "gy"):
                for s in (1, -1):
                    @pl.when(has[name, s])
                    def _():
                        pl.semaphore_signal(
                            sem, inc=1, device_id=beside[name, s], device_id_type=MESH
                        )

        if wide:
            expected = 0
            for group in groups:
                total, _, target = members(group)
                for d in range(1, total):
                    pl.semaphore_signal(
                        barrier, inc=1, device_id=target(d), device_id_type=MESH
                    )
                expected += total - 1
        else:
            greet(barrier)
            expected = n_ea - 1 + sides["gx"] + sides["gy"]

        loads = {}
        for at, (name, src, dst) in enumerate((
            ("w", load_w, w_first), ("node", node_h, ids.at[0]), ("kind", kind_h, ids.at[1]),
            ("v", load_v, vu.at[0]), ("cell", cell_h, cell), ("coupling", coupling_h, coupling),
            ("shift", shift_h, shift), ("off", off_h, off), ("diag", diag_h, diag),
        )):
            at = 1 if name == "kind" else at
            loads[name] = pltpu.make_async_copy(src, dst, load_s.at[at])
            loads[name].start()

        for s in (1, -1):
            for name, buffer in (("gx", x_in), ("gy", y_in), ("ea", z_in)):
                @pl.when(jnp.logical_not(has[name, -s]))
                def _():
                    for op in range(ITERS):
                        buffer[op, slot[s]] = jnp.zeros(buffer.shape[2:], F32)

        def partner(d):
            return lax.rem(ek + d, n_ea)

        def arrival(op, s):
            return op + 1 if op == last and s == 1 else op

        def x_copy(op, s):
            return remote(
                vu.at[op, :, dx - 1 if s == 1 else 0], x_in.at[op, slot[s]],
                x_s.at[0], x_r.at[arrival(op, s)], beside["gx", s],
            )

        def y_copy(op, s):
            edge = dy - 1 if s == 1 else 0
            return remote(
                vu.at[op, :, :, edge : edge + 1, :], y_in.at[op, slot[s]],
                y_s.at[0], y_r.at[arrival(op, s)], beside["gy", s],
            )

        def z_copy(op, s):
            return remote(
                z_out.at[op, slot[s]], z_in.at[op, slot[s]],
                z_s.at[0], z_r.at[arrival(op, s)], beside["ea", s],
            )

        def column_copy(src, dst, s_sem, r_sem, d):
            return remote(src, dst.at[ek], s_sem, r_sem, (gi, gj, partner(d)))

        def w_copy(d):
            return column_copy(wu.at[0], w_in, w_s.at[0], w_r.at[0], d)

        def p_copy(op, d):
            return column_copy(
                p_out.at[op, partner(d)], p_in.at[op], p_s.at[0], p_r.at[op], d
            )

        def s_copy(op, d):
            return column_copy(
                s_out.at[op, partner(d)], s_in.at[op], s_s.at[0], s_r.at[op], d
            )

        def ids_copy(d):
            return column_copy(
                ids.at[:, 0, pl.ds(partner(d), 1), :], ids_in, ids_s.at[0], ids_r.at[0], d
            )

        def block(d):
            return pl.ds(pl.multiple_of(partner(d) * cap, cap), cap)

        def coup_copy(d):
            return column_copy(
                coupling.at[:, :, block(d)], coup_in, coup_s.at[0], coup_r.at[0], d
            )

        def column_send(copy):
            for d in range(1, n_ea):
                copy(d).start()

        lane_i = iota((8, dz), 1)
        lane_r = iota((1, dz), 1)
        row_i = iota((dy, dz), 0)
        lane_b = iota((dy, dz), 1)

        def slabs(o):
            return slice(o * cap, (o + 1) * cap)

        def xy_send(op):
            for s in (1, -1):
                for name, copy in (("gx", x_copy), ("gy", y_copy)):
                    @pl.when(has[name, s])
                    def _():
                        copy(op, s).start()

        def z_send(op):
            v2 = vu[op].reshape(allrows, dz)
            up = jnp.zeros((8, dz), F32)
            down = jnp.zeros((8, dz), F32)
            for g in range(groups8):
                part = v2[8 * g : 8 * g + 8]
                up = jnp.where(lane_i == g, part[:, dz - 1 : dz], up)
                down = jnp.where(lane_i == g, part[:, 0:1], down)
            z_out[op, 0] = up
            z_out[op, 1] = down
            for s in (1, -1):
                @pl.when(has["ea", s])
                def _():
                    z_copy(op, s).start()

        def by_sides(name, two, one, sem):
            @pl.when(sides[name] == 2)
            def _():
                landed(two, sem)

            @pl.when(sides[name] == 1)
            def _():
                landed(one, sem)

        def x_wait(op):
            by_sides("gx", x_in.at[op], x_in.at[op, 0], x_r.at[op])

        def yz_wait(op):
            by_sides("gy", y_in.at[op], y_in.at[op, 0], y_r.at[op])
            by_sides("ea", z_in.at[op], z_in.at[op, 0], z_r.at[op])

        def side_wait(name, buffer, sem, s):
            @pl.when(has[name, -s])
            def _():
                landed(buffer.at[last, slot[s]], sem.at[arrival(last, s)])

        def pick(op):
            v3 = vu[op].reshape(comps, per, dz)
            folds = jnp.concatenate(
                [
                    jnp.concatenate([v3[i, :half], v3[i, half:]], axis=1)
                    for i in range(comps)
                ],
                axis=0,
            )
            seen = folded(jnp.dot(stacked(folds), lanes[...], preferred_element_type=F32))
            return [
                jnp.sum(seen[i * half : (i + 1) * half] * rows[...], axis=0, keepdims=True)
                for i in range(comps)
            ]

        def pick_send(op, picked, added=None):
            for i in range(comps):
                for o in range(n_ea):
                    line = picked[i][:, slabs(o)]
                    if added is not None:
                        line = line + s_in[added, o, i : i + 1, :]
                    p_out[op, o, i : i + 1, :] = line
            column_send(functools.partial(p_copy, op))

        def local(op):
            v4 = vu[op]
            v2 = v4.reshape(allrows, dz)
            zero = jnp.zeros((comps, 1, dy, dz), F32)
            near = jnp.concatenate([zero, v4[:, : dx - 1]], axis=1) + jnp.concatenate(
                [v4[:, 1:], zero], axis=1
            )
            near = near.reshape(allrows, dz)
            lane_all = iota((allrows, dz), 1)
            row_all = lax.rem(iota((allrows, dz), 0), dy)
            near = near + jnp.where(lane_all == 0, 0.0, pltpu.roll(v2, 1, 1))
            near = near + jnp.where(lane_all == dz - 1, 0.0, pltpu.roll(v2, dz - 1, 1))
            near = near + jnp.where(row_all == 0, 0.0, pltpu.roll(v2, 1, 0))
            near = near + jnp.where(row_all == dy - 1, 0.0, pltpu.roll(v2, allrows - 1, 0))
            vu[op + 1] = centre_diag[...][None] * v4 - near.reshape(v4.shape)

        def local_nodes(op):
            w = wu[op]
            acc = stiff[0] * w[0:1]
            for p in range(1, ecomp):
                acc = acc + stiff[p] * w[p : p + 1]
            wu[op + 1] = acc

        def product(op_a, op_b):
            pv = jnp.sum((vu[op_a] * vu[op_b]).reshape(groups8, 8, dz), axis=0)
            pw = jnp.sum(wu[op_a] * wu[op_b], axis=0, keepdims=True)
            total = jnp.sum(pv, axis=0, keepdims=True)
            for b in range(enb // dz):
                total = total + pw[:, b * dz : (b + 1) * dz]
            return total

        def picks_wait(op):
            p_in[op, ek] = p_out[op, ek]
            landed(p_in.at[op, : n_ea - 1], p_r.at[op])

        def slot_terms(op):
            terms = []
            for o in range(n_ea):
                total = None
                for i in range(comps):
                    term = win[o, i] * p_in[op, o, i : i + 1, :]
                    total = term if total is None else total + term
                terms.append(total)
            return stacked(jnp.concatenate(terms, axis=1))

        def nodes_step(op, terms):
            wu[op + 1] += folded(times_transposed(terms, nodes_t[...]))

        def at_slots(op):
            return folded(jnp.dot(stacked(wu[op]), nodes_t[...], preferred_element_type=F32))

        def sums_send(op, values):
            for o in range(n_ea):
                for i in range(comps):
                    s_out[op, o, i : i + 1, :] = jnp.sum(
                        win[o, i] * values[:, slabs(o)], axis=0, keepdims=True
                    )
            column_send(functools.partial(s_copy, op))

        def first_sums():
            w_in[ek] = wu[0]
            landed(w_in.at[: n_ea - 1], w_r.at[0])
            for o in range(n_ea):
                values = folded(jnp.dot(stacked(w_in[o]), nodes_mine[o], preferred_element_type=F32))
                for i in range(comps):
                    s_in[0, o, i : i + 1, :] = jnp.sum(
                        weights[o, i] * values, axis=0, keepdims=True
                    )

        def sums_wait(op):
            s_in[op, ek] = s_out[op, ek]
            landed(s_in.at[op, : n_ea - 1], s_r.at[op])

        def cells_step(op):
            spread_h, spread_l = [], []
            for i in range(comps):
                line = jnp.concatenate([s_in[op, o, i : i + 1, :] for o in range(n_ea)], axis=1)
                h, l = pieces(line)
                spread_h.append(rows_b[...] * h)
                spread_l.append(rows_b[...] * l)
            added = folded(
                times_transposed(jnp.concatenate(spread_h + spread_l, axis=0), lanes[...])
            )
            for i in range(comps):
                for a in range(dx):
                    at = a * dy
                    part = at // half
                    low = i * half + at - part * half
                    vu[op + 1, i, a] += added[low : low + dy, part * dz : (part + 1) * dz]

        def yz_apply(op):
            z_low, z_high = z_in[op, 0], z_in[op, 1]
            for i in range(comps):
                for a in range(dx):
                    at = i * dx + a
                    side = jnp.where(row_i == 0, y_in[op, 0, i, a], 0.0)
                    side = side + jnp.where(row_i == dy - 1, y_in[op, 1, i, a], 0.0)
                    z_l, z_h = [], []
                    for b in range(dy // 8):
                        g = at * (dy // 8) + b
                        z_l.append(jnp.broadcast_to(z_low[:, g : g + 1], (8, dz)))
                        z_h.append(jnp.broadcast_to(z_high[:, g : g + 1], (8, dz)))
                    side = side + jnp.where(lane_b == 0, jnp.concatenate(z_l, axis=0), 0.0)
                    side = side + jnp.where(lane_b == dz - 1, jnp.concatenate(z_h, axis=0), 0.0)
                    vu[op + 1, i, a] -= side

        def x_apply(op):
            vu[op + 1, :, 0] -= x_in[op, 0]
            vu[op + 1, :, dx - 1] -= x_in[op, 1]

        def near_moment(op):
            y = y_in[op, 1] * vu[op, :, :, dy - 1 : dy]
            side = jnp.sum(y.reshape(comps * dx, dz), axis=0, keepdims=True)
            z = z_out[op, 0] * z_in[op, 1]
            return side + jnp.sum(z, axis=0, keepdims=True)

        def slot_moment(op):
            cross = None
            for o in range(n_ea):
                term = p_in[op, o] * s_out[op, o]
                cross = term if cross is None else cross + term
            return jnp.sum(cross, axis=0, keepdims=True)

        def far_moment(op):
            x = x_in[op, 1] * vu[op, :, dx - 1]
            return jnp.sum(x.reshape(comps * dy, dz), axis=0, keepdims=True)

        loads["w"].wait()
        wu[0] = jnp.concatenate([w_first[...], jnp.zeros((epad - ecomp, enb), F32)], axis=0)
        landed(ids, load_s.at[1])

        pl.semaphore_wait(barrier, expected)

        column_send(ids_copy)
        column_send(w_copy)
        if not wide:
            greet(known.at[0])
        loads["v"].wait()
        xy_send(0)
        z_send(0)
        loads["cell"].wait()
        tile = cell[0]
        tile_row = lax.div(tile, dz)
        tile_lane = tile - tile_row * dz
        for o in range(n_ea):
            here = tile_lane[o : o + 1] + jnp.where(tile_row[o : o + 1] >= half, dz, 0)
            lanes[:, slabs(o)] = jnp.where(
                iota((2 * dz, cap), 0) == here, 1.0, 0.0
            ).astype(BF16)
            below = lax.rem(tile_row[o : o + 1], half)
            r = jnp.where(iota((half, cap), 0) == below, 1.0, 0.0)
            rows[:, slabs(o)] = r
            rows_b[:, slabs(o)] = r.astype(BF16)
        pick_send(0, pick(0))
        loads["coupling"].wait()
        column_send(coup_copy)

        for o in range(n_ea):
            nodes_mine[o] = jnp.where(
                iota((enb, cap), 0) == ids[0, 0, o : o + 1, :], 1.0, 0.0
            ).astype(BF16)
        no_row = jnp.zeros((epad - ecomp, cap), F32)

        def masked(raw, k):
            heavi = jnp.where(k >= 1, 1.0, 0.0)
            tip = jnp.where(k == 2, 1.0, 0.0)
            mask = jnp.where(iota((ecomp, cap), 0) < 3, heavi, tip)
            return jnp.concatenate([raw * mask, no_row], axis=0)

        for o in range(n_ea):
            for i in range(comps):
                weights[o, i] = masked(coupling[i, :, slabs(o)], ids[1, 0, o : o + 1, :])
        loads["shift"].wait()
        centre_diag[...] = shift[...] + (6.0 - CENTRE)
        local(0)
        loads["off"].wait()
        loads["diag"].wait()
        for p in range(ecomp):
            whole = 0.5 * (off[p] + off[:, p, :])
            whole = jnp.where(iota((ecomp, enb), 0) == p, diag[p : p + 1, :] - CENTRE, whole)
            stiff[p] = jnp.concatenate([whole, jnp.zeros((epad - ecomp, enb), F32)], axis=0)
        local_nodes(0)
        moments = [product(0, 0)]
        if not wide:
            pl.semaphore_wait(known.at[0], expected)
            greet(known.at[1])
        ids_in[ek] = ids[:, 0, pl.ds(ek, 1), :]
        coup_in[ek] = coupling[:, :, block(0)]
        yz_wait(0)
        yz_apply(0)
        landed(ids_in.at[: n_ea - 1], ids_r.at[0])
        own_rows = jnp.concatenate([ids_in[o, 0] for o in range(n_ea)], axis=0)
        own_columns = jnp.transpose(
            jnp.concatenate(
                [own_rows.astype(F32), jnp.zeros((cap - n_ea, cap), F32)], axis=0
            )
        ).astype(jnp.int32)
        for o in range(n_ea):
            nodes_t[:, slabs(o)] = jnp.where(
                iota((enb, cap), 0) == ids_in[o, 0], 1.0, 0.0
            ).astype(BF16)
        first_sums()
        cells_step(0)
        x_wait(0)
        x_apply(0)
        if not wide:
            pl.semaphore_wait(known.at[1], expected)
        xy_send(1)
        for a in range(n_ea):
            for b in range(n_ea):
                overlap[slabs(a), slabs(b)] = jnp.where(
                    own_columns[:, a : a + 1] == own_rows[b : b + 1, :], 1.0, 0.0
                ).astype(BF16)
        values = at_slots(1)
        landed(coup_in.at[: n_ea - 1], coup_r.at[0])
        for o in range(n_ea):
            for i in range(comps):
                win[o, i] = masked(coup_in[o, i], ids_in[o, 1])
        picks_wait(0)
        terms = slot_terms(0)
        values = values + folded(
            jnp.dot(terms, overlap[...], preferred_element_type=F32)
        )
        sums_send(1, values)
        z_send(1)
        pick_send(1, pick(1))
        nodes_step(0, terms)
        for op in range(1, last):
            local(op)
            local_nodes(op)
            moments.append(product(op - 1, op))
            moments.append(product(op, op))
            yz_wait(op)
            yz_apply(op)
            x_wait(op)
            x_apply(op)
            late = ek == n_ea // 2

            @pl.when(late)
            def _():
                sums_wait(op)
                cells_step(op)
                xy_send(op + 1)
                pick_send(op + 1, pick(op + 1))

            @pl.when(jnp.logical_not(late))
            def _():
                picked = pick(op + 1)
                sums_wait(op)
                pick_send(op + 1, picked, added=op)
                cells_step(op)
                xy_send(op + 1)

            z_send(op + 1)
            picks_wait(op)
            nodes_step(op, slot_terms(op))
            sums_send(op + 1, at_slots(op + 1))

        local(last)
        local_nodes(last)
        moments.append(product(last - 1, last))
        moments.append(product(last, last))
        row = product(last, last + 1)
        packed = jnp.zeros((1, dz), F32)
        for n, m in enumerate(moments):
            packed = jnp.where(lane_r == n, jnp.sum(m, axis=1, keepdims=True), packed)
        halos = (("ea", z_in, z_r), ("gy", y_in, y_r), ("gx", x_in, x_r))
        picks_wait(last)
        row = row + 2.0 * slot_moment(last)
        for name, buffer, sem in halos[:2]:
            side_wait(name, buffer, sem, -1)
        row = row - 2.0 * near_moment(last)
        side_wait(*halos[2], -1)
        final = jnp.sum(row - 2.0 * far_moment(last), axis=1, keepdims=True)
        red_out[0] = jnp.where(lane_r == 2 * ITERS - 1, final, packed)

        red_start(0, groups[0])
        nodes_step(last, slot_terms(last))
        for name, buffer, sem in halos:
            side_wait(name, buffer, sem, 1)
        yz_apply(last)
        x_apply(last)
        sums_wait(last)
        cells_step(last)
        for name, buffer, sem in (("gx", x_in, x_s), ("gy", y_in, y_s), ("ea", z_in, z_s)):
            by_sides(name, buffer, buffer.at[:, 0], sem.at[0])
        landed(p_in.at[:, : n_ea - 1], p_s.at[0])
        landed(s_in.at[1:, : n_ea - 1], s_s.at[0])
        landed(w_in.at[: n_ea - 1], w_s.at[0])
        landed(ids_in.at[: n_ea - 1], ids_s.at[0])
        landed(coup_in.at[: n_ea - 1], coup_s.at[0])

    dma = pltpu.SemaphoreType.DMA
    one, each, more = dma((1,)), dma((ITERS,)), dma((ITERS + 1,))
    pl.run_scoped(
        steps, dma((9,)), one, one, one, one, one, more, one, more, one, more,
        one, one, one, each, one, each, pltpu.SemaphoreType.REGULAR((2,)),
    )

    for stage, group in enumerate(groups):
        total = members(group)[0]
        if stage > 0:
            red_out[stage] = reduced
            red_start(stage, group)
        landed(red.at[stage, : total - 1], red_s.at[stage])
        landed(red.at[stage, : total - 1], red_r.at[stage])
        reduced = jnp.sum(red[stage, :total], axis=0)

    early = [jnp.broadcast_to(reduced[:, n : n + 1], (1, dz)) for n in range(2 * ITERS)]
    sol, res = cg_coefficients(early)
    for n, c in enumerate(sol + res):
        coefs[n : n + 1, :] = c


def combine_kernel(vu, wu, coefs, sol_v, res_v, sol_w, res_w):
    ecomp = sol_w.shape[0]
    lane_tiles = sol_w.shape[1] // coefs.shape[1]

    def wider(factor):
        return jnp.concatenate([factor] * lane_tiles, axis=1)

    solution = [coefs[n : n + 1, :] for n in range(ITERS)]
    residual = [coefs[ITERS + n : ITERS + n + 1, :] for n in range(ITERS + 1)]

    def combine(factors, terms):
        out = factors[0] * terms[0]
        for f, t in zip(factors[1:], terms[1:]):
            out = out + f * t
        return out

    shape = sol_v.shape
    flat = (shape[0] * shape[1] * shape[2], shape[3])
    v_terms = [vu[n].reshape(flat) for n in range(ITERS + 1)]
    w_terms = [wu[n] for n in range(ITERS + 1)]
    sol_v[...] = combine(solution, v_terms).reshape(shape)
    res_v[...] = combine(residual, v_terms).reshape(shape)
    sol_w[...] = combine([wider(f) for f in solution], w_terms)[:ecomp]
    res_w[...] = combine([wider(f) for f in residual], w_terms)[:ecomp]


def body(sizes, *args):
    load_v, load_w, shift, diag, off, coupling, kind, cell, node = args
    n_ea = sizes[2]
    total = sizes[0] * sizes[1] * sizes[2]
    groups = (AXES,) if total <= 64 else (("gx",), ("gy", "ea"))
    widest = total if total <= 64 else max(sizes[0], sizes[1] * sizes[2])
    comps, dx, dy, dz = load_v.shape
    ecomp, enb = load_w.shape
    cap = node.shape[2]
    vmem = pltpu.VMEM
    dma = pltpu.SemaphoreType.DMA
    epad = -(-ecomp // 16) * 16
    slots = n_ea * cap
    scratch = [
        vmem(load_w.shape, F32), vmem(shift.shape, F32), vmem(diag.shape, F32),
        vmem(off.shape, F32), vmem(coupling.shape, F32),
        vmem(cell.shape, jnp.int32), vmem((2,) + node.shape, jnp.int32),
        vmem((n_ea, comps, epad, cap), F32),
        vmem((n_ea, comps, epad, cap), F32),
        vmem((ecomp, epad, enb), F32),
        vmem((2 * dz, slots), BF16),
        vmem((dx * dy // 2, slots), F32),
        vmem((dx * dy // 2, slots), BF16),
        vmem((n_ea, enb, cap), BF16),
        vmem((enb, slots), BF16),
        vmem((slots, slots), BF16),
        vmem((dx, dy, dz), F32),
        vmem((n_ea, 2, 1, cap), jnp.int32),
        vmem((n_ea, comps, ecomp, cap), F32),
        vmem((ITERS, 2, comps, dy, dz), F32),
        vmem((ITERS, 2, comps, dx, 1, dz), F32),
        vmem((ITERS, 2, 8, dz), F32),
        vmem((n_ea, epad, enb), F32),
        vmem((ITERS, n_ea, comps, cap), F32),
        vmem((ITERS, n_ea, comps, cap), F32),
        vmem((ITERS, 2, 8, dz), F32),
        vmem((ITERS, n_ea, comps, cap), F32),
        vmem((ITERS, n_ea, comps, cap), F32),
        vmem((len(groups), widest, 1, dz), F32),
        vmem((len(groups), 1, dz), F32),
        dma((len(groups),)), dma((len(groups),)),
    ]
    basis = pl.pallas_call(
        functools.partial(kernel, sizes, groups),
        out_shape=(
            pltpu.VMEM((ITERS + 1,) + load_v.shape, F32),
            pltpu.VMEM((ITERS + 1, epad, enb), F32),
            pltpu.VMEM((2 * ITERS + 2, dz), F32),
        ),
        in_specs=[pl.BlockSpec(memory_space=pltpu.HBM)] * 9,
        out_specs=[pl.BlockSpec(memory_space=vmem)] * 3,
        scratch_shapes=scratch,
        compiler_params=pltpu.CompilerParams(
            collective_id=0, has_side_effects=True
        ),
        name="krylov",
    )(*args)
    return tuple(
        pl.pallas_call(
            combine_kernel,
            out_shape=tuple(
                jax.ShapeDtypeStruct(like.shape, F32)
                for like in (load_v, load_v, load_w, load_w)
            ),
            in_specs=[pl.BlockSpec(memory_space=vmem)] * 3,
            out_specs=[pl.BlockSpec(memory_space=vmem)] * 4,
            compiler_params=pltpu.CompilerParams(vmem_limit_bytes=8 << 20),
            name="combine",
        )(*basis)
    )


def solution(mesh):
    column = ("gx", "gy", "ea")
    placed = (
        P(None, "gx", "gy", "ea"),
        P(None, column),
        P("gx", "gy", "ea"),
        P(None, column),
        P(None, None, column),
        P(None, None, column),
        P(column, None, None),
        P(column, None, None),
        P(column, None, None),
    )
    return jax.shard_map(
        functools.partial(body, tuple(mesh.shape[a] for a in AXES)),
        mesh=mesh,
        in_specs=placed,
        out_specs=(
            P(None, "gx", "gy", "ea"),
            P(None, "gx", "gy", "ea"),
            P(None, column),
            P(None, column),
        ),
        check_vma=False,
    )
```
